32 devices in a mesh: groups: 2 (over y), patch: 8 (over z, x), sub: 2 (over core).
Axes of the slice: x: 2, y: 2, z: 4, core: 2. Of those that a mesh axis runs over, the one named last changes fastest.
Arguments:
- block_cols: int32 [64, 3], P(('groups', 'patch', 'sub')), parts along dimension 0, may hold values from 0 to 31, as said below
- step_tiles: float32 [64, 3, 128, 128], P(('groups', 'patch', 'sub')), parts along dimension 0, as said below
- mass: float32 [8192], P(('groups', 'patch', 'sub')), parts along dimension 0, as said below
- warm_start: float32 [8192, 128], P(('groups', 'patch', 'sub')), parts along dimension 0, may hold values from -2.5 to 2.5
- source_ids: int32 [256], P('groups'), parts along dimension 0, may hold values from 0 to 4095
Outputs:
- solution: float32 [8192, 128], P(('groups', 'patch', 'sub')), parts along dimension 0
The draws below stay inside these ranges and needn't reach their ends.
There are 2 independent parts, one for each index of `groups`. The reference program is written for one: setup_inputs(seed, part) draws one part's arguments, and reference() takes and returns one part's arrays. A program takes and returns all parts, laid end to end along the dimension named above; each array names one. Nothing has to cross between parts.
Inputs may be any that keep to these rules, and one draw needn't show every extreme that they name: `block_cols`: slot lists of block row g name g itself and blocks within 1 of g coupled to it; coupling is symmetric (g names h exactly when h names g). Unused slots name g and carry a zero tile. `step_tiles`: entries are not negative. The tile of block row h toward g is the transpose of the tile of row g toward h; the tile of a row toward itself is symmetric with a zero diagonal. `mass`: between 0.1 and 1.2.
All inputs are finite; a program needn't handle non-finite values.
Results may differ from the reference program's by a relative error of at most 0.00023.
Values sent between devices are 32-bit elements; how exact they have to be, the bound alone decides.
No kernel may reach another device: no remote copies, remote signals or barrier semaphores. Data moves between devices by JAX's collectives and lax.ppermute only.
A program may use at most 64 MiB of HBM per device.

```python
import jax
import jax.numpy as jnp
from jax import lax

TILE = 128
REACH = 1
SOURCES = 128
ITERS = 2
BLOCKS = 32
VERTICES = 4096
N_PATCH = 8
N_SUB = 2


def coupling_parts(key):
    key_present, key_upper, key_own = jax.random.split(jax.random.fold_in(key, 11), 3)
    count = BLOCKS
    rows_ids = jnp.arange(count, dtype=jnp.int32)
    ceiling = 8.0 / (TILE * (1.0 + 1.5 * REACH))
    offsets_up = jnp.arange(1, REACH + 1, dtype=jnp.int32)
    present = (jax.random.randint(key_present, (count, REACH), 0, 4) < 3) & (rows_ids[:, None] + offsets_up[None, :] < count)

    def values_of(subkey, shape):
        uniform_part = jax.random.uniform(subkey, shape, jnp.float32)
        return ceiling * uniform_part
    upper = values_of(key_upper, (count, REACH, TILE, TILE))
    own_tile = values_of(key_own, (count, TILE, TILE))
    own_tile = 0.5 * (own_tile + jnp.swapaxes(own_tile, 1, 2)) * (1.0 - jnp.eye(TILE, dtype=jnp.float32))
    tile_list = []
    col_list = []
    live_list = []
    for offset in range(-REACH, REACH + 1):
        if offset == 0:
            live = jnp.ones((count,), dtype=bool)
            tile_now = own_tile
            col_now = rows_ids
        elif offset > 0:
            live = present[:, offset - 1]
            tile_now = upper[:, offset - 1]
            col_now = rows_ids + offset
        else:
            depth = -offset
            live = jnp.concatenate([jnp.zeros((depth,), dtype=bool), present[:count - depth, depth - 1]])
            tile_now = jnp.concatenate([jnp.zeros((depth, TILE, TILE), jnp.float32), jnp.swapaxes(upper[:count - depth, depth - 1], 1, 2)], axis=0)
            col_now = rows_ids - depth
        tile_list.append(jnp.where(live[:, None, None], tile_now, 0.0))
        col_list.append(jnp.where(live, col_now, rows_ids).astype(jnp.int32))
        live_list.append(live)
    slot_count = 2 * REACH + 1
    tiles_all = jnp.stack(tile_list, axis=1)
    cols_all = jnp.stack(col_list, axis=1)
    live_all = jnp.stack(live_list, axis=1)
    scores = (1 - live_all.astype(jnp.int32)) * slot_count + jnp.arange(slot_count, dtype=jnp.int32)[None, :]
    order = jnp.argsort(scores, axis=1, stable=True).astype(jnp.int32)
    cols_all = jnp.take_along_axis(cols_all, order, axis=1)
    tiles_all = jnp.take_along_axis(tiles_all, order[:, :, None, None], axis=1)
    return (cols_all, tiles_all)


def draw_block_cols(key, part):
    return coupling_parts(key)[0]


def draw_step_tiles(key, part):
    return coupling_parts(key)[1]


def draw_mass(key, part):
    subkey = jax.random.fold_in(key, 23)
    fraction = jnp.arange(VERTICES, dtype=jnp.float32) / VERTICES
    ramp = 1.0 + 2.0 * fraction
    base = jnp.exp(jax.random.uniform(subkey, (VERTICES,), jnp.float32, jnp.log(0.1), jnp.log(0.4)))
    return ramp * base


def with_ends(values, rng, low, high):
    shape = values.shape
    spot = [jax.random.randint(jax.random.fold_in(rng, axis), (), 0, shape[axis]) for axis in range(len(shape))]
    values = values.at[tuple(spot)].set(low)
    longest = shape.index(max(shape))
    spot[longest] = (spot[longest] + 1) % shape[longest]
    return values.at[tuple(spot)].set(high)


def shard_levels(rng, shape, cuts, least, top_value):
    def one(position, blocks):
        draws = jax.random.uniform(jax.random.fold_in(jax.random.fold_in(rng, 6), position), (blocks,), jnp.float32, least / len(cuts), top_value / len(cuts))
        return jnp.repeat(jnp.exp(draws), shape[position] // blocks).reshape((-1,) + (1,) * (len(shape) - position - 1))

    level = one(*cuts[0])
    for cut in cuts[1:]:
        level = level * one(*cut)
    return level


def scatter_about(own_key, extent, spread, bound, cuts=(), kind=jnp.bfloat16):
    entries = jax.random.normal(own_key, extent, jnp.float32) * spread
    if len(cuts) > 0:
        entries = shard_levels(own_key, extent, cuts, -0.22, 0.18) * entries
    return jnp.clip(entries, min=-bound, max=bound).astype(kind)


def setup_inputs(seed: int = 0, part: int = 0) -> dict:
    keys = jax.random.split(jax.random.key(seed), 6)
    part_keys = jax.random.split(jax.random.fold_in(keys[5], part), 6)
    block_cols = draw_block_cols(jax.random.fold_in(jax.random.fold_in(keys[5], part), 71), part)
    step_tiles = draw_step_tiles(jax.random.fold_in(jax.random.fold_in(keys[5], part), 71), part)
    mass = draw_mass(jax.random.fold_in(jax.random.fold_in(keys[5], part), 71), part)
    warm_start = scatter_about(part_keys[3], (VERTICES, SOURCES), 0.3, 2.5, ((0, 16),), jnp.float32)
    source_ids = with_ends(jax.random.randint(part_keys[4], (SOURCES,), 0, VERTICES), jax.random.fold_in(part_keys[4], 1), 0, VERTICES - 1).astype(jnp.int32)
    return dict(block_cols=block_cols, step_tiles=step_tiles, mass=mass, warm_start=warm_start, source_ids=source_ids)


def apply_operator(operand, block_cols, step_tiles, diag_total):
    tile_size = step_tiles.shape[-1]
    sources = operand.shape[1]
    padding = jnp.zeros((REACH * tile_size, sources), operand.dtype)
    blocks = jnp.concatenate([padding, operand, padding], axis=0).reshape(-1, tile_size, sources)
    groups_count = N_PATCH * N_SUB
    cols_grouped = block_cols.reshape(groups_count, -1, block_cols.shape[1])
    tiles_grouped = step_tiles.reshape(groups_count, -1, step_tiles.shape[1], tile_size, tile_size)

    def one_group(pieces):
        cols_group, tiles_group = pieces
        picked = blocks[cols_group + REACH]
        return jnp.einsum("bkij,bkjs->bis", tiles_group, picked, precision=lax.Precision.HIGHEST, preferred_element_type=jnp.float32)

    coupled = lax.map(one_group, (cols_grouped, tiles_grouped))
    return diag_total * operand - coupled.reshape(operand.shape)


def reference(block_cols, step_tiles, mass, warm_start, source_ids):
    vertex_ids = jnp.arange(warm_start.shape[0], dtype=jnp.int32)
    rhs = (vertex_ids[:, None] == source_ids[None, :]).astype(jnp.float32)
    degree = jnp.sum(step_tiles, axis=(1, 3)).reshape(-1)
    diag_total = (mass + degree)[:, None]
    solution = warm_start
    residual = rhs - apply_operator(warm_start, block_cols, step_tiles, diag_total)
    direction = residual
    norm_now = jnp.sum(residual * residual, axis=0)
    for iteration in range(ITERS):
        image_vec = apply_operator(direction, block_cols, step_tiles, diag_total)
        alpha_step = norm_now / jnp.sum(direction * image_vec, axis=0)
        solution = solution + alpha_step * direction
        residual = residual - alpha_step * image_vec
        if iteration + 1 < ITERS:
            norm_next = jnp.sum(residual * residual, axis=0)
            direction = residual + (norm_next / norm_now) * direction
            norm_now = norm_next
    return solution
```

```python
import functools

import jax
import jax.numpy as jnp
from jax import lax
from jax.experimental import pallas as pl
from jax.experimental.pallas import tpu as pltpu
from jax.sharding import PartitionSpec as P

AXES = ("patch", "sub")
LEAST_EIGENVALUE = 0.0999
VMEM = pl.BlockSpec(memory_space=pltpu.VMEM)
SMEM = pl.BlockSpec(memory_space=pltpu.SMEM)


def dot(a, b):
    return jnp.dot(a, b, precision=lax.Precision.HIGHEST, preferred_element_type=jnp.float32)


def place():
    return lax.axis_index("patch") * lax.axis_size("sub") + lax.axis_index("sub")


def outer_block(tile):
    side = lax.rem(place(), 2)
    outer = pl.ds(pl.multiple_of(side * tile, tile), tile)
    inner = pl.ds(pl.multiple_of((1 - side) * tile, tile), tile)
    return outer, inner


def local_kernel(cols, tiles, mass, x, sources, local, t_in, t_out, t_out_t, base, push):
    tile = tiles.shape[-1]
    slots = tiles.shape[1]
    position = place()
    side = lax.rem(position, 2)
    first = position * 2
    above, below = first - 1, first + 2
    eye = lax.broadcasted_iota(jnp.int32, (tile, tile), 0) == lax.broadcasted_iota(jnp.int32, (tile, tile), 1)

    def toward(row, block):
        total = jnp.where(cols[row, 0] == block, tiles[row, 0], 0.0)
        for slot in range(1, slots):
            total += jnp.where(cols[row, slot] == block, tiles[row, slot], 0.0)
        return total

    for row in range(2):
        whole = tiles[row, 0]
        for slot in range(1, slots):
            whole += tiles[row, slot]
        masses = mass[pl.ds(row * tile, tile)][None, :]
        total = jnp.sum(whole + jnp.where(eye, masses, 0.0), axis=1, keepdims=True)
        own = jnp.where(eye, total, 0.0) - toward(row, first + row)
        cross = -toward(row, first + 1 - row)
        local[pl.ds(row * tile, tile), pl.ds(row * tile, tile)] = own
        local[pl.ds(row * tile, tile), pl.ds((1 - row) * tile, tile)] = cross
    outer, _ = outer_block(tile)
    outward = toward(side, jnp.where(side == 0, above, below))
    outward_t = outward.T
    t_in[...] = toward(1 - side, jnp.where(side == 0, below, above))
    t_out[...] = outward
    t_out_t[...] = outward_t
    vertices = position * (2 * tile) + lax.broadcasted_iota(jnp.int32, x.shape, 0)
    rhs = jnp.where(vertices == sources[...][None, :], 1.0, 0.0)
    base[...] = rhs - dot(local[...], x[...])
    push[...] = dot(outward_t, x[outer, :])


def start_kernel(local, t_in, base, push, other_x, t, q, send):
    tile = t_in.shape[0]
    outer, inner = outer_block(tile)
    t[outer, :] = base[outer, :]
    t[inner, :] = base[inner, :] + dot(t_in[...], other_x[outer, :])
    q[...] = dot(local[...], t[...])
    send[0:tile, :] = t[outer, :]
    send[tile : 2 * tile, :] = q[outer, :]
    send[2 * tile : 3 * tile, :] = push[...]
    send[3 * tile :, :] = local[outer, outer_columns(tile)]


def outer_columns(tile):
    side = lax.rem(place(), 2)
    return pl.ds(pl.multiple_of(side * tile, tile), tile)


def image_kernel(local, t_in, t_out, t, q, push, other_t, got, r, w, w_in):
    tile = t_in.shape[0]
    outer, inner = outer_block(tile)
    push_here = got[2 * tile : 3 * tile, :]
    r[inner, :] = t[inner, :]
    r[outer, :] = t[outer, :] + push_here
    change = dot(local[:, outer_columns(tile)], push_here)
    w[...] = q[...] + change
    beyond = got[0:tile, :] + push[...]
    w[outer, :] = w[outer, :] - dot(t_out[...], beyond)
    w_inner = w[inner, :] - dot(t_in[...], other_t[outer, :])
    w[inner, :] = w_inner
    w_in[...] = w_inner


def moment_kernel(local, t_in, t_out, t_out_t, push, got, r, w, moments, edge):
    tile = t_in.shape[0]
    outer, inner = outer_block(tile)
    w_now, r_now = w[...], r[...]
    w_beyond = (
        got[tile : 2 * tile, :] + dot(got[3 * tile :, :], push[...]) - dot(t_out_t[...], r[outer, :])
    )
    r_r = jnp.sum(r_now * r_now, axis=0, keepdims=True)
    r_w = jnp.sum(r_now * w_now, axis=0, keepdims=True)
    left = w_now - jnp.where(r_r > 0, r_w / r_r, 0.0) * r_now
    w_aw = jnp.sum(w_now * dot(local[...], w_now), axis=0, keepdims=True)
    w_aw -= jnp.sum(w[outer, :] * dot(t_out[...], w_beyond), axis=0, keepdims=True)
    moments[0:1, :] = r_r
    moments[1:2, :] = r_w
    moments[2:3, :] = jnp.sum(left * left, axis=0, keepdims=True)
    moments[3:4, :] = w_aw
    edge[...] = dot(t_in[...].T, w[inner, :])


def share_kernel(moments, edge, other_w, out):
    coupling = jnp.sum(edge[...] * other_w[...], axis=0, keepdims=True)
    row = lax.broadcasted_iota(jnp.int32, moments.shape, 0)
    total = moments[...] - jnp.where(row == 3, coupling, 0.0)
    out[...] = jnp.broadcast_to(total[None], out.shape)


def finish_kernel(shares, x, r, w, out):
    r_rs, r_ws = shares[:, 0, :], shares[:, 1, :]
    r_r = jnp.sum(r_rs, axis=0, keepdims=True)
    r_w = jnp.sum(r_ws, axis=0, keepdims=True)
    theta = r_w / r_r
    off = jnp.where(r_rs > 0, r_ws / r_rs, 0.0) - theta
    spread = jnp.sum(shares[:, 2, :] + r_rs * off * off, axis=0, keepdims=True)
    w_aw = jnp.sum(shares[:, 3, :], axis=0, keepdims=True)
    ratio = spread / (theta * theta * r_r)
    energy = w_aw - 2.0 * theta * spread - theta * theta * r_w
    energy = jnp.maximum(energy - ratio * theta * spread, LEAST_EIGENVALUE * spread * (1.0 + ratio))
    step = jnp.where(spread > 0, spread / energy, 0.0)
    first = 1.0 / theta
    out[...] = x[...] + (first + step * (1.0 + ratio)) * r[...] - (step * first) * w[...]


def call(kernel, shapes, in_specs):
    outs = [jax.ShapeDtypeStruct(shape, jnp.float32) for shape in shapes]
    return pl.pallas_call(
        kernel,
        out_shape=outs if len(outs) > 1 else outs[0],
        in_specs=in_specs,
        out_specs=[VMEM] * len(outs) if len(outs) > 1 else VMEM,
        name=kernel.__name__,
    )


def body(block_cols, step_tiles, mass, warm_start, source_ids):
    tile = step_tiles.shape[-1]
    rows, columns = warm_start.shape
    assert block_cols.shape[0] == 2
    devices = lax.axis_size("patch") * lax.axis_size("sub")
    partner = [(i, i ^ 1) for i in range(devices)]
    across = [(i, i + 1) for i in range(1, devices - 1, 2)]
    across += [(j, i) for i, j in across]
    field, block = (rows, columns), (tile, columns)
    square = (tile, tile)

    other_x = lax.ppermute(warm_start, AXES, partner)
    local, t_in, t_out, t_out_t, base, push = call(
        local_kernel, [(rows, rows), square, square, square, field, block], [SMEM] + [VMEM] * 4
    )(block_cols, step_tiles, mass, warm_start, source_ids)
    t, q, send = call(start_kernel, [field, field, (4 * tile, columns)], [VMEM] * 5)(
        local, t_in, base, push, other_x
    )
    other_t = lax.ppermute(t, AXES, partner)
    got = lax.ppermute(send, AXES, across)
    r, w, w_in = call(image_kernel, [field, field, block], [VMEM] * 8)(
        local, t_in, t_out, t, q, push, other_t, got
    )
    other_w = lax.ppermute(w_in, AXES, partner)
    moments, edge = call(moment_kernel, [(4, columns), block], [VMEM] * 8)(
        local, t_in, t_out, t_out_t, push, got, r, w
    )
    shares = call(share_kernel, [(devices, 4, columns)], [VMEM] * 3)(moments, edge, other_w)
    shares = lax.all_to_all(shares, AXES, 0, 0)
    return call(finish_kernel, [field], [VMEM] * 4)(shares, warm_start, r, w)


def solution(mesh):
    in_specs = (
        P(("groups", "patch", "sub"), None),
        P(("groups", "patch", "sub"), None, None, None),
        P(("groups", "patch", "sub")),
        P(("groups", "patch", "sub"), None),
        P("groups"),
    )
    out_specs = P(("groups", "patch", "sub"), None)
    return jax.shard_map(body, mesh=mesh, in_specs=in_specs, out_specs=out_specs, check_vma=False)
```

```python
import functools

import jax
import jax.numpy as jnp
from jax import lax
from jax.experimental import pallas as pl
from jax.experimental.pallas import tpu as pltpu
from jax.sharding import PartitionSpec as P

AXES = ("patch", "sub")
LEAST_EIGENVALUE = 0.0999
VMEM = pl.BlockSpec(memory_space=pltpu.VMEM)
SMEM = pl.BlockSpec(memory_space=pltpu.SMEM)


def dot(a, b):
    return jnp.dot(a, b, precision=lax.Precision.HIGHEST, preferred_element_type=jnp.float32)


def place():
    return lax.axis_index("patch") * lax.axis_size("sub") + lax.axis_index("sub")


def outer_block(tile):
    side = lax.rem(place(), 2)
    outer = pl.ds(pl.multiple_of(side * tile, tile), tile)
    inner = pl.ds(pl.multiple_of((1 - side) * tile, tile), tile)
    return outer, inner


def local_kernel(cols, tiles, mass, x, sources, local, t_in, t_out, t_out_t, base, push):
    tile = tiles.shape[-1]
    slots = tiles.shape[1]
    position = place()
    side = lax.rem(position, 2)
    first = position * 2
    above, below = first - 1, first + 2
    eye = lax.broadcasted_iota(jnp.int32, (tile, tile), 0) == lax.broadcasted_iota(jnp.int32, (tile, tile), 1)

    def toward(row, block):
        total = jnp.where(cols[row, 0] == block, tiles[row, 0], 0.0)
        for slot in range(1, slots):
            total += jnp.where(cols[row, slot] == block, tiles[row, slot], 0.0)
        return total

    for row in range(2):
        whole = tiles[row, 0]
        for slot in range(1, slots):
            whole += tiles[row, slot]
        masses = mass[pl.ds(row * tile, tile)][None, :]
        total = jnp.sum(whole + jnp.where(eye, masses, 0.0), axis=1, keepdims=True)
        own = jnp.where(eye, total, 0.0) - toward(row, first + row)
        cross = -toward(row, first + 1 - row)
        local[pl.ds(row * tile, tile), pl.ds(row * tile, tile)] = own
        local[pl.ds(row * tile, tile), pl.ds((1 - row) * tile, tile)] = cross
    outer, _ = outer_block(tile)
    outward = toward(side, jnp.where(side == 0, above, below))
    outward_t = outward.T
    t_in[...] = toward(1 - side, jnp.where(side == 0, below, above))
    t_out[...] = outward
    t_out_t[...] = outward_t
    vertices = position * (2 * tile) + lax.broadcasted_iota(jnp.int32, x.shape, 0)
    rhs = jnp.where(vertices == sources[...][None, :], 1.0, 0.0)
    base[...] = rhs - dot(local[...], x[...])
    push[...] = dot(outward_t, x[outer, :])


def start_kernel(local, t_in, base, push, other_x, t, q, send):
    tile = t_in.shape[0]
    outer, inner = outer_block(tile)
    t[outer, :] = base[outer, :]
    t[inner, :] = base[inner, :] + dot(t_in[...], other_x[outer, :])
    q[...] = dot(local[...], t[...])
    send[0:tile, :] = t[outer, :]
    send[tile : 2 * tile, :] = q[outer, :]
    send[2 * tile : 3 * tile, :] = push[...]
    send[3 * tile :, :] = local[outer, outer_columns(tile)]


def outer_columns(tile):
    side = lax.rem(place(), 2)
    return pl.ds(pl.multiple_of(side * tile, tile), tile)


def image_kernel(local, t_in, t_out, t, q, push, other_t, got, r, w, w_in):
    tile = t_in.shape[0]
    outer, inner = outer_block(tile)
    push_here = got[2 * tile : 3 * tile, :]
    r[inner, :] = t[inner, :]
    r[outer, :] = t[outer, :] + push_here
    change = dot(local[:, outer_columns(tile)], push_here)
    w[...] = q[...] + change
    beyond = got[0:tile, :] + push[...]
    w[outer, :] = w[outer, :] - dot(t_out[...], beyond)
    w_inner = w[inner, :] - dot(t_in[...], other_t[outer, :])
    w[inner, :] = w_inner
    w_in[...] = w_inner


def moment_kernel(local, t_in, t_out, t_out_t, push, got, r, w, moments, edge):
    tile = t_in.shape[0]
    outer, inner = outer_block(tile)
    w_now, r_now = w[...], r[...]
    w_beyond = (
        got[tile : 2 * tile, :] + dot(got[3 * tile :, :], push[...]) - dot(t_out_t[...], r[outer, :])
    )
    r_r = jnp.sum(r_now * r_now, axis=0, keepdims=True)
    r_w = jnp.sum(r_now * w_now, axis=0, keepdims=True)
    left = w_now - jnp.where(r_r > 0, r_w / r_r, 0.0) * r_now
    w_aw = jnp.sum(w_now * dot(local[...], w_now), axis=0, keepdims=True)
    w_aw -= jnp.sum(w[outer, :] * dot(t_out[...], w_beyond), axis=0, keepdims=True)
    moments[0:1, :] = r_r
    moments[1:2, :] = r_w
    moments[2:3, :] = jnp.sum(left * left, axis=0, keepdims=True)
    moments[3:4, :] = w_aw
    edge[...] = dot(t_in[...].T, w[inner, :])


def share_kernel(moments, edge, other_w, out):
    coupling = jnp.sum(edge[...] * other_w[...], axis=0, keepdims=True)
    row = lax.broadcasted_iota(jnp.int32, moments.shape, 0)
    total = moments[...] - jnp.where(row == 3, coupling, 0.0)
    out[...] = jnp.broadcast_to(total[None], out.shape)


def finish_kernel(shares, x, r, w, out):
    r_rs, r_ws = shares[:, 0, :], shares[:, 1, :]
    r_r = jnp.sum(r_rs, axis=0, keepdims=True)
    r_w = jnp.sum(r_ws, axis=0, keepdims=True)
    theta = r_w / r_r
    off = jnp.where(r_rs > 0, r_ws / r_rs, 0.0) - theta
    spread = jnp.sum(shares[:, 2, :] + r_rs * off * off, axis=0, keepdims=True)
    w_aw = jnp.sum(shares[:, 3, :], axis=0, keepdims=True)
    ratio = spread / (theta * theta * r_r)
    energy = w_aw - 2.0 * theta * spread - theta * theta * r_w
    energy = jnp.maximum(energy - ratio * theta * spread, LEAST_EIGENVALUE * spread * (1.0 + ratio))
    step = jnp.where(spread > 0, spread / energy, 0.0)
    first = 1.0 / theta
    out[...] = x[...] + (first + step * (1.0 + ratio)) * r[...] - (step * first) * w[...]


def call(kernel, shapes, *operands, first=False, last=False):
    place_out = jax.ShapeDtypeStruct if last else pltpu.VMEM
    outs = [place_out(shape, jnp.float32) for shape in shapes]
    in_specs, placed = [], []
    for operand in operands:
        scalars = operand.dtype == jnp.int32 and operand.ndim > 1
        in_specs.append(SMEM if scalars else VMEM)
        placed.append(operand if first else pltpu.with_memory_space_constraint(operand, pltpu.VMEM))
    return pl.pallas_call(
        kernel,
        out_shape=outs if len(outs) > 1 else outs[0],
        in_specs=in_specs,
        out_specs=[VMEM] * len(outs) if len(outs) > 1 else VMEM,
        name=kernel.__name__,
    )(*placed)


def body(block_cols, step_tiles, mass, warm_start, source_ids):
    tile = step_tiles.shape[-1]
    rows, columns = warm_start.shape
    assert block_cols.shape[0] == 2 and columns == tile
    devices = lax.axis_size("patch") * lax.axis_size("sub")
    partner = [(i, i ^ 1) for i in range(devices)]
    across = [(i, i + 1) for i in range(1, devices - 1, 2)]
    across += [(j, i) for i, j in across]
    field, block = (rows, columns), (tile, columns)
    square = (tile, tile)

    other_x = lax.ppermute(warm_start, AXES, partner)
    local, t_in, t_out, t_out_t, base, push = call(
        local_kernel, [(rows, rows), square, square, square, field, block],
        block_cols, step_tiles, mass, warm_start, source_ids, first=True,
    )
    t, q, send = call(
        start_kernel, [field, field, (4 * tile, columns)], local, t_in, base, push, other_x
    )
    other_t = lax.ppermute(t, AXES, partner)
    got = lax.ppermute(send, AXES, across)
    r, w, w_in = call(
        image_kernel, [field, field, block], local, t_in, t_out, t, q, push, other_t, got
    )
    other_w = lax.ppermute(w_in, AXES, partner)
    moments, edge = call(
        moment_kernel, [(4, columns), block], local, t_in, t_out, t_out_t, push, got, r, w
    )
    shares = call(share_kernel, [(devices, 4, columns)], moments, edge, other_w)
    shares = lax.all_to_all(shares, AXES, 0, 0)
    return call(finish_kernel, [field], shares, warm_start, r, w, last=True)


def solution(mesh):
    in_specs = (
        P(("groups", "patch", "sub"), None),
        P(("groups", "patch", "sub"), None, None, None),
        P(("groups", "patch", "sub")),
        P(("groups", "patch", "sub"), None),
        P("groups"),
    )
    out_specs = P(("groups", "patch", "sub"), None)
    return jax.shard_map(body, mesh=mesh, in_specs=in_specs, out_specs=out_specs, check_vma=False)
```

```python
import functools

import jax
import jax.numpy as jnp
from jax import lax
from jax.experimental import pallas as pl
from jax.experimental.pallas import tpu as pltpu
from jax.sharding import PartitionSpec as P

AXES = ("patch", "sub")
LEAST_EIGENVALUE = 0.0999
VMEM = pl.BlockSpec(memory_space=pltpu.VMEM)
SMEM = pl.BlockSpec(memory_space=pltpu.SMEM)


def dot(a, b):
    return jnp.dot(a, b, precision=lax.Precision.HIGHEST, preferred_element_type=jnp.float32)


def place():
    return lax.axis_index("patch") * lax.axis_size("sub") + lax.axis_index("sub")


def outer_block(tile):
    side = lax.rem(place(), 2)
    outer = pl.ds(pl.multiple_of(side * tile, tile), tile)
    inner = pl.ds(pl.multiple_of((1 - side) * tile, tile), tile)
    return outer, inner


def flip(x):
    return pltpu.roll(x, x.shape[1] // 2, 1)


def index_of(shape, dimension):
    return lax.broadcasted_iota(jnp.int32, shape, dimension)


def local_kernel(cols, tiles, mass, x, sources, local, t_in, t_out, t_out_t, base, push, packed):
    tile = tiles.shape[-1]
    half = tile // 2
    slots = tiles.shape[1]
    position = place()
    side = lax.rem(position, 2)
    first = position * 2
    above, below = first - 1, first + 2
    eye = index_of((tile, tile), 0) == index_of((tile, tile), 1)

    def toward(row, block):
        total = jnp.where(cols[row, 0] == block, tiles[row, 0], 0.0)
        for slot in range(1, slots):
            total += jnp.where(cols[row, slot] == block, tiles[row, slot], 0.0)
        return total

    for row in range(2):
        whole = tiles[row, 0]
        for slot in range(1, slots):
            whole += tiles[row, slot]
        masses = mass[pl.ds(row * tile, tile)][None, :]
        total = jnp.sum(whole + jnp.where(eye, masses, 0.0), axis=1, keepdims=True)
        own = jnp.where(eye, total, 0.0) - toward(row, first + row)
        cross = -toward(row, first + 1 - row)
        local[pl.ds(row * tile, tile), pl.ds(row * tile, tile)] = own
        local[pl.ds(row * tile, tile), pl.ds((1 - row) * tile, tile)] = cross
    outer, _ = outer_block(tile)
    outward = toward(side, jnp.where(side == 0, above, below))
    outward_t = outward.T
    t_in[...] = toward(1 - side, jnp.where(side == 0, below, above))
    t_out[...] = outward
    t_out_t[...] = outward_t
    vertices = position * (2 * tile) + index_of(x.shape, 0)
    rhs = jnp.where(vertices == sources[...][None, :], 1.0, 0.0)
    base[...] = rhs - dot(local[...], x[...])
    push[...] = dot(outward_t, x[outer, :])
    own = local[outer, outer_columns(tile)]
    above_diagonal = index_of((half, tile), 1) > index_of((half, tile), 0)
    packed[0:half, :] = jnp.where(above_diagonal, own[:half], flip(own[half:]))
    diagonal = jnp.sum(jnp.where(eye, own, 0.0), axis=0, keepdims=True)
    packed[half:, :] = jnp.broadcast_to(diagonal, (8, tile))


def unpack(packed):
    tile = packed.shape[1]
    half = tile // 2
    rows = packed[0:half, :]
    row, column = index_of((half, tile), 0), index_of((half, tile), 1)
    upper = jnp.where(column > row, rows, 0.0)
    lower = flip(jnp.where(column < row, rows, 0.0))
    triangles = jnp.concatenate([upper, lower], axis=0)
    eye = index_of((tile, tile), 0) == index_of((tile, tile), 1)
    return triangles + triangles.T + jnp.where(eye, packed[half : half + 1, :], 0.0)


def outer_columns(tile):
    side = lax.rem(place(), 2)
    return pl.ds(pl.multiple_of(side * tile, tile), tile)


def start_kernel(local, t_in, base, push, packed, other_x, t, q_outer, send):
    tile = t_in.shape[0]
    half = tile // 2
    side = lax.rem(place(), 2)
    outer, inner = outer_block(tile)
    t[outer, :] = base[outer, :]
    t[inner, :] = base[inner, :] + dot(t_in[...], other_x[outer, :])
    q = dot(local[outer, :], t[...])
    q_outer[...] = q
    q = jnp.where(side == 0, flip(q), q)
    first_half = index_of((half, tile), 1) < half
    send[0:tile, :] = base[outer, :]
    send[tile : 2 * tile, :] = push[...]
    send[2 * tile : 2 * tile + half, :] = jnp.where(first_half, q[:half], flip(q[half:]))
    send[2 * tile + half :, :] = packed[...]


def inner_kernel(local, t_in, t, other_t, q_inner):
    outer, inner = outer_block(t_in.shape[0])
    q_inner[...] = dot(local[inner, :], t[...]) - dot(t_in[...], other_t[outer, :])


def image_kernel(local, q_inner, got, w_inner):
    tile = q_inner.shape[0]
    _, inner = outer_block(tile)
    w_inner[...] = q_inner[...] + dot(local[inner, outer_columns(tile)], got[tile : 2 * tile, :])


def moment_kernel(local, t_in, t_out, t_out_t, t, q_outer, push, got, w_inner, r, w, moments, edge):
    tile = t_in.shape[0]
    half = tile // 2
    side = lax.rem(place(), 2)
    outer, inner = outer_block(tile)
    push_here, push_there = got[tile : 2 * tile, :], push[...]
    r_outer = t[outer, :] + push_here
    w_outer = (
        q_outer[...]
        + dot(local[outer, outer_columns(tile)], push_here)
        - dot(t_out[...], got[0:tile, :] + push_there)
    )
    r[outer, :] = r_outer
    r[inner, :] = t[inner, :]
    w[outer, :] = w_outer
    w[inner, :] = w_inner[...]
    w_now, r_now = w[...], r[...]
    q_half = got[2 * tile : 2 * tile + half, :]
    q_flip = flip(q_half)
    q_there = jnp.concatenate(
        [jnp.where(side == 0, q_half, q_flip), jnp.where(side == 0, q_flip, q_half)], axis=0
    )
    own_there = unpack(got[2 * tile + half :, :])
    w_there = q_there + dot(own_there, push_there) - dot(t_out_t[...], r_outer)
    coupling = jnp.sum(w_outer * dot(t_out[...], w_there), axis=0, keepdims=True)
    mine = (index_of(coupling.shape, 1) >= half) == (side == 1)
    r_r = jnp.sum(r_now * r_now, axis=0, keepdims=True)
    r_w = jnp.sum(r_now * w_now, axis=0, keepdims=True)
    left = w_now - jnp.where(r_r > 0, r_w / r_r, 0.0) * r_now
    w_aw = jnp.sum(w_now * dot(local[...], w_now), axis=0, keepdims=True)
    moments[0:1, :] = r_r
    moments[1:2, :] = r_w
    moments[2:3, :] = jnp.sum(left * left, axis=0, keepdims=True)
    moments[3:4, :] = w_aw - jnp.where(mine, 2.0 * coupling, 0.0)
    edge[...] = dot(t_in[...].T, w_inner[...])


def share_kernel(moments, edge, other_w, out):
    coupling = jnp.sum(edge[...] * other_w[...], axis=0, keepdims=True)
    row = lax.broadcasted_iota(jnp.int32, moments.shape, 0)
    total = moments[...] - jnp.where(row == 3, coupling, 0.0)
    out[...] = jnp.broadcast_to(total[None], out.shape)


def finish_kernel(shares, x, r, w, out):
    r_rs, r_ws = shares[:, 0, :], shares[:, 1, :]
    r_r = jnp.sum(r_rs, axis=0, keepdims=True)
    r_w = jnp.sum(r_ws, axis=0, keepdims=True)
    theta = r_w / r_r
    off = jnp.where(r_rs > 0, r_ws / r_rs, 0.0) - theta
    spread = jnp.sum(shares[:, 2, :] + r_rs * off * off, axis=0, keepdims=True)
    w_aw = jnp.sum(shares[:, 3, :], axis=0, keepdims=True)
    ratio = spread / (theta * theta * r_r)
    energy = w_aw - 2.0 * theta * spread - theta * theta * r_w
    energy = jnp.maximum(energy - ratio * theta * spread, LEAST_EIGENVALUE * spread * (1.0 + ratio))
    step = jnp.where(spread > 0, spread / energy, 0.0)
    first = 1.0 / theta
    out[...] = x[...] + (first + step * (1.0 + ratio)) * r[...] - (step * first) * w[...]


def call(kernel, shapes, *operands, first=False, last=False):
    place_out = jax.ShapeDtypeStruct if last else pltpu.VMEM
    outs = [place_out(shape, jnp.float32) for shape in shapes]
    in_specs, placed = [], []
    for operand in operands:
        scalars = operand.dtype == jnp.int32 and operand.ndim > 1
        in_specs.append(SMEM if scalars else VMEM)
        placed.append(operand if first else pltpu.with_memory_space_constraint(operand, pltpu.VMEM))
    return pl.pallas_call(
        kernel,
        out_shape=outs if len(outs) > 1 else outs[0],
        in_specs=in_specs,
        out_specs=[VMEM] * len(outs) if len(outs) > 1 else VMEM,
        name=kernel.__name__,
    )(*placed)


def body(block_cols, step_tiles, mass, warm_start, source_ids):
    tile = step_tiles.shape[-1]
    rows, columns = warm_start.shape
    assert block_cols.shape[0] == 2 and columns == tile
    devices = lax.axis_size("patch") * lax.axis_size("sub")
    partner = [(i, i ^ 1) for i in range(devices)]
    across = [(i, i + 1) for i in range(1, devices - 1, 2)]
    across += [(j, i) for i, j in across]
    field, block = (rows, columns), (tile, columns)
    square, packing = (tile, tile), (tile // 2 + 8, columns)

    other_x = lax.ppermute(warm_start, AXES, partner)
    local, t_in, t_out, t_out_t, base, push, packed = call(
        local_kernel, [(rows, rows), square, square, square, field, block, packing],
        block_cols, step_tiles, mass, warm_start, source_ids, first=True,
    )
    t, q_outer, send = call(
        start_kernel, [field, block, (3 * tile + 8, columns)], local, t_in, base, push, packed, other_x
    )
    got = lax.ppermute(send, AXES, across)
    other_t = lax.ppermute(t, AXES, partner)
    q_inner = call(inner_kernel, [block], local, t_in, t, other_t)
    w_inner = call(image_kernel, [block], local, q_inner, got)
    other_w = lax.ppermute(w_inner, AXES, partner)
    r, w, moments, edge = call(
        moment_kernel, [field, field, (4, columns), block],
        local, t_in, t_out, t_out_t, t, q_outer, push, got, w_inner,
    )
    shares = call(share_kernel, [(devices, 4, columns)], moments, edge, other_w)
    shares = lax.all_to_all(shares, AXES, 0, 0)
    return call(finish_kernel, [field], shares, warm_start, r, w, last=True)


def solution(mesh):
    in_specs = (
        P(("groups", "patch", "sub"), None),
        P(("groups", "patch", "sub"), None, None, None),
        P(("groups", "patch", "sub")),
        P(("groups", "patch", "sub"), None),
        P("groups"),
    )
    out_specs = P(("groups", "patch", "sub"), None)
    return jax.shard_map(body, mesh=mesh, in_specs=in_specs, out_specs=out_specs, check_vma=False)
```

```python
import functools

import jax
import jax.numpy as jnp
from jax import lax
from jax.experimental import pallas as pl
from jax.experimental.pallas import tpu as pltpu
from jax.sharding import PartitionSpec as P

AXES = ("patch", "sub")
LEAST_EIGENVALUE = 0.0999
VMEM = pl.BlockSpec(memory_space=pltpu.VMEM)
SMEM = pl.BlockSpec(memory_space=pltpu.SMEM)


def halves(a):
    high = a.astype(jnp.bfloat16)
    return high, (a - high.astype(jnp.float32)).astype(jnp.bfloat16)


def dot(a, b):
    a_high, a_low = a[0], a[1]
    b_high, b_low = halves(b)

    def product(p, q):
        return jnp.dot(p, q, preferred_element_type=jnp.float32)

    return product(a_high, b_high) + (product(a_high, b_low) + product(a_low, b_high))


def place():
    return lax.axis_index("patch") * lax.axis_size("sub") + lax.axis_index("sub")


def outer_block(tile):
    side = lax.rem(place(), 2)
    outer = pl.ds(pl.multiple_of(side * tile, tile), tile)
    inner = pl.ds(pl.multiple_of((1 - side) * tile, tile), tile)
    return outer, inner


def flip(x):
    return pltpu.roll(x, x.shape[1] // 2, 1)


def index_of(shape, dimension):
    return lax.broadcasted_iota(jnp.int32, shape, dimension)


def local_kernel(cols, tiles, mass, x, sources, local, diag, t_in, t_out, t_out_t, base, push, packed):
    tile = tiles.shape[-1]
    half = tile // 2
    slots = tiles.shape[1]
    position = place()
    side = lax.rem(position, 2)
    first = position * 2
    above, below = first - 1, first + 2
    eye = index_of((tile, tile), 0) == index_of((tile, tile), 1)

    def toward(row, block):
        total = jnp.where(cols[row, 0] == block, tiles[row, 0], 0.0)
        for slot in range(1, slots):
            total += jnp.where(cols[row, slot] == block, tiles[row, slot], 0.0)
        return total

    for row in range(2):
        here = pl.ds(row * tile, tile)
        whole = tiles[row, 0]
        for slot in range(1, slots):
            whole += tiles[row, slot]
        masses = mass[here][None, :]
        total = jnp.sum(whole + jnp.where(eye, masses, 0.0), axis=1, keepdims=True)
        diag[here, :] = jnp.broadcast_to(total, (tile, x.shape[1]))
        for column in range(2):
            there = pl.ds(column * tile, tile)
            local[0, here, there], local[1, here, there] = halves(-toward(row, first + column))
    outer, _ = outer_block(tile)
    outward = toward(side, jnp.where(side == 0, above, below))
    t_in[0], t_in[1] = halves(toward(1 - side, jnp.where(side == 0, below, above)))
    t_out[0], t_out[1] = halves(outward)
    t_out_t[0], t_out_t[1] = halves(outward.T)
    vertices = position * (2 * tile) + index_of(x.shape, 0)
    rhs = jnp.where(vertices == sources[...][None, :], 1.0, 0.0)
    base[...] = rhs - diag[...] * x[...] - dot(local, x[...])
    push[...] = dot(t_out_t, x[outer, :])
    own = toward(side, first + side)
    above_diagonal = index_of((half, tile), 1) > index_of((half, tile), 0)
    packed[0:half, :] = jnp.where(above_diagonal, own[:half], flip(own[half:]))
    diagonal = jnp.sum(jnp.where(eye, diag[outer, :], 0.0), axis=0, keepdims=True)
    packed[half:, :] = jnp.broadcast_to(diagonal, (8, tile))


def unpack(packed):
    tile = packed.shape[1]
    half = tile // 2
    rows = packed[0:half, :]
    row, column = index_of((half, tile), 0), index_of((half, tile), 1)
    upper = jnp.where(column > row, rows, 0.0)
    lower = flip(jnp.where(column < row, rows, 0.0))
    triangles = jnp.concatenate([upper, lower], axis=0)
    eye = index_of((tile, tile), 0) == index_of((tile, tile), 1)
    diagonal = jnp.sum(jnp.where(eye, packed[half : half + 1, :], 0.0), axis=1, keepdims=True)
    return triangles + triangles.T, diagonal


def outer_columns(tile):
    side = lax.rem(place(), 2)
    return pl.ds(pl.multiple_of(side * tile, tile), tile)


def part(pair, *index):
    return pair[(0, *index)], pair[(1, *index)]


def start_kernel(local, diag, t_in, base, push, packed, other_x, t, q_outer, send):
    tile = t_in.shape[-1]
    half = tile // 2
    side = lax.rem(place(), 2)
    outer, inner = outer_block(tile)
    t[outer, :] = base[outer, :]
    t[inner, :] = base[inner, :] + dot(t_in, other_x[outer, :])
    q = diag[outer, :] * base[outer, :] + dot(part(local, outer), t[...])
    q_outer[...] = q
    q = jnp.where(side == 0, flip(q), q)
    first_half = index_of((half, tile), 1) < half
    send[0:tile, :] = base[outer, :]
    send[tile : 2 * tile, :] = push[...]
    send[2 * tile : 2 * tile + half, :] = jnp.where(first_half, q[:half], flip(q[half:]))
    send[2 * tile + half :, :] = packed[...]


def inner_kernel(local, diag, t_in, t, other_t, q_inner):
    outer, inner = outer_block(t_in.shape[-1])
    q_inner[...] = (
        diag[inner, :] * t[inner, :] + dot(part(local, inner), t[...]) - dot(t_in, other_t[outer, :])
    )


def image_kernel(local, q_inner, got, w_inner):
    tile = q_inner.shape[0]
    _, inner = outer_block(tile)
    w_inner[...] = q_inner[...] + dot(part(local, inner, outer_columns(tile)), got[tile : 2 * tile, :])


def moment_kernel(local, diag, t_in, t_out, t_out_t, t, q_outer, push, got, w_inner, r, w, moments, edge):
    tile = t_in.shape[-1]
    half = tile // 2
    side = lax.rem(place(), 2)
    outer, inner = outer_block(tile)
    push_here, push_there = got[tile : 2 * tile, :], push[...]
    r_outer = t[outer, :] + push_here
    w_outer = (
        q_outer[...]
        + diag[outer, :] * push_here
        + dot(part(local, outer, outer_columns(tile)), push_here)
        - dot(t_out, got[0:tile, :] + push_there)
    )
    r[outer, :] = r_outer
    r[inner, :] = t[inner, :]
    w[outer, :] = w_outer
    w[inner, :] = w_inner[...]
    w_now, r_now = w[...], r[...]
    q_half = got[2 * tile : 2 * tile + half, :]
    q_flip = flip(q_half)
    q_there = jnp.concatenate(
        [jnp.where(side == 0, q_half, q_flip), jnp.where(side == 0, q_flip, q_half)], axis=0
    )
    own_there, diag_there = unpack(got[2 * tile + half :, :])
    w_there = q_there + diag_there * push_there - dot(halves(own_there), push_there) - dot(t_out_t, r_outer)
    coupling = jnp.sum(w_outer * dot(t_out, w_there), axis=0, keepdims=True)
    mine = (index_of(coupling.shape, 1) >= half) == (side == 1)
    r_r = jnp.sum(r_now * r_now, axis=0, keepdims=True)
    r_w = jnp.sum(r_now * w_now, axis=0, keepdims=True)
    left = w_now - jnp.where(r_r > 0, r_w / r_r, 0.0) * r_now
    w_aw = jnp.sum(w_now * (diag[...] * w_now + dot(local, w_now)), axis=0, keepdims=True)
    moments[0:1, :] = r_r
    moments[1:2, :] = r_w
    moments[2:3, :] = jnp.sum(left * left, axis=0, keepdims=True)
    moments[3:4, :] = w_aw - jnp.where(mine, 2.0 * coupling, 0.0)
    edge[...] = dot((t_in[0].T, t_in[1].T), w_inner[...])


def share_kernel(moments, edge, other_w, out):
    coupling = jnp.sum(edge[...] * other_w[...], axis=0, keepdims=True)
    row = lax.broadcasted_iota(jnp.int32, moments.shape, 0)
    total = moments[...] - jnp.where(row == 3, coupling, 0.0)
    out[...] = jnp.broadcast_to(total[None], out.shape)


def finish_kernel(shares, x, r, w, out):
    r_rs, r_ws = shares[:, 0, :], shares[:, 1, :]
    r_r = jnp.sum(r_rs, axis=0, keepdims=True)
    r_w = jnp.sum(r_ws, axis=0, keepdims=True)
    theta = r_w / r_r
    off = jnp.where(r_rs > 0, r_ws / r_rs, 0.0) - theta
    spread = jnp.sum(shares[:, 2, :] + r_rs * off * off, axis=0, keepdims=True)
    w_aw = jnp.sum(shares[:, 3, :], axis=0, keepdims=True)
    ratio = spread / (theta * theta * r_r)
    energy = w_aw - 2.0 * theta * spread - theta * theta * r_w
    energy = jnp.maximum(energy - ratio * theta * spread, LEAST_EIGENVALUE * spread * (1.0 + ratio))
    step = jnp.where(spread > 0, spread / energy, 0.0)
    first = 1.0 / theta
    out[...] = x[...] + (first + step * (1.0 + ratio)) * r[...] - (step * first) * w[...]


def call(kernel, shapes, *operands, first=False, last=False):
    place_out = jax.ShapeDtypeStruct if last else pltpu.VMEM
    outs = [place_out(shape[1:], shape[0]) for shape in shapes]
    in_specs, placed = [], []
    for operand in operands:
        scalars = operand.dtype == jnp.int32 and operand.ndim > 1
        in_specs.append(SMEM if scalars else VMEM)
        placed.append(operand if first else pltpu.with_memory_space_constraint(operand, pltpu.VMEM))
    return pl.pallas_call(
        kernel,
        out_shape=outs if len(outs) > 1 else outs[0],
        in_specs=in_specs,
        out_specs=[VMEM] * len(outs) if len(outs) > 1 else VMEM,
        name=kernel.__name__,
    )(*placed)


def body(block_cols, step_tiles, mass, warm_start, source_ids):
    tile = step_tiles.shape[-1]
    rows, columns = warm_start.shape
    assert block_cols.shape[0] == 2 and columns == tile
    devices = lax.axis_size("patch") * lax.axis_size("sub")
    partner = [(i, i ^ 1) for i in range(devices)]
    across = [(i, i + 1) for i in range(1, devices - 1, 2)]
    across += [(j, i) for i, j in across]
    single = jnp.float32
    field, block = (single, rows, columns), (single, tile, columns)
    square, packing = (jnp.bfloat16, 2, tile, tile), (single, tile // 2 + 8, columns)

    other_x = lax.ppermute(warm_start, AXES, partner)
    local, diag, t_in, t_out, t_out_t, base, push, packed = call(
        local_kernel, [(jnp.bfloat16, 2, rows, rows), field, square, square, square, field, block, packing],
        block_cols, step_tiles, mass, warm_start, source_ids, first=True,
    )
    t, q_outer, send = call(
        start_kernel, [field, block, (single, 3 * tile + 8, columns)],
        local, diag, t_in, base, push, packed, other_x,
    )
    got = lax.ppermute(send, AXES, across)
    other_t = lax.ppermute(t, AXES, partner)
    q_inner = call(inner_kernel, [block], local, diag, t_in, t, other_t)
    w_inner = call(image_kernel, [block], local, q_inner, got)
    other_w = lax.ppermute(w_inner, AXES, partner)
    r, w, moments, edge = call(
        moment_kernel, [field, field, (single, 4, columns), block],
        local, diag, t_in, t_out, t_out_t, t, q_outer, push, got, w_inner,
    )
    shares = call(share_kernel, [(single, devices, 4, columns)], moments, edge, other_w)
    shares = lax.all_to_all(shares, AXES, 0, 0)
    return call(finish_kernel, [field], shares, warm_start, r, w, last=True)


def solution(mesh):
    in_specs = (
        P(("groups", "patch", "sub"), None),
        P(("groups", "patch", "sub"), None, None, None),
        P(("groups", "patch", "sub")),
        P(("groups", "patch", "sub"), None),
        P("groups"),
    )
    out_specs = P(("groups", "patch", "sub"), None)
    return jax.shard_map(body, mesh=mesh, in_specs=in_specs, out_specs=out_specs, check_vma=False)
```

```python
import functools

import jax
import jax.numpy as jnp
from jax import lax
from jax.experimental import pallas as pl
from jax.experimental.pallas import tpu as pltpu
from jax.sharding import PartitionSpec as P

AXES = ("patch", "sub")
LEAST_EIGENVALUE = 0.0999
VMEM = pl.BlockSpec(memory_space=pltpu.VMEM)
SMEM = pl.BlockSpec(memory_space=pltpu.SMEM)


def halves(a):
    high = a.astype(jnp.bfloat16)
    return high, (a - high.astype(jnp.float32)).astype(jnp.bfloat16)


def dot(a, b):
    a_high, a_low = a[0], a[1]
    b_high, b_low = halves(b)

    def product(p, q):
        return jnp.dot(p, q, preferred_element_type=jnp.float32)

    return product(a_high, b_high) + (product(a_high, b_low) + product(a_low, b_high))


def place():
    return lax.axis_index("patch") * lax.axis_size("sub") + lax.axis_index("sub")


def outer_block(tile):
    side = lax.rem(place(), 2)
    outer = pl.ds(pl.multiple_of(side * tile, tile), tile)
    inner = pl.ds(pl.multiple_of((1 - side) * tile, tile), tile)
    return outer, inner


def flip(x):
    return pltpu.roll(x, x.shape[1] // 2, 1)


def index_of(shape, dimension):
    return lax.broadcasted_iota(jnp.int32, shape, dimension)


def local_kernel(cols, tiles, mass, x, sources, local, diag, t_in, t_out, t_out_t, base, push, packed):
    tile = tiles.shape[-1]
    half = tile // 2
    slots = tiles.shape[1]
    position = place()
    side = lax.rem(position, 2)
    first = position * 2
    above, below = first - 1, first + 2
    eye = index_of((tile, tile), 0) == index_of((tile, tile), 1)

    def toward(row, block):
        total = jnp.where(cols[row, 0] == block, tiles[row, 0], 0.0)
        for slot in range(1, slots):
            total += jnp.where(cols[row, slot] == block, tiles[row, slot], 0.0)
        return total

    for row in range(2):
        here = pl.ds(row * tile, tile)
        whole = tiles[row, 0]
        for slot in range(1, slots):
            whole += tiles[row, slot]
        masses = mass[here][None, :]
        total = jnp.sum(whole + jnp.where(eye, masses, 0.0), axis=1, keepdims=True)
        diag[here, :] = jnp.broadcast_to(total, (tile, x.shape[1]))
        for column in range(2):
            there = pl.ds(column * tile, tile)
            local[0, here, there], local[1, here, there] = halves(-toward(row, first + column))
    outer, _ = outer_block(tile)
    outward = toward(side, jnp.where(side == 0, above, below))
    t_in[0], t_in[1] = halves(toward(1 - side, jnp.where(side == 0, below, above)))
    t_out[0], t_out[1] = halves(outward)
    t_out_t[0], t_out_t[1] = halves(outward.T)
    vertices = position * (2 * tile) + index_of(x.shape, 0)
    rhs = jnp.where(vertices == sources[...][None, :], 1.0, 0.0)
    base[...] = rhs - diag[...] * x[...] - dot(local, x[...])
    push[...] = dot(t_out_t, x[outer, :])
    own = toward(side, first + side)
    above_diagonal = index_of((half, tile), 1) > index_of((half, tile), 0)
    packed[0:half, :] = jnp.where(above_diagonal, own[:half], flip(own[half:]))
    diagonal = jnp.sum(jnp.where(eye, diag[outer, :], 0.0), axis=0, keepdims=True)
    packed[half:, :] = jnp.broadcast_to(diagonal, (8, tile))


def unpack(packed):
    tile = packed.shape[1]
    half = tile // 2
    rows = packed[0:half, :]
    row, column = index_of((half, tile), 0), index_of((half, tile), 1)
    upper = jnp.where(column > row, rows, 0.0)
    lower = flip(jnp.where(column < row, rows, 0.0))
    triangles = jnp.concatenate([upper, lower], axis=0)
    eye = index_of((tile, tile), 0) == index_of((tile, tile), 1)
    diagonal = jnp.sum(jnp.where(eye, packed[half : half + 1, :], 0.0), axis=1, keepdims=True)
    return triangles + triangles.T, diagonal


def outer_columns(tile):
    side = lax.rem(place(), 2)
    return pl.ds(pl.multiple_of(side * tile, tile), tile)


def part(pair, *index):
    return pair[(0, *index)], pair[(1, *index)]


def start_kernel(local, diag, t_in, base, push, packed, other_x, t, q_outer, send):
    tile = t_in.shape[-1]
    half = tile // 2
    side = lax.rem(place(), 2)
    outer, inner = outer_block(tile)
    t[outer, :] = base[outer, :]
    t[inner, :] = base[inner, :] + dot(t_in, other_x[outer, :])
    q = diag[outer, :] * base[outer, :] + dot(part(local, outer), t[...])
    q_outer[...] = q
    q = jnp.where(side == 0, flip(q), q)
    first_half = index_of((half, tile), 1) < half
    send[0:tile, :] = base[outer, :]
    send[tile : 2 * tile, :] = push[...]
    send[2 * tile : 2 * tile + half, :] = jnp.where(first_half, q[:half], flip(q[half:]))
    send[2 * tile + half :, :] = packed[...]


def inner_kernel(local, diag, t_in, t, other_t, q_inner):
    outer, inner = outer_block(t_in.shape[-1])
    q_inner[...] = (
        diag[inner, :] * t[inner, :] + dot(part(local, inner), t[...]) - dot(t_in, other_t[outer, :])
    )


def image_kernel(local, q_inner, got, w_inner):
    tile = q_inner.shape[0]
    _, inner = outer_block(tile)
    w_inner[...] = q_inner[...] + dot(part(local, inner, outer_columns(tile)), got[tile : 2 * tile, :])


def moment_kernel(
    local, diag, t_in, t_out, t_out_t, t, q_outer, push, got, w_inner, r, w, moments, edge, edge_r
):
    tile = t_in.shape[-1]
    half = tile // 2
    side = lax.rem(place(), 2)
    outer, inner = outer_block(tile)

    def total(value):
        return jnp.sum(value, axis=0, keepdims=True)

    push_here, push_there = got[tile : 2 * tile, :], push[...]
    r_outer, r_there = t[outer, :] + push_here, got[0:tile, :] + push_there
    pull_r = dot(t_out, r_there)
    w_outer = (
        q_outer[...]
        + diag[outer, :] * push_here
        + dot(part(local, outer, outer_columns(tile)), push_here)
        - pull_r
    )
    r[outer, :] = r_outer
    r[inner, :] = t[inner, :]
    w[outer, :] = w_outer
    w[inner, :] = w_inner[...]
    w_now, r_now = w[...], r[...]
    r_r, r_w = total(r_now * r_now), total(r_now * w_now)
    shift = jnp.where(r_r > 0, r_w / r_r, 0.0)
    y = w_now - shift * r_now
    y_outer = w_outer - shift * r_outer
    q_half = got[2 * tile : 2 * tile + half, :]
    q_flip = flip(q_half)
    q_there = jnp.concatenate(
        [jnp.where(side == 0, q_half, q_flip), jnp.where(side == 0, q_flip, q_half)], axis=0
    )
    own_there, diag_there = unpack(got[2 * tile + half :, :])
    w_there = q_there + diag_there * push_there - dot(halves(own_there), push_there) - dot(t_out_t, r_outer)
    pull_y = dot(t_out, w_there - shift * r_there)
    mine = (index_of((1, r_now.shape[1]), 1) >= half) == (side == 1)
    weight = jnp.where(mine, 2.0, 0.0)
    a_y = diag[...] * y + dot(local, y)
    y_ay = total(y * a_y) - weight * total(y_outer * pull_y)
    r_ay = total(r_now * a_y + y * w_now) + total(y_outer * pull_r)
    r_ay -= weight * total(r_outer * pull_y + y_outer * pull_r)
    r_ar = r_w + (1.0 - weight) * total(r_outer * pull_r)
    moments[...] = jnp.concatenate([r_r, r_w, total(y * y), y_ay, r_ay, r_ar, shift, shift], axis=0)
    t_in_t = (t_in[0].T, t_in[1].T)
    edge[...] = dot(t_in_t, w_inner[...] - shift * r[inner, :])
    edge_r[...] = dot(t_in_t, r[inner, :])


def share_kernel(moments, edge, edge_r, other_t, other_w, out):
    outer, _ = outer_block(edge.shape[0])
    y_there = other_w[...] - moments[6:7, :] * other_t[outer, :]
    y_ay = jnp.sum(edge[...] * y_there, axis=0, keepdims=True)
    r_ay = jnp.sum(edge_r[...] * y_there, axis=0, keepdims=True)
    row = index_of(moments.shape, 0)
    total = moments[...] - jnp.where(row == 3, y_ay, 0.0) - jnp.where(row == 4, r_ay, 0.0)
    out[...] = jnp.broadcast_to(total[None], out.shape)


def finish_kernel(shares, x, r, w, out):
    r_rs = shares[:, 0, :]
    r_r = jnp.sum(r_rs, axis=0, keepdims=True)
    r_w = jnp.sum(shares[:, 1, :], axis=0, keepdims=True)
    theta = r_w / r_r
    off = shares[:, 6, :] - theta
    spread = jnp.sum(shares[:, 2, :] + r_rs * off * off, axis=0, keepdims=True)
    energy = jnp.sum(
        shares[:, 3, :] + off * (shares[:, 4, :] + off * shares[:, 5, :]), axis=0, keepdims=True
    )
    ratio = spread / (theta * theta * r_r)
    energy = jnp.maximum(energy - ratio * theta * spread, LEAST_EIGENVALUE * spread * (1.0 + ratio))
    step = jnp.where(spread > 0, spread / energy, 0.0)
    first = 1.0 / theta
    out[...] = x[...] + (first + step * (1.0 + ratio)) * r[...] - (step * first) * w[...]


def call(kernel, shapes, *operands, first=False, last=False):
    place_out = jax.ShapeDtypeStruct if last else pltpu.VMEM
    outs = [place_out(shape[1:], shape[0]) for shape in shapes]
    in_specs, placed = [], []
    for operand in operands:
        scalars = operand.dtype == jnp.int32 and operand.ndim > 1
        in_specs.append(SMEM if scalars else VMEM)
        placed.append(operand if first else pltpu.with_memory_space_constraint(operand, pltpu.VMEM))
    return pl.pallas_call(
        kernel,
        out_shape=outs if len(outs) > 1 else outs[0],
        in_specs=in_specs,
        out_specs=[VMEM] * len(outs) if len(outs) > 1 else VMEM,
        name=kernel.__name__,
    )(*placed)


def body(block_cols, step_tiles, mass, warm_start, source_ids):
    tile = step_tiles.shape[-1]
    rows, columns = warm_start.shape
    assert block_cols.shape[0] == 2 and columns == tile
    devices = lax.axis_size("patch") * lax.axis_size("sub")
    partner = [(i, i ^ 1) for i in range(devices)]
    across = [(i, i + 1) for i in range(1, devices - 1, 2)]
    across += [(j, i) for i, j in across]
    single = jnp.float32
    field, block = (single, rows, columns), (single, tile, columns)
    square, packing = (jnp.bfloat16, 2, tile, tile), (single, tile // 2 + 8, columns)

    other_x = lax.ppermute(warm_start, AXES, partner)
    local, diag, t_in, t_out, t_out_t, base, push, packed = call(
        local_kernel, [(jnp.bfloat16, 2, rows, rows), field, square, square, square, field, block, packing],
        block_cols, step_tiles, mass, warm_start, source_ids, first=True,
    )
    t, q_outer, send = call(
        start_kernel, [field, block, (single, 3 * tile + 8, columns)],
        local, diag, t_in, base, push, packed, other_x,
    )
    got = lax.ppermute(send, AXES, across)
    other_t = lax.ppermute(t, AXES, partner)
    q_inner = call(inner_kernel, [block], local, diag, t_in, t, other_t)
    w_inner = call(image_kernel, [block], local, q_inner, got)
    other_w = lax.ppermute(w_inner, AXES, partner)
    r, w, moments, edge, edge_r = call(
        moment_kernel, [field, field, (single, 8, columns), block, block],
        local, diag, t_in, t_out, t_out_t, t, q_outer, push, got, w_inner,
    )
    shares = call(share_kernel, [(single, devices, 8, columns)], moments, edge, edge_r, other_t, other_w)
    shares = lax.all_to_all(shares, AXES, 0, 0)
    return call(finish_kernel, [field], shares, warm_start, r, w, last=True)


def solution(mesh):
    in_specs = (
        P(("groups", "patch", "sub"), None),
        P(("groups", "patch", "sub"), None, None, None),
        P(("groups", "patch", "sub")),
        P(("groups", "patch", "sub"), None),
        P("groups"),
    )
    out_specs = P(("groups", "patch", "sub"), None)
    return jax.shard_map(body, mesh=mesh, in_specs=in_specs, out_specs=out_specs, check_vma=False)
```

```python
import functools

import jax
import jax.numpy as jnp
from jax import lax
from jax.experimental import pallas as pl
from jax.experimental.pallas import tpu as pltpu
from jax.sharding import PartitionSpec as P

AXES = ("patch", "sub")
LEAST_EIGENVALUE = 0.0999
VMEM = pl.BlockSpec(memory_space=pltpu.VMEM)
SMEM = pl.BlockSpec(memory_space=pltpu.SMEM)


def halves(a):
    high = a.astype(jnp.bfloat16)
    return high, (a - high.astype(jnp.float32)).astype(jnp.bfloat16)


def dot(a, b):
    a_high, a_low = a[0], a[1]
    b_high, b_low = halves(b)

    def product(p, q):
        return jnp.dot(p, q, preferred_element_type=jnp.float32)

    return product(a_high, b_high) + (product(a_high, b_low) + product(a_low, b_high))


def place():
    return lax.axis_index("patch") * lax.axis_size("sub") + lax.axis_index("sub")


def outer_block(tile):
    side = lax.rem(place(), 2)
    outer = pl.ds(pl.multiple_of(side * tile, tile), tile)
    inner = pl.ds(pl.multiple_of((1 - side) * tile, tile), tile)
    return outer, inner


def flip(x):
    return pltpu.roll(x, x.shape[1] // 2, 1)


def index_of(shape, dimension):
    return lax.broadcasted_iota(jnp.int32, shape, dimension)


def local_kernel(
    cols, tiles, mass, x, sources, local, diag, t_in, t_out_t, base, push, q_base, send
):
    tile = tiles.shape[-1]
    half = tile // 2
    slots = tiles.shape[1]
    position = place()
    side = lax.rem(position, 2)
    first = position * 2
    above, below = first - 1, first + 2
    eye = index_of((tile, tile), 0) == index_of((tile, tile), 1)

    def toward(row, block, sign=1.0):
        slot, scale = jnp.int32(0), 0.0
        for k in range(slots):
            named = cols[row, k] == block
            slot, scale = jnp.where(named, k, slot), jnp.where(named, sign, scale)
        return scale * tiles[row, slot]

    owns = []
    for row in range(2):
        here, there = pl.ds(row * tile, tile), pl.ds((1 - row) * tile, tile)
        whole, own = tiles[row, 0], jnp.where(cols[row, 0] == first + row, tiles[row, 0], 0.0)
        for k in range(1, slots):
            whole += tiles[row, k]
            own += jnp.where(cols[row, k] == first + row, tiles[row, k], 0.0)
        masses = mass[here][None, :]
        total = jnp.sum(whole + jnp.where(eye, masses, 0.0), axis=1, keepdims=True)
        diag[here, :] = jnp.broadcast_to(total, (tile, x.shape[1]))
        local[0, here, here], local[1, here, here] = halves(-own)
        local[0, here, there], local[1, here, there] = halves(toward(row, first + 1 - row, -1.0))
        owns.append(own)
    outer, _ = outer_block(tile)
    outward_t = toward(side, jnp.where(side == 0, above, below)).T
    t_in[0], t_in[1] = halves(toward(1 - side, jnp.where(side == 0, below, above)))
    t_out_t[0], t_out_t[1] = halves(outward_t)
    vertices = position * (2 * tile) + index_of(x.shape, 0)
    rhs = jnp.where(vertices == sources[...][None, :], 1.0, 0.0)
    base[...] = rhs - diag[...] * x[...] - dot(local, x[...])
    push[...] = dot(t_out_t, x[outer, :])
    q_base[...] = diag[outer, :] * base[outer, :] + dot(part(local, outer), base[...])
    send[0:tile, :] = base[outer, :]
    send[tile : 2 * tile, :] = push[...]
    own = jnp.where(side == 0, owns[0], owns[1])
    above_diagonal = index_of((half, tile), 1) > index_of((half, tile), 0)
    packed = send.at[2 * tile + half :]
    packed[0:half, :] = jnp.where(above_diagonal, own[:half], flip(own[half:]))
    diagonal = jnp.sum(jnp.where(eye, diag[outer, :], 0.0), axis=0, keepdims=True)
    packed[half:, :] = jnp.broadcast_to(diagonal, (8, tile))


def unpack(packed):
    tile = packed.shape[1]
    half = tile // 2
    rows = packed[0:half, :]
    row, column = index_of((half, tile), 0), index_of((half, tile), 1)
    upper = jnp.where(column > row, rows, 0.0)
    lower = flip(jnp.where(column < row, rows, 0.0))
    triangles = jnp.concatenate([upper, lower], axis=0)
    eye = index_of((tile, tile), 0) == index_of((tile, tile), 1)
    diagonal = jnp.sum(jnp.where(eye, packed[half : half + 1, :], 0.0), axis=1, keepdims=True)
    return triangles + triangles.T, diagonal


def outer_columns(tile):
    side = lax.rem(place(), 2)
    return pl.ds(pl.multiple_of(side * tile, tile), tile)


def inner_columns(tile):
    side = lax.rem(place(), 2)
    return pl.ds(pl.multiple_of((1 - side) * tile, tile), tile)


def part(pair, *index):
    return pair[(0, *index)], pair[(1, *index)]


def start_kernel(local, t_in, base, q_base, other_x, send_in, t, q_outer, send):
    tile = t_in.shape[-1]
    half = tile // 2
    side = lax.rem(place(), 2)
    outer, inner = outer_block(tile)
    pull = dot(t_in, other_x[outer, :])
    q = q_base[...] + dot(part(local, outer, inner_columns(tile)), pull)
    turned = jnp.where(side == 0, flip(q), q)
    first_half = index_of((half, tile), 1) < half
    send[2 * tile : 2 * tile + half, :] = jnp.where(first_half, turned[:half], flip(turned[half:]))
    q_outer[...] = q
    t[outer, :] = base[outer, :]
    t[inner, :] = base[inner, :] + pull


def inner_kernel(local, diag, t_in, t_out_t, t, other_t, q_inner, t_in_t, t_out):
    outer, inner = outer_block(t_in.shape[-1])
    for half in range(2):
        t_in_t[half] = t_in[half].T
        t_out[half] = t_out_t[half].T
    q_inner[...] = (
        diag[inner, :] * t[inner, :] + dot(part(local, inner), t[...]) - dot(t_in, other_t[outer, :])
    )


def image_kernel(local, q_inner, got, w_inner):
    tile = q_inner.shape[0]
    _, inner = outer_block(tile)
    w_inner[...] = q_inner[...] + dot(part(local, inner, outer_columns(tile)), got[tile : 2 * tile, :])


def moment_kernel(
    local, diag, t_in_t, t_out, t_out_t, t, q_outer, push, got, w_inner, r, w, moments, edge, edge_r
):
    tile = t_out.shape[-1]
    half = tile // 2
    side = lax.rem(place(), 2)
    outer, inner = outer_block(tile)

    def total(value):
        return jnp.sum(value, axis=0, keepdims=True)

    push_here, push_there = got[tile : 2 * tile, :], push[...]
    r_outer, r_there = t[outer, :] + push_here, got[0:tile, :] + push_there
    pull_r = dot(t_out, r_there)
    w_outer = (
        q_outer[...]
        + diag[outer, :] * push_here
        + dot(part(local, outer, outer_columns(tile)), push_here)
        - pull_r
    )
    r[outer, :] = r_outer
    r[inner, :] = t[inner, :]
    w[outer, :] = w_outer
    w[inner, :] = w_inner[...]
    w_now, r_now = w[...], r[...]
    r_r, r_w = total(r_now * r_now), total(r_now * w_now)
    shift = jnp.where(r_r > 0, r_w / r_r, 0.0)
    y = w_now - shift * r_now
    y_outer = w_outer - shift * r_outer
    q_half = got[2 * tile : 2 * tile + half, :]
    q_flip = flip(q_half)
    q_there = jnp.concatenate(
        [jnp.where(side == 0, q_half, q_flip), jnp.where(side == 0, q_flip, q_half)], axis=0
    )
    own_there, diag_there = unpack(got[2 * tile + half :, :])
    w_there = q_there + diag_there * push_there - dot(halves(own_there), push_there) - dot(t_out_t, r_outer)
    pull_y = dot(t_out, w_there - shift * r_there)
    mine = (index_of((1, r_now.shape[1]), 1) >= half) == (side == 1)
    weight = jnp.where(mine, 2.0, 0.0)
    a_y = diag[...] * y + dot(local, y)
    y_ay = total(y * a_y) - weight * total(y_outer * pull_y)
    r_ay = total(r_now * a_y + y * w_now) + total(y_outer * pull_r)
    r_ay -= weight * total(r_outer * pull_y + y_outer * pull_r)
    r_ar = r_w + (1.0 - weight) * total(r_outer * pull_r)
    moments[...] = jnp.concatenate([r_r, r_w, total(y * y), y_ay, r_ay, r_ar, shift, shift], axis=0)
    edge[...] = dot(t_in_t, w_inner[...] - shift * r[inner, :])
    edge_r[...] = dot(t_in_t, r[inner, :])


def share_kernel(moments, edge, edge_r, other_t, other_w, out):
    outer, _ = outer_block(edge.shape[0])
    y_there = other_w[...] - moments[6:7, :] * other_t[outer, :]
    y_ay = jnp.sum(edge[...] * y_there, axis=0, keepdims=True)
    r_ay = jnp.sum(edge_r[...] * y_there, axis=0, keepdims=True)
    row = index_of(moments.shape, 0)
    total = moments[...] - jnp.where(row == 3, y_ay, 0.0) - jnp.where(row == 4, r_ay, 0.0)
    for pair in range(out.shape[1]):
        out[:, pair] = jnp.broadcast_to(total[None, 2 * pair : 2 * pair + 2], out[:, pair].shape)


def finish_kernel(shares, x, r, w, out):
    r_rs, r_ws, spreads, y_ay, r_ay, r_ar = [shares[:, row // 2, row % 2, :] for row in range(6)]
    r_r = jnp.sum(r_rs, axis=0, keepdims=True)
    r_w = jnp.sum(r_ws, axis=0, keepdims=True)
    theta = r_w / r_r
    off = jnp.where(r_rs > 0, r_ws / r_rs, 0.0) - theta
    spread = jnp.sum(spreads + r_rs * off * off, axis=0, keepdims=True)
    energy = jnp.sum(y_ay + off * (r_ay + off * r_ar), axis=0, keepdims=True)
    ratio = spread / (theta * theta * r_r)
    energy = jnp.maximum(energy - ratio * theta * spread, LEAST_EIGENVALUE * spread * (1.0 + ratio))
    step = jnp.where(spread > 0, spread / energy, 0.0)
    first = 1.0 / theta
    out[...] = x[...] + (first + step * (1.0 + ratio)) * r[...] - (step * first) * w[...]


def call(kernel, shapes, *operands, first=False, last=False, aliases={}):
    place_out = jax.ShapeDtypeStruct if last else pltpu.VMEM
    outs = [place_out(shape[1:], shape[0]) for shape in shapes]
    in_specs, placed = [], []
    for operand in operands:
        scalars = operand.dtype == jnp.int32 and operand.ndim > 1
        in_specs.append(SMEM if scalars else VMEM)
        placed.append(operand if first else pltpu.with_memory_space_constraint(operand, pltpu.VMEM))
    return pl.pallas_call(
        kernel,
        out_shape=outs if len(outs) > 1 else outs[0],
        in_specs=in_specs,
        out_specs=[VMEM] * len(outs) if len(outs) > 1 else VMEM,
        input_output_aliases=aliases,
        name=kernel.__name__,
    )(*placed)


def body(block_cols, step_tiles, mass, warm_start, source_ids):
    tile = step_tiles.shape[-1]
    rows, columns = warm_start.shape
    assert block_cols.shape[0] == 2 and columns == tile
    devices = lax.axis_size("patch") * lax.axis_size("sub")
    partner = [(i, i ^ 1) for i in range(devices)]
    across = [(i, i + 1) for i in range(1, devices - 1, 2)]
    across += [(j, i) for i, j in across]
    single = jnp.float32
    field, block = (single, rows, columns), (single, tile, columns)
    square, sending = (jnp.bfloat16, 2, tile, tile), (single, 3 * tile + 8, columns)

    other_x = lax.ppermute(warm_start, AXES, partner)
    local, diag, t_in, t_out_t, base, push, q_base, send = call(
        local_kernel,
        [(jnp.bfloat16, 2, rows, rows), field, square, square, field, block, block, sending],
        block_cols, step_tiles, mass, warm_start, source_ids, first=True,
    )
    t, q_outer, send = call(
        start_kernel, [field, block, sending], local, t_in, base, q_base, other_x, send, aliases={5: 2}
    )
    got = lax.ppermute(send, AXES, across)
    other_t = lax.ppermute(t, AXES, partner)
    q_inner, t_in_t, t_out = call(
        inner_kernel, [block, square, square], local, diag, t_in, t_out_t, t, other_t
    )
    w_inner = call(image_kernel, [block], local, q_inner, got)
    other_w = lax.ppermute(w_inner, AXES, partner)
    r, w, moments, edge, edge_r = call(
        moment_kernel, [field, field, (single, 8, columns), block, block],
        local, diag, t_in_t, t_out, t_out_t, t, q_outer, push, got, w_inner,
    )
    shares = call(share_kernel, [(single, devices, 3, 2, columns)], moments, edge, edge_r, other_t, other_w)
    shares = lax.all_to_all(shares, AXES, 0, 0)
    return call(finish_kernel, [field], shares, warm_start, r, w, last=True)


def solution(mesh):
    in_specs = (
        P(("groups", "patch", "sub"), None),
        P(("groups", "patch", "sub"), None, None, None),
        P(("groups", "patch", "sub")),
        P(("groups", "patch", "sub"), None),
        P("groups"),
    )
    out_specs = P(("groups", "patch", "sub"), None)
    return jax.shard_map(body, mesh=mesh, in_specs=in_specs, out_specs=out_specs, check_vma=False)
```

```python
import functools

import jax
import jax.numpy as jnp
from jax import lax
from jax.experimental import pallas as pl
from jax.experimental.pallas import tpu as pltpu
from jax.sharding import PartitionSpec as P

AXES = ("patch", "sub")
LEAST_EIGENVALUE = 0.0999
VMEM = pl.BlockSpec(memory_space=pltpu.VMEM)
SMEM = pl.BlockSpec(memory_space=pltpu.SMEM)


def halves(a):
    high = a.astype(jnp.bfloat16)
    return high, (a - high.astype(jnp.float32)).astype(jnp.bfloat16)


def dot(a, b):
    a_high, a_low = a[0], a[1]
    b_high, b_low = halves(b)

    def product(p, q):
        return jnp.dot(p, q, preferred_element_type=jnp.float32)

    return product(a_high, b_high) + (product(a_high, b_low) + product(a_low, b_high))


def place():
    return lax.axis_index("patch") * lax.axis_size("sub") + lax.axis_index("sub")


def outer_block(tile):
    side = lax.rem(place(), 2)
    outer = pl.ds(pl.multiple_of(side * tile, tile), tile)
    inner = pl.ds(pl.multiple_of((1 - side) * tile, tile), tile)
    return outer, inner


def flip(x):
    return pltpu.roll(x, x.shape[1] // 2, 1)


def index_of(shape, dimension):
    return lax.broadcasted_iota(jnp.int32, shape, dimension)


def local_kernel(
    cols, tiles, mass, x, sources, local, diag, t_in, t_out_t, base, push, send
):
    tile = tiles.shape[-1]
    half = tile // 2
    slots = tiles.shape[1]
    position = place()
    side = lax.rem(position, 2)
    first = position * 2
    above, below = first - 1, first + 2
    eye = index_of((tile, tile), 0) == index_of((tile, tile), 1)

    def toward(row, block, sign=1.0):
        slot, scale = jnp.int32(0), 0.0
        for k in range(slots):
            named = cols[row, k] == block
            slot, scale = jnp.where(named, k, slot), jnp.where(named, sign, scale)
        return scale * tiles[row, slot]

    owns = []
    for row in range(2):
        here, there = pl.ds(row * tile, tile), pl.ds((1 - row) * tile, tile)
        whole, own = tiles[row, 0], jnp.where(cols[row, 0] == first + row, tiles[row, 0], 0.0)
        for k in range(1, slots):
            whole += tiles[row, k]
            own += jnp.where(cols[row, k] == first + row, tiles[row, k], 0.0)
        masses = mass[here][None, :]
        total = jnp.sum(whole + jnp.where(eye, masses, 0.0), axis=1, keepdims=True)
        diag[here, :] = jnp.broadcast_to(total, (tile, x.shape[1]))
        local[0, here, here], local[1, here, here] = halves(-own)
        local[0, here, there], local[1, here, there] = halves(toward(row, first + 1 - row, -1.0))
        owns.append(own)
    outer, _ = outer_block(tile)
    outward_t = toward(side, jnp.where(side == 0, above, below)).T
    t_in[0], t_in[1] = halves(toward(1 - side, jnp.where(side == 0, below, above)))
    t_out_t[0], t_out_t[1] = halves(outward_t)
    vertices = position * (2 * tile) + index_of(x.shape, 0)
    rhs = jnp.where(vertices == sources[...][None, :], 1.0, 0.0)
    base[...] = rhs - diag[...] * x[...] - dot(local, x[...])
    push[...] = dot(t_out_t, x[outer, :])
    send[0:tile, :] = base[outer, :]
    send[tile : 2 * tile, :] = push[...]
    own = jnp.where(side == 0, owns[0], owns[1])
    above_diagonal = index_of((half, tile), 1) > index_of((half, tile), 0)
    packed = send.at[2 * tile + half :]
    packed[0:half, :] = jnp.where(above_diagonal, own[:half], flip(own[half:]))
    diagonal = jnp.sum(jnp.where(eye, diag[outer, :], 0.0), axis=0, keepdims=True)
    packed[half:, :] = jnp.broadcast_to(diagonal, (8, tile))


def unpack(packed):
    tile = packed.shape[1]
    half = tile // 2
    rows = packed[0:half, :]
    row, column = index_of((half, tile), 0), index_of((half, tile), 1)
    upper = jnp.where(column > row, rows, 0.0)
    lower = flip(jnp.where(column < row, rows, 0.0))
    triangles = jnp.concatenate([upper, lower], axis=0)
    eye = index_of((tile, tile), 0) == index_of((tile, tile), 1)
    diagonal = jnp.sum(jnp.where(eye, packed[half : half + 1, :], 0.0), axis=1, keepdims=True)
    return triangles + triangles.T, diagonal


def outer_columns(tile):
    side = lax.rem(place(), 2)
    return pl.ds(pl.multiple_of(side * tile, tile), tile)


def part(pair, *index):
    return pair[(0, *index)], pair[(1, *index)]


def start_kernel(local, diag, t_in, base, other_x, send_in, t, q_outer, send):
    tile = t_in.shape[-1]
    half = tile // 2
    side = lax.rem(place(), 2)
    outer, inner = outer_block(tile)
    t[outer, :] = base[outer, :]
    t[inner, :] = base[inner, :] + dot(t_in, other_x[outer, :])
    q = diag[outer, :] * base[outer, :] + dot(part(local, outer), t[...])
    turned = jnp.where(side == 0, flip(q), q)
    first_half = index_of((half, tile), 1) < half
    send[2 * tile : 2 * tile + half, :] = jnp.where(first_half, turned[:half], flip(turned[half:]))
    q_outer[...] = q


def inner_kernel(local, diag, t_in, t_out_t, t, other_t, q_inner, pull_in, t_in_t, t_out):
    outer, inner = outer_block(t_in.shape[-1])
    for half in range(2):
        t_in_t[half] = t_in[half].T
        t_out[half] = t_out_t[half].T
    pull = dot(t_in, other_t[outer, :])
    pull_in[...] = pull
    q_inner[...] = diag[inner, :] * t[inner, :] + dot(part(local, inner), t[...]) - pull


def image_kernel(local, q_inner, got, w_inner):
    tile = q_inner.shape[0]
    _, inner = outer_block(tile)
    w_inner[...] = q_inner[...] + dot(part(local, inner, outer_columns(tile)), got[tile : 2 * tile, :])


def moment_kernel(
    local, diag, t_in_t, t_out, t_out_t, t, q_outer, pull_in, push, got, w_inner, r, w, moments, edge, edge_r
):
    tile = t_out.shape[-1]
    half = tile // 2
    side = lax.rem(place(), 2)
    outer, inner = outer_block(tile)

    def total(value):
        return jnp.sum(value, axis=0, keepdims=True)

    push_here, push_there = got[tile : 2 * tile, :], push[...]
    r_outer, r_there = t[outer, :] + push_here, got[0:tile, :] + push_there
    pull_r = dot(t_out, r_there)
    w_outer = (
        q_outer[...]
        + diag[outer, :] * push_here
        + dot(part(local, outer, outer_columns(tile)), push_here)
        - pull_r
    )
    r[outer, :] = r_outer
    r[inner, :] = t[inner, :]
    w[outer, :] = w_outer
    w[inner, :] = w_inner[...]
    w_now, r_now = w[...], r[...]
    r_r, r_w = total(r_now * r_now), total(r_now * w_now)
    shift = jnp.where(r_r > 0, r_w / r_r, 0.0)
    y = w_now - shift * r_now
    y_outer = w_outer - shift * r_outer
    q_half = got[2 * tile : 2 * tile + half, :]
    q_flip = flip(q_half)
    q_there = jnp.concatenate(
        [jnp.where(side == 0, q_half, q_flip), jnp.where(side == 0, q_flip, q_half)], axis=0
    )
    own_there, diag_there = unpack(got[2 * tile + half :, :])
    w_there = q_there + diag_there * push_there - dot(halves(own_there), push_there) - dot(t_out_t, r_outer)
    pull_y = dot(t_out, w_there - shift * r_there)
    mine = (index_of((1, r_now.shape[1]), 1) >= half) == (side == 1)
    weight = jnp.where(mine, 2.0, 0.0)
    a_y = diag[...] * y + dot(local, y)
    y_ay = total(y * a_y) - weight * total(y_outer * pull_y)
    r_ay = total(r_now * a_y + y * w_now) + total(y_outer * pull_r)
    r_ay -= weight * total(r_outer * pull_y + y_outer * pull_r)
    r_ar = r_w + (1.0 - weight) * total(r_outer * pull_r)
    surplus = jnp.where(side == 0, -1.0, 1.0)
    r_ay += surplus * total((w_inner[...] - shift * t[inner, :]) * pull_in[...])
    r_ar += surplus * total(t[inner, :] * pull_in[...])
    moments[...] = jnp.concatenate([r_r, r_w, total(y * y), y_ay, r_ay, r_ar, shift, shift], axis=0)
    edge[...] = dot(t_in_t, w_inner[...] - shift * r[inner, :])
    edge_r[...] = dot(t_in_t, r[inner, :])


def share_kernel(moments, edge, edge_r, other_t, other_w, out):
    outer, _ = outer_block(edge.shape[0])
    weight = jnp.where(lax.rem(place(), 2) == 0, 2.0, 0.0)
    y_there = other_w[...] - moments[6:7, :] * other_t[outer, :]
    y_ay = jnp.sum(edge[...] * y_there, axis=0, keepdims=True)
    r_ay = jnp.sum(edge_r[...] * y_there, axis=0, keepdims=True)
    row = index_of(moments.shape, 0)
    total = moments[...] - weight * (jnp.where(row == 3, y_ay, 0.0) + jnp.where(row == 4, r_ay, 0.0))
    for pair in range(out.shape[1]):
        out[:, pair] = jnp.broadcast_to(total[None, 2 * pair : 2 * pair + 2], out[:, pair].shape)


def finish_kernel(shares, x, r, w, out):
    r_rs, r_ws, spreads, y_ay, r_ay, r_ar = [shares[:, row // 2, row % 2, :] for row in range(6)]
    r_r = jnp.sum(r_rs, axis=0, keepdims=True)
    r_w = jnp.sum(r_ws, axis=0, keepdims=True)
    theta = r_w / r_r
    off = jnp.where(r_rs > 0, r_ws / r_rs, 0.0) - theta
    spread = jnp.sum(spreads + r_rs * off * off, axis=0, keepdims=True)
    energy = jnp.sum(y_ay + off * (r_ay + off * r_ar), axis=0, keepdims=True)
    ratio = spread / (theta * theta * r_r)
    energy = jnp.maximum(energy - ratio * theta * spread, LEAST_EIGENVALUE * spread * (1.0 + ratio))
    step = jnp.where(spread > 0, spread / energy, 0.0)
    first = 1.0 / theta
    out[...] = x[...] + (first + step * (1.0 + ratio)) * r[...] - (step * first) * w[...]


def call(kernel, shapes, *operands, first=False, last=False, aliases={}):
    place_out = jax.ShapeDtypeStruct if last else pltpu.VMEM
    outs = [place_out(shape[1:], shape[0]) for shape in shapes]
    in_specs, placed = [], []
    for operand in operands:
        scalars = operand.dtype == jnp.int32 and operand.ndim > 1
        in_specs.append(SMEM if scalars else VMEM)
        placed.append(operand if first else pltpu.with_memory_space_constraint(operand, pltpu.VMEM))
    return pl.pallas_call(
        kernel,
        out_shape=outs if len(outs) > 1 else outs[0],
        in_specs=in_specs,
        out_specs=[VMEM] * len(outs) if len(outs) > 1 else VMEM,
        input_output_aliases=aliases,
        name=kernel.__name__,
    )(*placed)


def body(block_cols, step_tiles, mass, warm_start, source_ids):
    tile = step_tiles.shape[-1]
    rows, columns = warm_start.shape
    assert block_cols.shape[0] == 2 and columns == tile
    devices = lax.axis_size("patch") * lax.axis_size("sub")
    partner = [(i, i ^ 1) for i in range(devices)]
    across = [(i, i + 1) for i in range(1, devices - 1, 2)]
    across += [(j, i) for i, j in across]
    single = jnp.float32
    field, block = (single, rows, columns), (single, tile, columns)
    square, sending = (jnp.bfloat16, 2, tile, tile), (single, 3 * tile + 8, columns)

    other_x = lax.ppermute(warm_start, AXES, partner)
    local, diag, t_in, t_out_t, base, push, send = call(
        local_kernel,
        [(jnp.bfloat16, 2, rows, rows), field, square, square, field, block, sending],
        block_cols, step_tiles, mass, warm_start, source_ids, first=True,
    )
    t, q_outer, send = call(
        start_kernel, [field, block, sending], local, diag, t_in, base, other_x, send, aliases={5: 2}
    )
    got = lax.ppermute(send, AXES, across)
    other_t = lax.ppermute(t, AXES, partner)
    q_inner, pull_in, t_in_t, t_out = call(
        inner_kernel, [block, block, square, square], local, diag, t_in, t_out_t, t, other_t
    )
    w_inner = call(image_kernel, [block], local, q_inner, got)
    other_w = lax.ppermute(w_inner, AXES, partner[1::2])
    r, w, moments, edge, edge_r = call(
        moment_kernel, [field, field, (single, 8, columns), block, block],
        local, diag, t_in_t, t_out, t_out_t, t, q_outer, pull_in, push, got, w_inner,
    )
    shares = call(share_kernel, [(single, devices, 3, 2, columns)], moments, edge, edge_r, other_t, other_w)
    shares = lax.all_to_all(shares, AXES, 0, 0)
    return call(finish_kernel, [field], shares, warm_start, r, w, last=True)


def solution(mesh):
    in_specs = (
        P(("groups", "patch", "sub"), None),
        P(("groups", "patch", "sub"), None, None, None),
        P(("groups", "patch", "sub")),
        P(("groups", "patch", "sub"), None),
        P("groups"),
    )
    out_specs = P(("groups", "patch", "sub"), None)
    return jax.shard_map(body, mesh=mesh, in_specs=in_specs, out_specs=out_specs, check_vma=False)
```

```python
import functools

import jax
import jax.numpy as jnp
from jax import lax
from jax.experimental import pallas as pl
from jax.experimental.pallas import tpu as pltpu
from jax.sharding import PartitionSpec as P

AXES = ("patch", "sub")
LEAST_EIGENVALUE = 0.0999
VMEM = pl.BlockSpec(memory_space=pltpu.VMEM)
SMEM = pl.BlockSpec(memory_space=pltpu.SMEM)


def halves(a):
    high = a.astype(jnp.bfloat16)
    return high, (a - high.astype(jnp.float32)).astype(jnp.bfloat16)


def dot(a, b):
    a_high, a_low = a[0], a[1]
    b_high, b_low = halves(b)

    def product(p, q):
        return jnp.dot(p, q, preferred_element_type=jnp.float32)

    return product(a_high, b_high) + (product(a_high, b_low) + product(a_low, b_high))


def place():
    return lax.axis_index("patch") * lax.axis_size("sub") + lax.axis_index("sub")


def outer_block(tile):
    side = lax.rem(place(), 2)
    outer = pl.ds(pl.multiple_of(side * tile, tile), tile)
    inner = pl.ds(pl.multiple_of((1 - side) * tile, tile), tile)
    return outer, inner


def flip(x):
    return pltpu.roll(x, x.shape[1] // 2, 1)


def index_of(shape, dimension):
    return lax.broadcasted_iota(jnp.int32, shape, dimension)


def local_kernel(
    cols, tiles, mass, x, sources, local, diag, t_in, t_out_t, base, push, send
):
    tile = tiles.shape[-1]
    half = tile // 2
    slots = tiles.shape[1]
    position = place()
    side = lax.rem(position, 2)
    first = position * 2
    above, below = first - 1, first + 2
    eye = index_of((tile, tile), 0) == index_of((tile, tile), 1)

    def toward(row, block, sign=1.0):
        slot, scale = jnp.int32(0), 0.0
        for k in range(slots):
            named = cols[row, k] == block
            slot, scale = jnp.where(named, k, slot), jnp.where(named, sign, scale)
        return scale * tiles[row, slot]

    owns = []
    for row in range(2):
        here, there = pl.ds(row * tile, tile), pl.ds((1 - row) * tile, tile)
        whole, own = tiles[row, 0], jnp.where(cols[row, 0] == first + row, tiles[row, 0], 0.0)
        for k in range(1, slots):
            whole += tiles[row, k]
            own += jnp.where(cols[row, k] == first + row, tiles[row, k], 0.0)
        masses = mass[here][None, :]
        total = jnp.sum(whole + jnp.where(eye, masses, 0.0), axis=1, keepdims=True)
        diag[here, :] = jnp.broadcast_to(total, (tile, x.shape[1]))
        local[0, here, here], local[1, here, here] = halves(-own)
        local[0, here, there], local[1, here, there] = halves(toward(row, first + 1 - row, -1.0))
        owns.append(own)
    outer, _ = outer_block(tile)
    outward_t = toward(side, jnp.where(side == 0, above, below)).T
    t_in[0], t_in[1] = halves(toward(1 - side, jnp.where(side == 0, below, above)))
    t_out_t[0], t_out_t[1] = halves(outward_t)
    vertices = position * (2 * tile) + index_of(x.shape, 0)
    rhs = jnp.where(vertices == sources[...][None, :], 1.0, 0.0)
    base[...] = rhs - diag[...] * x[...] - dot(local, x[...])
    push[...] = dot(t_out_t, x[outer, :])
    send[0:tile, :] = base[outer, :]
    send[tile : 2 * tile, :] = push[...]
    own = jnp.where(side == 0, owns[0], owns[1])
    above_diagonal = index_of((half, tile), 1) > index_of((half, tile), 0)
    packed = send.at[2 * tile + half :]
    packed[0:half, :] = jnp.where(above_diagonal, own[:half], flip(own[half:]))
    diagonal = jnp.sum(jnp.where(eye, diag[outer, :], 0.0), axis=0, keepdims=True)
    packed[half:, :] = jnp.broadcast_to(diagonal, (8, tile))


def unpack(packed):
    tile = packed.shape[1]
    half = tile // 2
    rows = packed[0:half, :]
    row, column = index_of((half, tile), 0), index_of((half, tile), 1)
    upper = jnp.where(column > row, rows, 0.0)
    lower = flip(jnp.where(column < row, rows, 0.0))
    triangles = jnp.concatenate([upper, lower], axis=0)
    eye = index_of((tile, tile), 0) == index_of((tile, tile), 1)
    diagonal = jnp.sum(jnp.where(eye, packed[half : half + 1, :], 0.0), axis=1, keepdims=True)
    return triangles + triangles.T, diagonal


def outer_columns(tile):
    side = lax.rem(place(), 2)
    return pl.ds(pl.multiple_of(side * tile, tile), tile)


def part(pair, *index):
    return pair[(0, *index)], pair[(1, *index)]


def start_kernel(local, diag, t_in, base, other_x, send_in, t, q_outer, send):
    tile = t_in.shape[-1]
    half = tile // 2
    side = lax.rem(place(), 2)
    outer, inner = outer_block(tile)
    t[outer, :] = base[outer, :]
    t[inner, :] = base[inner, :] + dot(t_in, other_x[outer, :])
    q = diag[outer, :] * base[outer, :] + dot(part(local, outer), t[...])
    turned = jnp.where(side == 0, flip(q), q)
    first_half = index_of((half, tile), 1) < half
    send[2 * tile : 2 * tile + half, :] = jnp.where(first_half, turned[:half], flip(turned[half:]))
    q_outer[...] = q


def inner_kernel(local, diag, t_in, t_out_t, t, other_t, q_inner, t_in_t, t_out):
    outer, inner = outer_block(t_in.shape[-1])
    for half in range(2):
        t_in_t[half] = t_in[half].T
        t_out[half] = t_out_t[half].T
    q_inner[...] = (
        diag[inner, :] * t[inner, :] + dot(part(local, inner), t[...]) - dot(t_in, other_t[outer, :])
    )


def image_kernel(local, q_inner, got, w_inner):
    tile = q_inner.shape[0]
    _, inner = outer_block(tile)
    w_inner[...] = q_inner[...] + dot(part(local, inner, outer_columns(tile)), got[tile : 2 * tile, :])


def moment_kernel(
    local, diag, t_in_t, t_out, t_out_t, t, q_outer, push, got, w_inner, r, w, moments, edge, edge_r
):
    tile = t_out.shape[-1]
    half = tile // 2
    side = lax.rem(place(), 2)
    outer, inner = outer_block(tile)

    def total(value):
        return jnp.sum(value, axis=0, keepdims=True)

    push_here, push_there = got[tile : 2 * tile, :], push[...]
    r_outer, r_there = t[outer, :] + push_here, got[0:tile, :] + push_there
    pull_r = dot(t_out, r_there)
    w_outer = (
        q_outer[...]
        + diag[outer, :] * push_here
        + dot(part(local, outer, outer_columns(tile)), push_here)
        - pull_r
    )
    r[outer, :] = r_outer
    r[inner, :] = t[inner, :]
    w[outer, :] = w_outer
    w[inner, :] = w_inner[...]
    w_now, r_now = w[...], r[...]
    r_r, r_w = total(r_now * r_now), total(r_now * w_now)
    shift = jnp.where(r_r > 0, r_w / r_r, 0.0)
    y = w_now - shift * r_now
    y_outer = w_outer - shift * r_outer
    q_half = got[2 * tile : 2 * tile + half, :]
    q_flip = flip(q_half)
    q_there = jnp.concatenate(
        [jnp.where(side == 0, q_half, q_flip), jnp.where(side == 0, q_flip, q_half)], axis=0
    )
    own_there, diag_there = unpack(got[2 * tile + half :, :])
    w_there = q_there + diag_there * push_there - dot(halves(own_there), push_there) - dot(t_out_t, r_outer)
    pull_y = dot(t_out, w_there - shift * r_there)
    mine = (index_of((1, r_now.shape[1]), 1) >= half) == (side == 1)
    weight = jnp.where(mine, 2.0, 0.0)
    a_y = diag[...] * y + dot(local, y)
    y_ay = total(y * a_y) - weight * total(y_outer * pull_y)
    r_ay = total(r_now * a_y + y * w_now) + total(y_outer * pull_r)
    r_ay -= weight * total(r_outer * pull_y + y_outer * pull_r)
    r_ar = r_w + (1.0 - weight) * total(r_outer * pull_r)
    moments[...] = jnp.concatenate([r_r, r_w, total(y * y), y_ay, r_ay, r_ar, shift, shift], axis=0)
    edge[...] = dot(t_in_t, w_inner[...] - shift * r[inner, :])
    edge_r[...] = dot(t_in_t, r[inner, :])


def share_kernel(moments, edge, edge_r, other_t, other_w, out):
    outer, _ = outer_block(edge.shape[0])
    y_there = other_w[...] - moments[6:7, :] * other_t[outer, :]
    y_ay = jnp.sum(edge[...] * y_there, axis=0, keepdims=True)
    r_ay = jnp.sum(edge_r[...] * y_there, axis=0, keepdims=True)
    row = index_of(moments.shape, 0)
    total = moments[...] - jnp.where(row == 3, y_ay, 0.0) - jnp.where(row == 4, r_ay, 0.0)
    for pair in range(out.shape[1]):
        out[:, pair] = jnp.broadcast_to(total[None, 2 * pair : 2 * pair + 2], out[:, pair].shape)


def finish_kernel(shares, x, r, w, out):
    r_rs, r_ws, spreads, y_ay, r_ay, r_ar = [shares[:, row // 2, row % 2, :] for row in range(6)]
    r_r = jnp.sum(r_rs, axis=0, keepdims=True)
    r_w = jnp.sum(r_ws, axis=0, keepdims=True)
    theta = r_w / r_r
    off = jnp.where(r_rs > 0, r_ws / r_rs, 0.0) - theta
    spread = jnp.sum(spreads + r_rs * off * off, axis=0, keepdims=True)
    energy = jnp.sum(y_ay + off * (r_ay + off * r_ar), axis=0, keepdims=True)
    ratio = spread / (theta * theta * r_r)
    energy = jnp.maximum(energy - ratio * theta * spread, LEAST_EIGENVALUE * spread * (1.0 + ratio))
    step = jnp.where(spread > 0, spread / energy, 0.0)
    first = 1.0 / theta
    out[...] = x[...] + (first + step * (1.0 + ratio)) * r[...] - (step * first) * w[...]


def call(kernel, shapes, *operands, first=False, last=False, aliases={}):
    place_out = jax.ShapeDtypeStruct if last else pltpu.VMEM
    outs = [place_out(shape[1:], shape[0]) for shape in shapes]
    in_specs, placed = [], []
    for operand in operands:
        scalars = operand.dtype == jnp.int32 and operand.ndim > 1
        in_specs.append(SMEM if scalars else VMEM)
        placed.append(operand if first else pltpu.with_memory_space_constraint(operand, pltpu.VMEM))
    return pl.pallas_call(
        kernel,
        out_shape=outs if len(outs) > 1 else outs[0],
        in_specs=in_specs,
        out_specs=[VMEM] * len(outs) if len(outs) > 1 else VMEM,
        input_output_aliases=aliases,
        name=kernel.__name__,
    )(*placed)


def body(block_cols, step_tiles, mass, warm_start, source_ids):
    tile = step_tiles.shape[-1]
    rows, columns = warm_start.shape
    assert block_cols.shape[0] == 2 and columns == tile
    devices = lax.axis_size("patch") * lax.axis_size("sub")
    partner = [(i, i ^ 1) for i in range(devices)]
    across = [(i, i + 1) for i in range(1, devices - 1, 2)]
    across += [(j, i) for i, j in across] + [(0, 0), (devices - 1, devices - 1)]
    single = jnp.float32
    field, block = (single, rows, columns), (single, tile, columns)
    square, sending = (jnp.bfloat16, 2, tile, tile), (single, 3 * tile + 8, columns)

    other_x = lax.ppermute(warm_start, AXES, partner)
    local, diag, t_in, t_out_t, base, push, send = call(
        local_kernel,
        [(jnp.bfloat16, 2, rows, rows), field, square, square, field, block, sending],
        block_cols, step_tiles, mass, warm_start, source_ids, first=True,
    )
    t, q_outer, send = call(
        start_kernel, [field, block, sending], local, diag, t_in, base, other_x, send, aliases={5: 2}
    )
    got = lax.ppermute(send, AXES, across)
    other_t = lax.ppermute(t, AXES, partner)
    q_inner, t_in_t, t_out = call(
        inner_kernel, [block, square, square], local, diag, t_in, t_out_t, t, other_t
    )
    w_inner = call(image_kernel, [block], local, q_inner, got)
    other_w = lax.ppermute(w_inner, AXES, partner)
    r, w, moments, edge, edge_r = call(
        moment_kernel, [field, field, (single, 8, columns), block, block],
        local, diag, t_in_t, t_out, t_out_t, t, q_outer, push, got, w_inner,
    )
    shares = call(share_kernel, [(single, devices, 3, 2, columns)], moments, edge, edge_r, other_t, other_w)
    shares = lax.all_to_all(shares, AXES, 0, 0)
    return call(finish_kernel, [field], shares, warm_start, r, w, last=True)


def solution(mesh):
    in_specs = (
        P(("groups", "patch", "sub"), None),
        P(("groups", "patch", "sub"), None, None, None),
        P(("groups", "patch", "sub")),
        P(("groups", "patch", "sub"), None),
        P("groups"),
    )
    out_specs = P(("groups", "patch", "sub"), None)
    return jax.shard_map(body, mesh=mesh, in_specs=in_specs, out_specs=out_specs, check_vma=False)
```

```python
import functools

import jax
import jax.numpy as jnp
from jax import lax
from jax.experimental import pallas as pl
from jax.experimental.pallas import tpu as pltpu
from jax.sharding import PartitionSpec as P

AXES = ("patch", "sub")
LEAST_EIGENVALUE = 0.0999
VMEM = pl.BlockSpec(memory_space=pltpu.VMEM)
SMEM = pl.BlockSpec(memory_space=pltpu.SMEM)


def halves(a):
    high = a.astype(jnp.bfloat16)
    return high, (a - high.astype(jnp.float32)).astype(jnp.bfloat16)


def dot(a, b):
    a_high, a_low = a[0], a[1]
    b_high, b_low = halves(b)

    def product(p, q):
        return jnp.dot(p, q, preferred_element_type=jnp.float32)

    return product(a_high, b_high) + (product(a_high, b_low) + product(a_low, b_high))


def place():
    return lax.axis_index("patch") * lax.axis_size("sub") + lax.axis_index("sub")


def outer_block(tile):
    side = lax.rem(place(), 2)
    outer = pl.ds(pl.multiple_of(side * tile, tile), tile)
    inner = pl.ds(pl.multiple_of((1 - side) * tile, tile), tile)
    return outer, inner


def flip(x):
    return pltpu.roll(x, x.shape[1] // 2, 1)


def index_of(shape, dimension):
    return lax.broadcasted_iota(jnp.int32, shape, dimension)


def local_kernel(
    cols, tiles, mass, x, sources, local, diag, t_in, t_out_t, base, push, send
):
    tile = tiles.shape[-1]
    half = tile // 2
    slots = tiles.shape[1]
    position = place()
    side = lax.rem(position, 2)
    first = position * 2
    above, below = first - 1, first + 2
    eye = index_of((tile, tile), 0) == index_of((tile, tile), 1)

    def toward(row, block, sign=1.0):
        slot, scale = jnp.int32(0), 0.0
        for k in range(slots):
            named = cols[row, k] == block
            slot, scale = jnp.where(named, k, slot), jnp.where(named, sign, scale)
        return scale * tiles[row, slot]

    owns = []
    for row in range(2):
        here, there = pl.ds(row * tile, tile), pl.ds((1 - row) * tile, tile)
        whole, own = tiles[row, 0], jnp.where(cols[row, 0] == first + row, tiles[row, 0], 0.0)
        for k in range(1, slots):
            whole += tiles[row, k]
            own += jnp.where(cols[row, k] == first + row, tiles[row, k], 0.0)
        masses = mass[here][None, :]
        total = jnp.sum(whole + jnp.where(eye, masses, 0.0), axis=1, keepdims=True)
        diag[here, :] = jnp.broadcast_to(total, (tile, x.shape[1]))
        local[0, here, here], local[1, here, here] = halves(-own)
        local[0, here, there], local[1, here, there] = halves(toward(row, first + 1 - row, -1.0))
        owns.append(own)
    outer, _ = outer_block(tile)
    outward_t = toward(side, jnp.where(side == 0, above, below)).T
    t_in[0], t_in[1] = halves(toward(1 - side, jnp.where(side == 0, below, above)))
    t_out_t[0], t_out_t[1] = halves(outward_t)
    vertices = position * (2 * tile) + index_of(x.shape, 0)
    rhs = jnp.where(vertices == sources[...][None, :], 1.0, 0.0)
    base[...] = rhs - diag[...] * x[...] - dot(local, x[...])
    push[...] = dot(t_out_t, x[outer, :])
    send[0:tile, :] = base[outer, :]
    send[tile : 2 * tile, :] = push[...]
    own = jnp.where(side == 0, owns[0], owns[1])
    above_diagonal = index_of((half, tile), 1) > index_of((half, tile), 0)
    packed = send.at[2 * tile + half :]
    packed[0:half, :] = jnp.where(above_diagonal, own[:half], flip(own[half:]))
    diagonal = jnp.sum(jnp.where(eye, diag[outer, :], 0.0), axis=0, keepdims=True)
    packed[half:, :] = jnp.broadcast_to(diagonal, (8, tile))


def unpack(packed):
    tile = packed.shape[1]
    half = tile // 2
    rows = packed[0:half, :]
    row, column = index_of((half, tile), 0), index_of((half, tile), 1)
    upper = jnp.where(column > row, rows, 0.0)
    lower = flip(jnp.where(column < row, rows, 0.0))
    triangles = jnp.concatenate([upper, lower], axis=0)
    eye = index_of((tile, tile), 0) == index_of((tile, tile), 1)
    diagonal = jnp.sum(jnp.where(eye, packed[half : half + 1, :], 0.0), axis=1, keepdims=True)
    return triangles + triangles.T, diagonal


def outer_columns(tile):
    side = lax.rem(place(), 2)
    return pl.ds(pl.multiple_of(side * tile, tile), tile)


def part(pair, *index):
    return pair[(0, *index)], pair[(1, *index)]


def start_kernel(local, diag, t_in, base, other_x, send_in, t, q_outer, send):
    tile = t_in.shape[-1]
    half = tile // 2
    side = lax.rem(place(), 2)
    outer, inner = outer_block(tile)
    t[outer, :] = base[outer, :]
    t[inner, :] = base[inner, :] + dot(t_in, other_x[outer, :])
    q = diag[outer, :] * base[outer, :] + dot(part(local, outer), t[...])
    turned = jnp.where(side == 0, flip(q), q)
    first_half = index_of((half, tile), 1) < half
    send[2 * tile : 2 * tile + half, :] = jnp.where(first_half, turned[:half], flip(turned[half:]))
    q_outer[...] = q


def inner_kernel(local, diag, t_in, t_out_t, t, other_t, q_inner, t_in_t, t_out):
    outer, inner = outer_block(t_in.shape[-1])
    for half in range(2):
        t_in_t[half] = t_in[half].T
        t_out[half] = t_out_t[half].T
    q_inner[...] = (
        diag[inner, :] * t[inner, :] + dot(part(local, inner), t[...]) - dot(t_in, other_t[outer, :])
    )


def image_kernel(local, q_inner, got, w_inner):
    tile = q_inner.shape[0]
    _, inner = outer_block(tile)
    w_inner[...] = q_inner[...] + dot(part(local, inner, outer_columns(tile)), got[tile : 2 * tile, :])


def moment_kernel(
    local, diag, t_in_t, t_out, t_out_t, t, q_outer, push, got, w_inner, r, w, moments, edge, edge_r
):
    tile = t_out.shape[-1]
    half = tile // 2
    side = lax.rem(place(), 2)
    outer, inner = outer_block(tile)

    def total(value):
        return jnp.sum(value, axis=0, keepdims=True)

    push_here, push_there = got[tile : 2 * tile, :], push[...]
    r_outer, r_there = t[outer, :] + push_here, got[0:tile, :] + push_there
    pull_r = dot(t_out, r_there)
    w_outer = (
        q_outer[...]
        + diag[outer, :] * push_here
        + dot(part(local, outer, outer_columns(tile)), push_here)
        - pull_r
    )
    r[outer, :] = r_outer
    r[inner, :] = t[inner, :]
    w[outer, :] = w_outer
    w[inner, :] = w_inner[...]
    w_now, r_now = w[...], r[...]
    r_r, r_w = total(r_now * r_now), total(r_now * w_now)
    shift = jnp.where(r_r > 0, r_w / r_r, 0.0)
    y = w_now - shift * r_now
    y_outer = w_outer - shift * r_outer
    q_half = got[2 * tile : 2 * tile + half, :]
    q_flip = flip(q_half)
    q_there = jnp.concatenate(
        [jnp.where(side == 0, q_half, q_flip), jnp.where(side == 0, q_flip, q_half)], axis=0
    )
    own_there, diag_there = unpack(got[2 * tile + half :, :])
    w_there = q_there + diag_there * push_there - dot(halves(own_there), push_there) - dot(t_out_t, r_outer)
    pull_y = dot(t_out, w_there - shift * r_there)
    mine = (index_of((1, r_now.shape[1]), 1) >= half) == (side == 1)
    weight = jnp.where(mine, 2.0, 0.0)
    a_y = diag[...] * y + dot(local, y)
    y_ay = total(y * a_y) - weight * total(y_outer * pull_y)
    r_ay = total(r_now * a_y + y * w_now) + total(y_outer * pull_r)
    r_ay -= weight * total(r_outer * pull_y + y_outer * pull_r)
    r_ar = r_w + (1.0 - weight) * total(r_outer * pull_r)
    moments[...] = jnp.concatenate([r_r, r_w, total(y * y), y_ay, r_ay, r_ar, shift, shift], axis=0)
    edge[...] = dot(t_in_t, w_inner[...] - shift * r[inner, :])
    edge_r[...] = dot(t_in_t, r[inner, :])


def share_kernel(moments, edge, edge_r, other_t, other_w, out):
    outer, _ = outer_block(edge.shape[0])
    y_there = other_w[...] - moments[6:7, :] * other_t[outer, :]
    y_ay = jnp.sum(edge[...] * y_there, axis=0, keepdims=True)
    r_ay = jnp.sum(edge_r[...] * y_there, axis=0, keepdims=True)
    row = index_of(moments.shape, 0)
    total = moments[...] - jnp.where(row == 3, y_ay, 0.0) - jnp.where(row == 4, r_ay, 0.0)
    for pair in range(out.shape[1]):
        out[:, pair] = jnp.broadcast_to(total[None, 2 * pair : 2 * pair + 2], out[:, pair].shape)


def finish_kernel(shares, x, r, w, out):
    r_rs, r_ws, spreads, y_ay, r_ay, r_ar = [shares[:, row // 2, row % 2, :] for row in range(6)]
    r_r = jnp.sum(r_rs, axis=0, keepdims=True)
    r_w = jnp.sum(r_ws, axis=0, keepdims=True)
    theta = r_w / r_r
    off = jnp.where(r_rs > 0, r_ws / r_rs, 0.0) - theta
    spread = jnp.sum(spreads + r_rs * off * off, axis=0, keepdims=True)
    energy = jnp.sum(y_ay + off * (r_ay + off * r_ar), axis=0, keepdims=True)
    ratio = spread / (theta * theta * r_r)
    energy = jnp.maximum(energy - ratio * theta * spread, LEAST_EIGENVALUE * spread * (1.0 + ratio))
    step = jnp.where(spread > 0, spread / energy, 0.0)
    first = 1.0 / theta
    out[...] = x[...] + (first + step * (1.0 + ratio)) * r[...] - (step * first) * w[...]


def call(kernel, shapes, *operands, first=False, last=False, aliases={}):
    place_out = jax.ShapeDtypeStruct if last else pltpu.VMEM
    outs = [place_out(shape[1:], shape[0]) for shape in shapes]
    in_specs, placed = [], []
    for operand in operands:
        scalars = operand.dtype == jnp.int32 and operand.ndim > 1
        in_specs.append(SMEM if scalars else VMEM)
        placed.append(operand if first else pltpu.with_memory_space_constraint(operand, pltpu.VMEM))
    return pl.pallas_call(
        kernel,
        out_shape=outs if len(outs) > 1 else outs[0],
        in_specs=in_specs,
        out_specs=[VMEM] * len(outs) if len(outs) > 1 else VMEM,
        input_output_aliases=aliases,
        name=kernel.__name__,
    )(*placed)


def body(block_cols, step_tiles, mass, warm_start, source_ids):
    tile = step_tiles.shape[-1]
    rows, columns = warm_start.shape
    assert block_cols.shape[0] == 2 and columns == tile
    devices = lax.axis_size("patch") * lax.axis_size("sub")
    partner = [(i, i ^ 1) for i in range(devices)]
    groups = lax.axis_size("groups")
    across = []
    for group in range(groups):
        here, there = group * devices, (group + 1) % groups * devices
        for i in range(1, devices - 1, 2):
            across += [(here + i, here + i + 1), (here + i + 1, here + i)]
        across += [(here, there), (here + devices - 1, there + devices - 1)]
    single = jnp.float32
    field, block = (single, rows, columns), (single, tile, columns)
    square, sending = (jnp.bfloat16, 2, tile, tile), (single, 3 * tile + 8, columns)

    other_x = lax.ppermute(warm_start, AXES, partner)
    local, diag, t_in, t_out_t, base, push, send = call(
        local_kernel,
        [(jnp.bfloat16, 2, rows, rows), field, square, square, field, block, sending],
        block_cols, step_tiles, mass, warm_start, source_ids, first=True,
    )
    t, q_outer, send = call(
        start_kernel, [field, block, sending], local, diag, t_in, base, other_x, send, aliases={5: 2}
    )
    got = lax.ppermute(send, ("groups",) + AXES, across)
    other_t = lax.ppermute(t, AXES, partner)
    q_inner, t_in_t, t_out = call(
        inner_kernel, [block, square, square], local, diag, t_in, t_out_t, t, other_t
    )
    w_inner = call(image_kernel, [block], local, q_inner, got)
    other_w = lax.ppermute(w_inner, AXES, partner)
    r, w, moments, edge, edge_r = call(
        moment_kernel, [field, field, (single, 8, columns), block, block],
        local, diag, t_in_t, t_out, t_out_t, t, q_outer, push, got, w_inner,
    )
    shares = call(share_kernel, [(single, devices, 3, 2, columns)], moments, edge, edge_r, other_t, other_w)
    shares = lax.all_to_all(shares, AXES, 0, 0)
    return call(finish_kernel, [field], shares, warm_start, r, w, last=True)


def solution(mesh):
    in_specs = (
        P(("groups", "patch", "sub"), None),
        P(("groups", "patch", "sub"), None, None, None),
        P(("groups", "patch", "sub")),
        P(("groups", "patch", "sub"), None),
        P("groups"),
    )
    out_specs = P(("groups", "patch", "sub"), None)
    return jax.shard_map(body, mesh=mesh, in_specs=in_specs, out_specs=out_specs, check_vma=False)
```

```python
import jax
import jax.numpy as jnp
from jax import lax
from jax.experimental import pallas as pl
from jax.experimental.pallas import tpu as pltpu
from jax.sharding import PartitionSpec as P


AXES = ("patch", "sub")
LEAST_EIGENVALUE = 0.0999
VMEM = pl.BlockSpec(memory_space=pltpu.VMEM)


def halves(a):
    high = a.astype(jnp.bfloat16)
    return high, (a - high.astype(jnp.float32)).astype(jnp.bfloat16)


def dot(a, b):
    a_high, a_low = a[0], a[1]
    b_high, b_low = halves(b)

    def product(p, q):
        return jnp.dot(p, q, preferred_element_type=jnp.float32)

    return product(a_high, b_high) + (product(a_high, b_low) + product(a_low, b_high))


def place():
    return lax.axis_index("patch") * lax.axis_size("sub") + lax.axis_index("sub")


def outer_block(tile):
    side = lax.rem(place(), 2)
    outer = pl.ds(pl.multiple_of(side * tile, tile), tile)
    inner = pl.ds(pl.multiple_of((1 - side) * tile, tile), tile)
    return outer, inner


def flip(x):
    return pltpu.roll(x, x.shape[1] // 2, 1)


def index_of(shape, dimension):
    return lax.broadcasted_iota(jnp.int32, shape, dimension)


def outer_kernel(
    cols_there, tiles_there, mass_there, x_there, sources_there,
    local_outer, diag_outer, t_out_t, x, tiles_inner, names, mass_inner, send,
    cols, tiles, mass, sources, arrived,
):
    tile = tiles.shape[-1]
    half = tile // 2
    slots = tiles.shape[0]
    position = place()
    side = lax.rem(position, 2)
    first = position * 2
    moves = (
        (cols_there, cols),
        (tiles_there.at[side], tiles),
        (x_there, x),
        (mass_there, mass),
        (sources_there, sources),
        (tiles_there.at[1 - side], tiles_inner),
    )
    copies = [pltpu.make_async_copy(start, end, arrived.at[i]) for i, (start, end) in enumerate(moves)]
    for copy in copies:
        copy.start()
    for copy in copies[:-1]:
        copy.wait()
    eye = index_of((tile, tile), 0) == index_of((tile, tile), 1)
    outer, _ = outer_block(tile)

    def toward(block, sign=1.0):
        slot, scale = jnp.int32(0), 0.0
        for k in range(slots):
            named = cols[side, k] == block
            slot, scale = jnp.where(named, k, slot), jnp.where(named, sign, scale)
        return scale * tiles[slot]

    whole, own = tiles[0], jnp.where(cols[side, 0] == first + side, tiles[0], 0.0)
    for k in range(1, slots):
        whole += tiles[k]
        own += jnp.where(cols[side, k] == first + side, tiles[k], 0.0)
    masses = mass[0:tile][None, :], mass[tile : 2 * tile][None, :]
    mass_here = jnp.where(side == 0, masses[0], masses[1])
    total = jnp.sum(whole + jnp.where(eye, mass_here, 0.0), axis=1, keepdims=True)
    diag_outer[...] = jnp.broadcast_to(total, diag_outer.shape)
    cross = toward(first + 1 - side, -1.0)
    store_halves(local_outer, (slice(None), slice(0, tile)), jnp.where(side == 0, -own, cross))
    store_halves(local_outer, (slice(None), slice(tile, 2 * tile)), jnp.where(side == 0, cross, -own))
    store_halves(t_out_t, (slice(None),), toward(jnp.where(side == 0, first - 1, first + 2)).T)
    vertices = (first + side) * tile + index_of((tile, x.shape[1]), 0)
    rhs = jnp.where(vertices == sources[...][None, :], 1.0, 0.0)
    send[0:tile, :] = rhs - total * x[outer, :] - dot(local_outer, x[...])
    send[tile : 2 * tile, :] = dot(t_out_t, x[outer, :])
    above_diagonal = index_of((half, tile), 1) > index_of((half, tile), 0)
    send[2 * tile : 2 * tile + half, :] = jnp.where(above_diagonal, own[:half], flip(own[half:]))
    diagonal = jnp.sum(jnp.where(eye, total, 0.0), axis=0, keepdims=True)
    send[2 * tile + half :, :] = jnp.broadcast_to(diagonal, (8, tile))
    mass_inner[...] = jnp.broadcast_to(jnp.where(side == 0, masses[1], masses[0]), mass_inner.shape)
    row = index_of(names.shape, 0)
    named = jnp.broadcast_to(sources[...][None, :], names.shape)
    for k in range(slots):
        named = jnp.where(row == k, cols[1 - side, k], named)
    names[...] = named
    copies[-1].wait()


def store_halves(pair, index, value):
    pair[(0, *index)], pair[(1, *index)] = halves(value)


def inner_row_kernel(
    local_outer, diag_outer, x, tiles, names, mass_inner, other_x, send,
    local, diag, t_in, t, q_outer, q_send,
):
    tile = tiles.shape[-1]
    half = tile // 2
    slots = tiles.shape[0]
    position = place()
    side = lax.rem(position, 2)
    first = position * 2
    outer, inner = outer_block(tile)
    eye = index_of((tile, tile), 0) == index_of((tile, tile), 1)

    def toward(block):
        total = jnp.where(names[0:1, :] == block, tiles[0], 0.0)
        for k in range(1, slots):
            total += jnp.where(names[k : k + 1, :] == block, tiles[k], 0.0)
        return total

    whole = tiles[0]
    for k in range(1, slots):
        whole += tiles[k]
    total = jnp.sum(whole + jnp.where(eye, mass_inner[0:1, :], 0.0), axis=1, keepdims=True)
    diag[outer, :] = diag_outer[...]
    diag[inner, :] = jnp.broadcast_to(total, diag_outer.shape)
    own, cross = -toward(first + 1 - side), -toward(first + side)
    store_halves(local, (inner, slice(0, tile)), jnp.where(side == 0, cross, own))
    store_halves(local, (inner, slice(tile, 2 * tile)), jnp.where(side == 0, own, cross))
    for k in range(2):
        local[k, outer, :] = local_outer[k]
    store_halves(t_in, (slice(None),), toward(jnp.where(side == 0, first + 2, first - 1)))
    vertices = (first + 1 - side) * tile + index_of((tile, x.shape[1]), 0)
    rhs = jnp.where(vertices == names[slots : slots + 1, :], 1.0, 0.0)
    t[outer, :] = send[0:tile, :]
    t[inner, :] = (
        rhs - total * x[inner, :] - dot(part(local, inner), x[...]) + dot(t_in, other_x[outer, :])
    )
    q = diag_outer[...] * send[0:tile, :] + dot(local_outer, t[...])
    q_outer[...] = q
    turned = jnp.where(side == 0, flip(q), q)
    first_half = index_of((half, tile), 1) < half
    q_send[...] = jnp.where(first_half, turned[:half], flip(turned[half:]))


def unpack(packed):
    tile = packed.shape[1]
    half = tile // 2
    rows = packed[0:half, :]
    row, column = index_of((half, tile), 0), index_of((half, tile), 1)
    upper = jnp.where(column > row, rows, 0.0)
    lower = flip(jnp.where(column < row, rows, 0.0))
    triangles = jnp.concatenate([upper, lower], axis=0)
    eye = index_of((tile, tile), 0) == index_of((tile, tile), 1)
    diagonal = jnp.sum(jnp.where(eye, packed[half : half + 1, :], 0.0), axis=1, keepdims=True)
    return triangles + triangles.T, diagonal


def outer_columns(tile):
    side = lax.rem(place(), 2)
    return pl.ds(pl.multiple_of(side * tile, tile), tile)


def part(pair, *index):
    return pair[(0, *index)], pair[(1, *index)]


def inner_kernel(local, diag, t_in, t_out_t, t, other_t, q_inner, t_in_t, t_out):
    outer, inner = outer_block(t_in.shape[-1])
    for half in range(2):
        t_in_t[half] = t_in[half].T
        t_out[half] = t_out_t[half].T
    q_inner[...] = (
        diag[inner, :] * t[inner, :] + dot(part(local, inner), t[...]) - dot(t_in, other_t[outer, :])
    )


def image_kernel(local, q_inner, got, w_inner):
    tile = q_inner.shape[0]
    _, inner = outer_block(tile)
    w_inner[...] = q_inner[...] + dot(part(local, inner, outer_columns(tile)), got[tile : 2 * tile, :])


def moment_kernel(
    local, diag, t_in_t, t_out, t_out_t, t, q_outer, send, got, got_q, w_inner, r, w, moments, edge, edge_r
):
    tile = t_out.shape[-1]
    half = tile // 2
    side = lax.rem(place(), 2)
    outer, inner = outer_block(tile)

    def total(value):
        return jnp.sum(value, axis=0, keepdims=True)

    push_here, push_there = got[tile : 2 * tile, :], send[tile : 2 * tile, :]
    r_outer, r_there = t[outer, :] + push_here, got[0:tile, :] + push_there
    pull_r = dot(t_out, r_there)
    w_outer = (
        q_outer[...]
        + diag[outer, :] * push_here
        + dot(part(local, outer, outer_columns(tile)), push_here)
        - pull_r
    )
    r[outer, :] = r_outer
    r[inner, :] = t[inner, :]
    w[outer, :] = w_outer
    w[inner, :] = w_inner[...]
    w_now, r_now = w[...], r[...]
    r_r, r_w = total(r_now * r_now), total(r_now * w_now)
    shift = jnp.where(r_r > 0, r_w / r_r, 0.0)
    y = w_now - shift * r_now
    y_outer = w_outer - shift * r_outer
    q_half = got_q[...]
    q_flip = flip(q_half)
    q_there = jnp.concatenate(
        [jnp.where(side == 0, q_half, q_flip), jnp.where(side == 0, q_flip, q_half)], axis=0
    )
    own_there, diag_there = unpack(got[2 * tile :, :])
    w_there = q_there + diag_there * push_there - dot(halves(own_there), push_there) - dot(t_out_t, r_outer)
    pull_y = dot(t_out, w_there - shift * r_there)
    mine = (index_of((1, r_now.shape[1]), 1) >= half) == (side == 1)
    weight = jnp.where(mine, 2.0, 0.0)
    a_y = diag[...] * y + dot(local, y)
    y_ay = total(y * a_y) - weight * total(y_outer * pull_y)
    r_ay = total(r_now * a_y + y * w_now) + total(y_outer * pull_r)
    r_ay -= weight * total(r_outer * pull_y + y_outer * pull_r)
    r_ar = r_w + (1.0 - weight) * total(r_outer * pull_r)
    moments[...] = jnp.concatenate([r_r, r_w, total(y * y), y_ay, r_ay, r_ar, shift, shift], axis=0)
    edge[...] = dot(t_in_t, w_inner[...] - shift * r[inner, :])
    edge_r[...] = dot(t_in_t, r[inner, :])


def share_kernel(moments, edge, edge_r, other_t, other_w, out):
    outer, _ = outer_block(edge.shape[0])
    y_there = other_w[...] - moments[6:7, :] * other_t[outer, :]
    y_ay = jnp.sum(edge[...] * y_there, axis=0, keepdims=True)
    r_ay = jnp.sum(edge_r[...] * y_there, axis=0, keepdims=True)
    row = index_of(moments.shape, 0)
    total = moments[...] - jnp.where(row == 3, y_ay, 0.0) - jnp.where(row == 4, r_ay, 0.0)
    for pair in range(out.shape[1]):
        out[:, pair] = jnp.broadcast_to(total[None, 2 * pair : 2 * pair + 2], out[:, pair].shape)


def finish_kernel(shares, x, r, w, out):
    r_rs, r_ws, spreads, y_ay, r_ay, r_ar = [shares[:, row // 2, row % 2, :] for row in range(6)]
    r_r = jnp.sum(r_rs, axis=0, keepdims=True)
    r_w = jnp.sum(r_ws, axis=0, keepdims=True)
    theta = r_w / r_r
    off = jnp.where(r_rs > 0, r_ws / r_rs, 0.0) - theta
    spread = jnp.sum(spreads + r_rs * off * off, axis=0, keepdims=True)
    energy = jnp.sum(y_ay + off * (r_ay + off * r_ar), axis=0, keepdims=True)
    ratio = spread / (theta * theta * r_r)
    energy = jnp.maximum(energy - ratio * theta * spread, LEAST_EIGENVALUE * spread * (1.0 + ratio))
    step = jnp.where(spread > 0, spread / energy, 0.0)
    first = 1.0 / theta
    out[...] = x[...] + (first + step * (1.0 + ratio)) * r[...] - (step * first) * w[...]


def call(kernel, shapes, *operands, last=False):
    place_out = jax.ShapeDtypeStruct if last else pltpu.VMEM
    outs = [place_out(shape[1:], shape[0]) for shape in shapes]
    return pl.pallas_call(
        kernel,
        out_shape=outs if len(outs) > 1 else outs[0],
        in_specs=[VMEM] * len(operands),
        out_specs=[VMEM] * len(outs) if len(outs) > 1 else VMEM,
    )(*[pltpu.with_memory_space_constraint(operand, pltpu.VMEM) for operand in operands])


def body(block_cols, step_tiles, mass, warm_start, source_ids):
    tile = step_tiles.shape[-1]
    rows, columns = warm_start.shape
    assert block_cols.shape[0] == 2 and columns == tile
    devices = lax.axis_size("patch") * lax.axis_size("sub")
    partner = [(i, i ^ 1) for i in range(devices)]
    groups = lax.axis_size("groups")
    across = []
    for group in range(groups):
        here, there = group * devices, (group + 1) % groups * devices
        for i in range(1, devices - 1, 2):
            across += [(here + i, here + i + 1), (here + i + 1, here + i)]
        across += [(here, there), (here + devices - 1, there + devices - 1)]
    single, slots = jnp.float32, block_cols.shape[1]
    assert slots < 8
    field, block = (single, rows, columns), (single, tile, columns)
    square, halfway = (jnp.bfloat16, 2, tile, tile), (single, tile // 2, columns)

    other_x = lax.ppermute(warm_start, AXES, partner)
    results = [
        (jnp.bfloat16, 2, tile, rows), block, square, field, (single, slots, tile, tile),
        (jnp.int32, 8, tile), (single, 8, tile), (single, 2 * tile + tile // 2 + 8, columns),
    ]
    local_outer, diag_outer, t_out_t, x, tiles_inner, names, mass_inner, send = pl.pallas_call(
        outer_kernel,
        out_shape=[pltpu.VMEM(shape[1:], shape[0]) for shape in results],
        in_specs=[pl.BlockSpec(memory_space=pl.ANY)] * 5,
        out_specs=[VMEM] * len(results),
        scratch_shapes=[
            pltpu.SMEM(block_cols.shape, jnp.int32),
            pltpu.VMEM((slots, tile, tile), single),
            pltpu.VMEM(mass.shape, single),
            pltpu.VMEM(source_ids.shape, jnp.int32),
            pltpu.SemaphoreType.DMA((6,)),
        ],
        name="outer_kernel",
    )(block_cols, step_tiles, mass, warm_start, source_ids)
    got = lax.ppermute(send, ("groups",) + AXES, across)
    local, diag, t_in, t, q_outer, q_send = call(
        inner_row_kernel,
        [(jnp.bfloat16, 2, rows, rows), field, square, field, block, halfway],
        local_outer, diag_outer, x, tiles_inner, names, mass_inner, other_x, send,
    )
    got_q = lax.ppermute(q_send, ("groups",) + AXES, across)
    other_t = lax.ppermute(t, AXES, partner)
    q_inner, t_in_t, t_out = call(
        inner_kernel, [block, square, square], local, diag, t_in, t_out_t, t, other_t
    )
    w_inner = call(image_kernel, [block], local, q_inner, got)
    other_w = lax.ppermute(w_inner, AXES, partner)
    r, w, moments, edge, edge_r = call(
        moment_kernel, [field, field, (single, 8, columns), block, block],
        local, diag, t_in_t, t_out, t_out_t, t, q_outer, send, got, got_q, w_inner,
    )
    shares = call(share_kernel, [(single, devices, 3, 2, columns)], moments, edge, edge_r, other_t, other_w)
    shares = lax.all_to_all(shares, AXES, 0, 0)
    return call(finish_kernel, [field], shares, x, r, w, last=True)


def solution(mesh):
    in_specs = (
        P(("groups", "patch", "sub"), None),
        P(("groups", "patch", "sub"), None, None, None),
        P(("groups", "patch", "sub")),
        P(("groups", "patch", "sub"), None),
        P("groups"),
    )
    out_specs = P(("groups", "patch", "sub"), None)
    return jax.shard_map(body, mesh=mesh, in_specs=in_specs, out_specs=out_specs, check_vma=False)
```

```python
import jax
import jax.numpy as jnp
from jax import lax
from jax.experimental import pallas as pl
from jax.experimental.pallas import tpu as pltpu
from jax.sharding import PartitionSpec as P


AXES = ("patch", "sub")
LEAST_EIGENVALUE = 0.0999
VMEM = pl.BlockSpec(memory_space=pltpu.VMEM)


def halves(a):
    high = a.astype(jnp.bfloat16)
    return high, (a - high.astype(jnp.float32)).astype(jnp.bfloat16)


def dot(a, b):
    a_high, a_low = a[0], a[1]
    b_high, b_low = halves(b)

    def product(p, q):
        return jnp.dot(p, q, preferred_element_type=jnp.float32)

    return product(a_high, b_high) + (product(a_high, b_low) + product(a_low, b_high))


def place():
    return lax.axis_index("patch") * lax.axis_size("sub") + lax.axis_index("sub")


def outer_block(tile):
    side = lax.rem(place(), 2)
    outer = pl.ds(pl.multiple_of(side * tile, tile), tile)
    inner = pl.ds(pl.multiple_of((1 - side) * tile, tile), tile)
    return outer, inner


def flip(x):
    return pltpu.roll(x, x.shape[1] // 2, 1)


def index_of(shape, dimension):
    return lax.broadcasted_iota(jnp.int32, shape, dimension)


def push_kernel(
    cols_there, tiles_there, mass_there, x_there, sources_there,
    push, t_out_t, x, tiles_outer, tiles_inner, names, masses,
    cols, mass, sources, arrived,
):
    tile = tiles_outer.shape[-1]
    slots = tiles_outer.shape[0]
    position = place()
    side = lax.rem(position, 2)
    moves = (
        (cols_there, cols),
        (tiles_there.at[side], tiles_outer),
        (x_there, x),
        (mass_there, mass),
        (sources_there, sources),
        (tiles_there.at[1 - side], tiles_inner),
    )
    copies = [pltpu.make_async_copy(start, end, arrived.at[i]) for i, (start, end) in enumerate(moves)]
    for copy in copies:
        copy.start()
    for copy in copies[:3]:
        copy.wait()
    outer, _ = outer_block(tile)
    beyond = 2 * position + jnp.where(side == 0, -1, 2)
    slot, scale = jnp.int32(0), 0.0
    for k in range(slots):
        named = cols[side, k] == beyond
        slot, scale = jnp.where(named, k, slot), jnp.where(named, 1.0, scale)
    store_halves(t_out_t, (slice(None),), (scale * tiles_outer[slot]).T)
    push[...] = dot(t_out_t, x[outer, :])
    for copy in copies[3:]:
        copy.wait()
    row = index_of(names.shape, 0)
    named = jnp.broadcast_to(sources[...][None, :], names.shape)
    for k in range(slots):
        named = jnp.where(row == k, cols[side, k], named)
        named = jnp.where(row == 8 + k, cols[1 - side, k], named)
    names[...] = named
    first, second = mass[0:tile][None, :], mass[tile : 2 * tile][None, :]
    masses[0:8, :] = jnp.broadcast_to(jnp.where(side == 0, first, second), (8, tile))
    masses[8:16, :] = jnp.broadcast_to(jnp.where(side == 0, second, first), (8, tile))


def toward(tiles, names, block):
    total = jnp.where(names[0:1, :] == block, tiles[0], 0.0)
    for k in range(1, tiles.shape[0]):
        total += jnp.where(names[k : k + 1, :] == block, tiles[k], 0.0)
    return total


def row_sums(tiles, masses):
    tile = tiles.shape[-1]
    whole = tiles[0]
    for k in range(1, tiles.shape[0]):
        whole += tiles[k]
    eye = index_of((tile, tile), 0) == index_of((tile, tile), 1)
    return jnp.sum(whole + jnp.where(eye, masses[0:1, :], 0.0), axis=1, keepdims=True)


def right_side(names, block, shape):
    vertices = block * shape[0] + index_of(shape, 0)
    return jnp.where(vertices == names[7:8, :], 1.0, 0.0)


def outer_kernel(x, tiles, names, masses, local_outer, diag_outer, send):
    tile = tiles.shape[-1]
    half = tile // 2
    position = place()
    side = lax.rem(position, 2)
    first = position * 2
    outer, _ = outer_block(tile)
    names, masses = names[0:8, :], masses[0:8, :]
    total = row_sums(tiles, masses)
    diag_outer[...] = jnp.broadcast_to(total, diag_outer.shape)
    own, cross = toward(tiles, names, first + side), toward(tiles, names, first + 1 - side)
    store_halves(local_outer, (slice(None), slice(0, tile)), jnp.where(side == 0, -own, -cross))
    store_halves(local_outer, (slice(None), slice(tile, 2 * tile)), jnp.where(side == 0, -cross, -own))
    x_outer = x[outer, :]
    send[0:tile, :] = (
        right_side(names, first + side, x_outer.shape) - total * x_outer - dot(local_outer, x[...])
    )
    above_diagonal = index_of((half, tile), 1) > index_of((half, tile), 0)
    send[tile : tile + half, :] = jnp.where(above_diagonal, own[:half], flip(own[half:]))
    eye = index_of((tile, tile), 0) == index_of((tile, tile), 1)
    diagonal = jnp.sum(jnp.where(eye, total, 0.0), axis=0, keepdims=True)
    send[tile + half :, :] = jnp.broadcast_to(diagonal, (8, tile))


def store_halves(pair, index, value):
    pair[(0, *index)], pair[(1, *index)] = halves(value)


def inner_row_kernel(
    local_outer, diag_outer, x, tiles, names, masses, other_x, send,
    local, diag, t_in, t, q_outer, q_send,
):
    tile = tiles.shape[-1]
    half = tile // 2
    position = place()
    side = lax.rem(position, 2)
    first = position * 2
    outer, inner = outer_block(tile)
    names, masses = names[8:16, :], masses[8:16, :]
    total = row_sums(tiles, masses)
    diag[outer, :] = diag_outer[...]
    diag[inner, :] = jnp.broadcast_to(total, diag_outer.shape)
    own, cross = toward(tiles, names, first + 1 - side), toward(tiles, names, first + side)
    store_halves(local, (inner, slice(0, tile)), jnp.where(side == 0, -cross, -own))
    store_halves(local, (inner, slice(tile, 2 * tile)), jnp.where(side == 0, -own, -cross))
    for k in range(2):
        local[k, outer, :] = local_outer[k]
    store_halves(t_in, (slice(None),), toward(tiles, names, jnp.where(side == 0, first + 2, first - 1)))
    x_inner = x[inner, :]
    t[outer, :] = send[0:tile, :]
    t[inner, :] = (
        right_side(names, first + 1 - side, x_inner.shape)
        - total * x_inner
        - dot(part(local, inner), x[...])
        + dot(t_in, other_x[outer, :])
    )
    q = diag_outer[...] * send[0:tile, :] + dot(local_outer, t[...])
    q_outer[...] = q
    turned = jnp.where(side == 0, flip(q), q)
    first_half = index_of((half, tile), 1) < half
    q_send[...] = jnp.where(first_half, turned[:half], flip(turned[half:]))


def unpack(packed):
    tile = packed.shape[1]
    half = tile // 2
    rows = packed[0:half, :]
    row, column = index_of((half, tile), 0), index_of((half, tile), 1)
    upper = jnp.where(column > row, rows, 0.0)
    lower = flip(jnp.where(column < row, rows, 0.0))
    triangles = jnp.concatenate([upper, lower], axis=0)
    eye = index_of((tile, tile), 0) == index_of((tile, tile), 1)
    diagonal = jnp.sum(jnp.where(eye, packed[half : half + 1, :], 0.0), axis=1, keepdims=True)
    return triangles + triangles.T, diagonal


def outer_columns(tile):
    side = lax.rem(place(), 2)
    return pl.ds(pl.multiple_of(side * tile, tile), tile)


def part(pair, *index):
    return pair[(0, *index)], pair[(1, *index)]


def inner_kernel(local, diag, t_in, t_out_t, t, other_t, q_inner, t_in_t, t_out):
    outer, inner = outer_block(t_in.shape[-1])
    for half in range(2):
        t_in_t[half] = t_in[half].T
        t_out[half] = t_out_t[half].T
    q_inner[...] = (
        diag[inner, :] * t[inner, :] + dot(part(local, inner), t[...]) - dot(t_in, other_t[outer, :])
    )


def image_kernel(local, q_inner, push_here, w_inner):
    tile = q_inner.shape[0]
    _, inner = outer_block(tile)
    w_inner[...] = q_inner[...] + dot(part(local, inner, outer_columns(tile)), push_here[...])


def total(value):
    return jnp.sum(value, axis=0, keepdims=True)


def moment_kernel(
    local, diag, t_in_t, t_out, t, q_outer, push_here, push_there, got, w_inner,
    r, w, y_outer, pull_r, moments, edge, edge_r,
):
    tile = t_out.shape[-1]
    outer, inner = outer_block(tile)
    r_outer = t[outer, :] + push_here[...]
    pull = dot(t_out, got[0:tile, :] + push_there[...])
    w_outer = (
        q_outer[...]
        + diag[outer, :] * push_here[...]
        + dot(part(local, outer, outer_columns(tile)), push_here[...])
        - pull
    )
    r[outer, :] = r_outer
    r[inner, :] = t[inner, :]
    w[outer, :] = w_outer
    w[inner, :] = w_inner[...]
    w_now, r_now = w[...], r[...]
    r_r, r_w = total(r_now * r_now), total(r_now * w_now)
    shift = jnp.where(r_r > 0, r_w / r_r, 0.0)
    y = w_now - shift * r_now
    y_out = w_outer - shift * r_outer
    a_y = diag[...] * y + dot(local, y)
    r_ay = total(r_now * a_y + y * w_now) + total(y_out * pull)
    r_ar = r_w + total(r_outer * pull)
    y_outer[...] = y_out
    pull_r[...] = pull
    moments[...] = jnp.concatenate([r_r, r_w, total(y * y), total(y * a_y), r_ay, r_ar, shift, shift], axis=0)
    edge[...] = dot(t_in_t, w_inner[...] - shift * r[inner, :])
    edge_r[...] = dot(t_in_t, r[inner, :])


def share_kernel(
    moments, edge, edge_r, y_outer, pull_r, r, t_out, t_out_t, push_there, got, got_q, other_t, other_w, out
):
    tile = t_out.shape[-1]
    half = tile // 2
    side = lax.rem(place(), 2)
    outer, _ = outer_block(tile)
    shift = moments[6:7, :]
    q_half = got_q[...]
    q_flip = flip(q_half)
    q_there = jnp.concatenate(
        [jnp.where(side == 0, q_half, q_flip), jnp.where(side == 0, q_flip, q_half)], axis=0
    )
    own_there, diag_there = unpack(got[tile:, :])
    r_outer, r_there = r[outer, :], got[0:tile, :] + push_there[...]
    w_there = (
        q_there
        + diag_there * push_there[...]
        - dot(halves(own_there), push_there[...])
        - dot(t_out_t, r_outer)
    )
    pull_y = dot(t_out, w_there - shift * r_there)
    mine = (index_of(shift.shape, 1) >= half) == (side == 1)
    weight = jnp.where(mine, 2.0, 0.0)
    y_partner = other_w[...] - shift * other_t[outer, :]
    y_ay = total(edge[...] * y_partner) + weight * total(y_outer[...] * pull_y)
    r_ay = total(edge_r[...] * y_partner)
    r_ay += weight * total(r_outer * pull_y + y_outer[...] * pull_r[...])
    r_ar = weight * total(r_outer * pull_r[...])
    row = index_of(moments.shape, 0)
    sums = moments[...]
    for place_of, value in ((3, y_ay), (4, r_ay), (5, r_ar)):
        sums -= jnp.where(row == place_of, value, 0.0)
    for pair in range(out.shape[1]):
        out[:, pair] = jnp.broadcast_to(sums[None, 2 * pair : 2 * pair + 2], out[:, pair].shape)


def finish_kernel(shares, x, r, w, out):
    r_rs, r_ws, spreads, y_ay, r_ay, r_ar = [shares[:, row // 2, row % 2, :] for row in range(6)]
    r_r = jnp.sum(r_rs, axis=0, keepdims=True)
    r_w = jnp.sum(r_ws, axis=0, keepdims=True)
    theta = r_w / r_r
    off = jnp.where(r_rs > 0, r_ws / r_rs, 0.0) - theta
    spread = jnp.sum(spreads + r_rs * off * off, axis=0, keepdims=True)
    energy = jnp.sum(y_ay + off * (r_ay + off * r_ar), axis=0, keepdims=True)
    ratio = spread / (theta * theta * r_r)
    energy = jnp.maximum(energy - ratio * theta * spread, LEAST_EIGENVALUE * spread * (1.0 + ratio))
    step = jnp.where(spread > 0, spread / energy, 0.0)
    first = 1.0 / theta
    out[...] = x[...] + (first + step * (1.0 + ratio)) * r[...] - (step * first) * w[...]


def call(kernel, shapes, *operands, last=False):
    place_out = jax.ShapeDtypeStruct if last else pltpu.VMEM
    outs = [place_out(shape[1:], shape[0]) for shape in shapes]
    return pl.pallas_call(
        kernel,
        out_shape=outs if len(outs) > 1 else outs[0],
        in_specs=[VMEM] * len(operands),
        out_specs=[VMEM] * len(outs) if len(outs) > 1 else VMEM,
    )(*[pltpu.with_memory_space_constraint(operand, pltpu.VMEM) for operand in operands])


def body(block_cols, step_tiles, mass, warm_start, source_ids):
    tile = step_tiles.shape[-1]
    rows, columns = warm_start.shape
    assert block_cols.shape[0] == 2 and columns == tile
    devices = lax.axis_size("patch") * lax.axis_size("sub")
    partner = [(i, i ^ 1) for i in range(devices)]
    groups = lax.axis_size("groups")
    across = []
    for group in range(groups):
        here, there = group * devices, (group + 1) % groups * devices
        for i in range(1, devices - 1, 2):
            across += [(here + i, here + i + 1), (here + i + 1, here + i)]
        across += [(here, there), (here + devices - 1, there + devices - 1)]
    single, slots = jnp.float32, block_cols.shape[1]
    assert slots < 8
    field, block = (single, rows, columns), (single, tile, columns)
    square, halfway = (jnp.bfloat16, 2, tile, tile), (single, tile // 2, columns)
    tiles = (single, slots, tile, tile)

    def exchange(value):
        return lax.ppermute(value, ("groups",) + AXES, across)

    other_x = lax.ppermute(warm_start, AXES, partner)
    results = [block, square, field, tiles, tiles, (jnp.int32, 16, tile), (single, 16, tile)]
    push_there, t_out_t, x, tiles_outer, tiles_inner, names, masses = pl.pallas_call(
        push_kernel,
        out_shape=[pltpu.VMEM(shape[1:], shape[0]) for shape in results],
        in_specs=[pl.BlockSpec(memory_space=pl.ANY)] * 5,
        out_specs=[VMEM] * len(results),
        scratch_shapes=[
            pltpu.SMEM(block_cols.shape, jnp.int32),
            pltpu.VMEM(mass.shape, single),
            pltpu.VMEM(source_ids.shape, jnp.int32),
            pltpu.SemaphoreType.DMA((6,)),
        ],
        name="push_kernel",
    )(block_cols, step_tiles, mass, warm_start, source_ids)
    push_here = exchange(push_there)
    local_outer, diag_outer, send = call(
        outer_kernel,
        [(jnp.bfloat16, 2, tile, rows), block, (single, tile + tile // 2 + 8, columns)],
        x, tiles_outer, names, masses,
    )
    got = exchange(send)
    local, diag, t_in, t, q_outer, q_send = call(
        inner_row_kernel,
        [(jnp.bfloat16, 2, rows, rows), field, square, field, block, halfway],
        local_outer, diag_outer, x, tiles_inner, names, masses, other_x, send,
    )
    got_q = exchange(q_send)
    other_t = lax.ppermute(t, AXES, partner)
    q_inner, t_in_t, t_out = call(
        inner_kernel, [block, square, square], local, diag, t_in, t_out_t, t, other_t
    )
    w_inner = call(image_kernel, [block], local, q_inner, push_here)
    other_w = lax.ppermute(w_inner, AXES, partner)
    r, w, y_outer, pull_r, moments, edge, edge_r = call(
        moment_kernel, [field, field, block, block, (single, 8, columns), block, block],
        local, diag, t_in_t, t_out, t, q_outer, push_here, push_there, got, w_inner,
    )
    shares = call(
        share_kernel, [(single, devices, 3, 2, columns)],
        moments, edge, edge_r, y_outer, pull_r, r, t_out, t_out_t, push_there, got, got_q, other_t, other_w,
    )
    shares = lax.all_to_all(shares, AXES, 0, 0)
    return call(finish_kernel, [field], shares, x, r, w, last=True)


def solution(mesh):
    in_specs = (
        P(("groups", "patch", "sub"), None),
        P(("groups", "patch", "sub"), None, None, None),
        P(("groups", "patch", "sub")),
        P(("groups", "patch", "sub"), None),
        P("groups"),
    )
    out_specs = P(("groups", "patch", "sub"), None)
    return jax.shard_map(body, mesh=mesh, in_specs=in_specs, out_specs=out_specs, check_vma=False)
```

```python
import jax
import jax.numpy as jnp
from jax import lax
from jax.experimental import pallas as pl
from jax.experimental.pallas import tpu as pltpu
from jax.sharding import PartitionSpec as P


AXES = ("patch", "sub")
LEAST_EIGENVALUE = 0.0999
VMEM = pl.BlockSpec(memory_space=pltpu.VMEM)


def halves(a):
    high = a.astype(jnp.bfloat16)
    return high, (a - high.astype(jnp.float32)).astype(jnp.bfloat16)


def dot(a, b):
    a_high, a_low = a[0], a[1]
    b_high, b_low = halves(b)

    def product(p, q):
        return jnp.dot(p, q, preferred_element_type=jnp.float32)

    return product(a_high, b_high) + (product(a_high, b_low) + product(a_low, b_high))


def place():
    return lax.axis_index("patch") * lax.axis_size("sub") + lax.axis_index("sub")


def outer_block(tile):
    side = lax.rem(place(), 2)
    outer = pl.ds(pl.multiple_of(side * tile, tile), tile)
    inner = pl.ds(pl.multiple_of((1 - side) * tile, tile), tile)
    return outer, inner


def flip(x):
    return pltpu.roll(x, x.shape[1] // 2, 1)


def index_of(shape, dimension):
    return lax.broadcasted_iota(jnp.int32, shape, dimension)


def toward(tiles, names, block):
    total = jnp.where(names[0:1, :] == block, tiles[0], 0.0)
    for k in range(1, tiles.shape[0]):
        total += jnp.where(names[k : k + 1, :] == block, tiles[k], 0.0)
    return total


def row_sums(tiles, masses):
    tile = tiles.shape[-1]
    whole = tiles[0]
    for k in range(1, tiles.shape[0]):
        whole += tiles[k]
    eye = index_of((tile, tile), 0) == index_of((tile, tile), 1)
    return jnp.sum(whole + jnp.where(eye, masses[0:1, :], 0.0), axis=1, keepdims=True)


def right_side(names, block, shape):
    vertices = block * shape[0] + index_of(shape, 0)
    return jnp.where(vertices == names[7:8, :], 1.0, 0.0)


def outer_kernel(
    cols_there, tiles_there, mass_there, x_there, sources_there,
    local_outer, diag_outer, t_out_t, x, tiles_inner, names, masses, send, packed,
    cols, tiles, mass, sources, arrived,
):
    tile = tiles.shape[-1]
    half = tile // 2
    slots = tiles.shape[0]
    position = place()
    side = lax.rem(position, 2)
    first = position * 2
    moves = (
        (cols_there, cols),
        (tiles_there.at[side], tiles),
        (x_there, x),
        (mass_there, mass),
        (sources_there, sources),
        (tiles_there.at[1 - side], tiles_inner),
    )
    copies = [pltpu.make_async_copy(start, end, arrived.at[i]) for i, (start, end) in enumerate(moves)]
    for copy in copies:
        copy.start()
    for copy in copies[:-1]:
        copy.wait()
    eye = index_of((tile, tile), 0) == index_of((tile, tile), 1)
    outer, _ = outer_block(tile)
    row = index_of(names.shape, 0)
    named = jnp.broadcast_to(sources[...][None, :], names.shape)
    for k in range(slots):
        named = jnp.where(row == k, cols[1 - side, k], named)
    names[...] = named
    mass_0, mass_1 = mass[0:tile][None, :], mass[tile : 2 * tile][None, :]
    masses[...] = jnp.broadcast_to(jnp.where(side == 0, mass_1, mass_0), masses.shape)

    def one_toward(block):
        slot, scale = jnp.int32(0), 0.0
        for k in range(slots):
            found = cols[side, k] == block
            slot, scale = jnp.where(found, k, slot), jnp.where(found, 1.0, scale)
        return scale * tiles[slot]

    own = jnp.where(cols[side, 0] == first + side, tiles[0], 0.0)
    for k in range(1, slots):
        own += jnp.where(cols[side, k] == first + side, tiles[k], 0.0)
    cross = one_toward(first + 1 - side)
    total = row_sums(tiles, jnp.where(side == 0, mass_0, mass_1))
    diag_outer[...] = jnp.broadcast_to(total, diag_outer.shape)
    store_halves(local_outer, (slice(None), slice(0, tile)), jnp.where(side == 0, -own, -cross))
    store_halves(local_outer, (slice(None), slice(tile, 2 * tile)), jnp.where(side == 0, -cross, -own))
    store_halves(t_out_t, (slice(None),), one_toward(jnp.where(side == 0, first - 1, first + 2)).T)
    x_outer = x[outer, :]
    send[0:tile, :] = (
        right_side(named, first + side, x_outer.shape) - total * x_outer - dot(local_outer, x[...])
    )
    send[tile:, :] = dot(t_out_t, x_outer)
    above_diagonal = index_of((half, tile), 1) > index_of((half, tile), 0)
    packed[0:half, :] = jnp.where(above_diagonal, own[:half], flip(own[half:]))
    diagonal = jnp.sum(jnp.where(eye, total, 0.0), axis=0, keepdims=True)
    packed[half:, :] = jnp.broadcast_to(diagonal, (8, tile))
    copies[-1].wait()


def store_halves(pair, index, value):
    pair[(0, *index)], pair[(1, *index)] = halves(value)


def inner_row_kernel(
    local_outer, diag_outer, x, tiles, names, masses, other_x, send, packed,
    local, diag, t_in, t, q_outer, send_late,
):
    tile = tiles.shape[-1]
    half = tile // 2
    position = place()
    side = lax.rem(position, 2)
    first = position * 2
    outer, inner = outer_block(tile)
    total = row_sums(tiles, masses)
    diag[outer, :] = diag_outer[...]
    diag[inner, :] = jnp.broadcast_to(total, diag_outer.shape)
    own, cross = toward(tiles, names, first + 1 - side), toward(tiles, names, first + side)
    store_halves(local, (inner, slice(0, tile)), jnp.where(side == 0, -cross, -own))
    store_halves(local, (inner, slice(tile, 2 * tile)), jnp.where(side == 0, -own, -cross))
    for k in range(2):
        local[k, outer, :] = local_outer[k]
    store_halves(t_in, (slice(None),), toward(tiles, names, jnp.where(side == 0, first + 2, first - 1)))
    x_inner = x[inner, :]
    t[outer, :] = send[0:tile, :]
    t[inner, :] = (
        right_side(names, first + 1 - side, x_inner.shape)
        - total * x_inner
        - dot(part(local, inner), x[...])
        + dot(t_in, other_x[outer, :])
    )
    q = diag_outer[...] * send[0:tile, :] + dot(local_outer, t[...])
    q_outer[...] = q
    turned = jnp.where(side == 0, flip(q), q)
    first_half = index_of((half, tile), 1) < half
    send_late[0:half, :] = jnp.where(first_half, turned[:half], flip(turned[half:]))
    send_late[half:, :] = packed[...]


def unpack(packed):
    tile = packed.shape[1]
    half = tile // 2
    rows = packed[0:half, :]
    row, column = index_of((half, tile), 0), index_of((half, tile), 1)
    upper = jnp.where(column > row, rows, 0.0)
    lower = flip(jnp.where(column < row, rows, 0.0))
    triangles = jnp.concatenate([upper, lower], axis=0)
    eye = index_of((tile, tile), 0) == index_of((tile, tile), 1)
    diagonal = jnp.sum(jnp.where(eye, packed[half : half + 1, :], 0.0), axis=1, keepdims=True)
    return triangles + triangles.T, diagonal


def outer_columns(tile):
    side = lax.rem(place(), 2)
    return pl.ds(pl.multiple_of(side * tile, tile), tile)


def part(pair, *index):
    return pair[(0, *index)], pair[(1, *index)]


def inner_kernel(local, diag, t_in, t_out_t, t, other_t, q_inner, t_in_t, t_out):
    outer, inner = outer_block(t_in.shape[-1])
    for half in range(2):
        t_in_t[half] = t_in[half].T
        t_out[half] = t_out_t[half].T
    q_inner[...] = (
        diag[inner, :] * t[inner, :] + dot(part(local, inner), t[...]) - dot(t_in, other_t[outer, :])
    )


def image_kernel(local, q_inner, got, w_inner):
    tile = q_inner.shape[0]
    _, inner = outer_block(tile)
    w_inner[...] = q_inner[...] + dot(part(local, inner, outer_columns(tile)), got[tile:, :])


def total(value):
    return jnp.sum(value, axis=0, keepdims=True)


def moment_kernel(
    local, diag, t_in_t, t_out, t_out_t, t, q_outer, send, got, w_inner,
    r, w, there, edge_y_out, edge_r_out, moments, edge_y_in, edge_r_in,
):
    tile = t_out.shape[-1]
    outer, inner = outer_block(tile)
    push_here, push_there = got[tile:, :], send[tile:, :]
    r_outer, r_there = t[outer, :] + push_here, got[0:tile, :] + push_there
    pull = dot(t_out, r_there)
    w_outer = (
        q_outer[...]
        + diag[outer, :] * push_here
        + dot(part(local, outer, outer_columns(tile)), push_here)
        - pull
    )
    r[outer, :] = r_outer
    r[inner, :] = t[inner, :]
    w[outer, :] = w_outer
    w[inner, :] = w_inner[...]
    w_now, r_now = w[...], r[...]
    r_r, r_w = total(r_now * r_now), total(r_now * w_now)
    shift = jnp.where(r_r > 0, r_w / r_r, 0.0)
    y = w_now - shift * r_now
    y_outer = w_outer - shift * r_outer
    a_y = diag[...] * y + dot(local, y)
    y_pull, r_pull = total(y_outer * pull), total(r_outer * pull)
    r_ay = total(r_now * a_y + y * w_now) + y_pull
    moments[...] = jnp.concatenate(
        [r_r, r_w, total(y * y), total(y * a_y), r_ay, r_w + r_pull, shift, y_pull, r_pull]
        + [shift] * (moments.shape[0] - 9),
        axis=0,
    )
    back = dot(t_out_t, r_outer)
    edge_r_out[...] = back
    edge_y_out[...] = dot(t_out_t, y_outer)
    there[...] = -back - shift * r_there
    edge_y_in[...] = dot(t_in_t, w_inner[...] - shift * r[inner, :])
    edge_r_in[...] = dot(t_in_t, r[inner, :])


def share_kernel(
    moments, edge_y_in, edge_r_in, edge_y_out, edge_r_out, there, send, got, other_t, other_w, out
):
    tile = there.shape[0]
    half = tile // 2
    side = lax.rem(place(), 2)
    outer, _ = outer_block(tile)
    shift = moments[6:7, :]
    q_half = got[0:half, :]
    q_flip = flip(q_half)
    q_there = jnp.concatenate(
        [jnp.where(side == 0, q_half, q_flip), jnp.where(side == 0, q_flip, q_half)], axis=0
    )
    own_there, diag_there = unpack(got[half:, :])
    push_there = send[tile:, :]
    y_there = q_there + there[...] + diag_there * push_there - dot(halves(own_there), push_there)
    mine = (index_of(shift.shape, 1) >= half) == (side == 1)
    weight = jnp.where(mine, 2.0, 0.0)
    y_partner = other_w[...] - shift * other_t[outer, :]
    y_ay = total(edge_y_in[...] * y_partner) + weight * total(edge_y_out[...] * y_there)
    r_ay = total(edge_r_in[...] * y_partner)
    r_ay += weight * (total(edge_r_out[...] * y_there) + moments[7:8, :])
    r_ar = weight * moments[8:9, :]
    sums = moments[0:8, :]
    row = index_of(sums.shape, 0)
    for place_of, value in ((3, y_ay), (4, r_ay), (5, r_ar)):
        sums -= jnp.where(row == place_of, value, 0.0)
    for pair in range(out.shape[1]):
        out[:, pair] = jnp.broadcast_to(sums[None, 2 * pair : 2 * pair + 2], out[:, pair].shape)


def finish_kernel(shares, x, r, w, out):
    r_rs, r_ws, spreads, y_ay, r_ay, r_ar = [shares[:, row // 2, row % 2, :] for row in range(6)]
    r_r = jnp.sum(r_rs, axis=0, keepdims=True)
    r_w = jnp.sum(r_ws, axis=0, keepdims=True)
    theta = r_w / r_r
    off = jnp.where(r_rs > 0, r_ws / r_rs, 0.0) - theta
    spread = jnp.sum(spreads + r_rs * off * off, axis=0, keepdims=True)
    energy = jnp.sum(y_ay + off * (r_ay + off * r_ar), axis=0, keepdims=True)
    ratio = spread / (theta * theta * r_r)
    energy = jnp.maximum(energy - ratio * theta * spread, LEAST_EIGENVALUE * spread * (1.0 + ratio))
    step = jnp.where(spread > 0, spread / energy, 0.0)
    first = 1.0 / theta
    out[...] = x[...] + (first + step * (1.0 + ratio)) * r[...] - (step * first) * w[...]


def call(kernel, shapes, *operands, last=False):
    place_out = jax.ShapeDtypeStruct if last else pltpu.VMEM
    outs = [place_out(shape[1:], shape[0]) for shape in shapes]
    return pl.pallas_call(
        kernel,
        out_shape=outs if len(outs) > 1 else outs[0],
        in_specs=[VMEM] * len(operands),
        out_specs=[VMEM] * len(outs) if len(outs) > 1 else VMEM,
    )(*[pltpu.with_memory_space_constraint(operand, pltpu.VMEM) for operand in operands])


def body(block_cols, step_tiles, mass, warm_start, source_ids):
    tile = step_tiles.shape[-1]
    rows, columns = warm_start.shape
    assert block_cols.shape[0] == 2 and columns == tile
    devices = lax.axis_size("patch") * lax.axis_size("sub")
    partner = [(i, i ^ 1) for i in range(devices)]
    groups = lax.axis_size("groups")
    across = []
    for group in range(groups):
        here, there = group * devices, (group + 1) % groups * devices
        for i in range(1, devices - 1, 2):
            across += [(here + i, here + i + 1), (here + i + 1, here + i)]
        across += [(here, there), (here + devices - 1, there + devices - 1)]
    single, slots = jnp.float32, block_cols.shape[1]
    assert slots < 8
    field, block = (single, rows, columns), (single, tile, columns)
    square, late = (jnp.bfloat16, 2, tile, tile), tile // 2 + 8

    def exchange(value):
        return lax.ppermute(value, ("groups",) + AXES, across)

    other_x = lax.ppermute(warm_start, AXES, partner)
    results = [
        (jnp.bfloat16, 2, tile, rows), block, square, field, (single, slots, tile, tile),
        (jnp.int32, 8, tile), (single, 8, tile), (single, 2 * tile, columns), (single, late, columns),
    ]
    local_outer, diag_outer, t_out_t, x, tiles_inner, names, masses, send, packed = pl.pallas_call(
        outer_kernel,
        out_shape=[pltpu.VMEM(shape[1:], shape[0]) for shape in results],
        in_specs=[pl.BlockSpec(memory_space=pl.ANY)] * 5,
        out_specs=[VMEM] * len(results),
        scratch_shapes=[
            pltpu.SMEM(block_cols.shape, jnp.int32),
            pltpu.VMEM((slots, tile, tile), single),
            pltpu.VMEM(mass.shape, single),
            pltpu.VMEM(source_ids.shape, jnp.int32),
            pltpu.SemaphoreType.DMA((6,)),
        ],
        name="outer_kernel",
    )(block_cols, step_tiles, mass, warm_start, source_ids)
    got = exchange(send)
    local, diag, t_in, t, q_outer, send_late = call(
        inner_row_kernel,
        [(jnp.bfloat16, 2, rows, rows), field, square, field, block, (single, tile // 2 + late, columns)],
        local_outer, diag_outer, x, tiles_inner, names, masses, other_x, send, packed,
    )
    got_late = exchange(send_late)
    other_t = lax.ppermute(t, AXES, partner)
    q_inner, t_in_t, t_out = call(
        inner_kernel, [block, square, square], local, diag, t_in, t_out_t, t, other_t
    )
    w_inner = call(image_kernel, [block], local, q_inner, got)
    other_w = lax.ppermute(w_inner, AXES, partner)
    r, w, there, edge_y_out, edge_r_out, moments, edge_y_in, edge_r_in = call(
        moment_kernel, [field, field, block, block, block, (single, 16, columns), block, block],
        local, diag, t_in_t, t_out, t_out_t, t, q_outer, send, got, w_inner,
    )
    shares = call(
        share_kernel, [(single, devices, 3, 2, columns)],
        moments, edge_y_in, edge_r_in, edge_y_out, edge_r_out, there, send, got_late, other_t, other_w,
    )
    shares = lax.all_to_all(shares, AXES, 0, 0)
    return call(finish_kernel, [field], shares, x, r, w, last=True)


def solution(mesh):
    in_specs = (
        P(("groups", "patch", "sub"), None),
        P(("groups", "patch", "sub"), None, None, None),
        P(("groups", "patch", "sub")),
        P(("groups", "patch", "sub"), None),
        P("groups"),
    )
    out_specs = P(("groups", "patch", "sub"), None)
    return jax.shard_map(body, mesh=mesh, in_specs=in_specs, out_specs=out_specs, check_vma=False)
```

```python
import jax
import jax.numpy as jnp
from jax import lax
from jax.experimental import pallas as pl
from jax.experimental.pallas import tpu as pltpu
from jax.sharding import PartitionSpec as P


AXES = ("patch", "sub")
LEAST_EIGENVALUE = 0.0999
VMEM = pl.BlockSpec(memory_space=pltpu.VMEM)


def halves(a):
    high = a.astype(jnp.bfloat16)
    return high, (a - high.astype(jnp.float32)).astype(jnp.bfloat16)


def dot(a, b):
    a_high, a_low = a[0], a[1]
    b_high, b_low = halves(b)

    def product(p, q):
        return jnp.dot(p, q, preferred_element_type=jnp.float32)

    return product(a_high, b_high) + (product(a_high, b_low) + product(a_low, b_high))


def place():
    return lax.axis_index("patch") * lax.axis_size("sub") + lax.axis_index("sub")


def outer_block(tile):
    side = lax.rem(place(), 2)
    outer = pl.ds(pl.multiple_of(side * tile, tile), tile)
    inner = pl.ds(pl.multiple_of((1 - side) * tile, tile), tile)
    return outer, inner


def flip(x):
    return pltpu.roll(x, x.shape[1] // 2, 1)


def index_of(shape, dimension):
    return lax.broadcasted_iota(jnp.int32, shape, dimension)


def toward(tiles, names, block):
    total = jnp.where(names[0:1, :] == block, tiles[0], 0.0)
    for k in range(1, tiles.shape[0]):
        total += jnp.where(names[k : k + 1, :] == block, tiles[k], 0.0)
    return total


def row_sums(tiles, masses):
    tile = tiles.shape[-1]
    whole = tiles[0]
    for k in range(1, tiles.shape[0]):
        whole += tiles[k]
    eye = index_of((tile, tile), 0) == index_of((tile, tile), 1)
    return jnp.sum(whole + jnp.where(eye, masses[0:1, :], 0.0), axis=1, keepdims=True)


def right_side(names, block, shape):
    vertices = block * shape[0] + index_of(shape, 0)
    return jnp.where(vertices == names[7:8, :], 1.0, 0.0)


def outer_kernel(
    cols_there, tiles_there, mass_there, x_there, sources_there,
    local_outer, diag_outer, t_out_t, x, tiles_inner, names, masses, push, send,
    cols, tiles, mass, sources, arrived,
):
    tile = tiles.shape[-1]
    half = tile // 2
    slots = tiles.shape[0]
    position = place()
    side = lax.rem(position, 2)
    first = position * 2
    moves = (
        (cols_there, cols),
        (tiles_there.at[side], tiles),
        (x_there, x),
        (mass_there, mass),
        (sources_there, sources),
        (tiles_there.at[1 - side], tiles_inner),
    )
    copies = [pltpu.make_async_copy(start, end, arrived.at[i]) for i, (start, end) in enumerate(moves)]
    for copy in copies:
        copy.start()
    for copy in copies[:-1]:
        copy.wait()
    eye = index_of((tile, tile), 0) == index_of((tile, tile), 1)
    outer, _ = outer_block(tile)
    row = index_of(names.shape, 0)
    named = jnp.broadcast_to(sources[...][None, :], names.shape)
    for k in range(slots):
        named = jnp.where(row == k, cols[1 - side, k], named)
    names[...] = named
    mass_0, mass_1 = mass[0:tile][None, :], mass[tile : 2 * tile][None, :]
    masses[...] = jnp.broadcast_to(jnp.where(side == 0, mass_1, mass_0), masses.shape)

    def one_toward(block):
        slot, scale = jnp.int32(0), 0.0
        for k in range(slots):
            found = cols[side, k] == block
            slot, scale = jnp.where(found, k, slot), jnp.where(found, 1.0, scale)
        return scale * tiles[slot]

    own = jnp.where(cols[side, 0] == first + side, tiles[0], 0.0)
    for k in range(1, slots):
        own += jnp.where(cols[side, k] == first + side, tiles[k], 0.0)
    cross = one_toward(first + 1 - side)
    total = row_sums(tiles, jnp.where(side == 0, mass_0, mass_1))
    diag_outer[...] = jnp.broadcast_to(total, diag_outer.shape)
    store_halves(local_outer, (slice(None), slice(0, tile)), jnp.where(side == 0, -own, -cross))
    store_halves(local_outer, (slice(None), slice(tile, 2 * tile)), jnp.where(side == 0, -cross, -own))
    store_halves(t_out_t, (slice(None),), one_toward(jnp.where(side == 0, first - 1, first + 2)).T)
    x_outer = x[outer, :]
    send[0:tile, :] = (
        right_side(named, first + side, x_outer.shape) - total * x_outer - dot(local_outer, x[...])
    )
    push[...] = dot(t_out_t, x_outer)
    above_diagonal = index_of((half, tile), 1) > index_of((half, tile), 0)
    send[tile : tile + half, :] = jnp.where(above_diagonal, own[:half], flip(own[half:]))
    diagonal = jnp.sum(jnp.where(eye, total, 0.0), axis=0, keepdims=True)
    send[tile + half :, :] = jnp.broadcast_to(diagonal, (8, tile))
    copies[-1].wait()


def store_halves(pair, index, value):
    pair[(0, *index)], pair[(1, *index)] = halves(value)


def inner_row_kernel(
    local_outer, diag_outer, x, tiles, names, masses, other_x, send,
    local, diag, t_in, t, q_outer, q_send,
):
    tile = tiles.shape[-1]
    half = tile // 2
    position = place()
    side = lax.rem(position, 2)
    first = position * 2
    outer, inner = outer_block(tile)
    total = row_sums(tiles, masses)
    diag[outer, :] = diag_outer[...]
    diag[inner, :] = jnp.broadcast_to(total, diag_outer.shape)
    own, cross = toward(tiles, names, first + 1 - side), toward(tiles, names, first + side)
    store_halves(local, (inner, slice(0, tile)), jnp.where(side == 0, -cross, -own))
    store_halves(local, (inner, slice(tile, 2 * tile)), jnp.where(side == 0, -own, -cross))
    for k in range(2):
        local[k, outer, :] = local_outer[k]
    store_halves(t_in, (slice(None),), toward(tiles, names, jnp.where(side == 0, first + 2, first - 1)))
    x_inner = x[inner, :]
    t[outer, :] = send[0:tile, :]
    t[inner, :] = (
        right_side(names, first + 1 - side, x_inner.shape)
        - total * x_inner
        - dot(part(local, inner), x[...])
        + dot(t_in, other_x[outer, :])
    )
    q = diag_outer[...] * send[0:tile, :] + dot(local_outer, t[...])
    q_outer[...] = q
    turned = jnp.where(side == 0, flip(q), q)
    first_half = index_of((half, tile), 1) < half
    q_send[...] = jnp.where(first_half, turned[:half], flip(turned[half:]))


def unpack(packed):
    tile = packed.shape[1]
    half = tile // 2
    rows = packed[0:half, :]
    row, column = index_of((half, tile), 0), index_of((half, tile), 1)
    upper = jnp.where(column > row, rows, 0.0)
    lower = flip(jnp.where(column < row, rows, 0.0))
    triangles = jnp.concatenate([upper, lower], axis=0)
    eye = index_of((tile, tile), 0) == index_of((tile, tile), 1)
    diagonal = jnp.sum(jnp.where(eye, packed[half : half + 1, :], 0.0), axis=1, keepdims=True)
    return triangles + triangles.T, diagonal


def outer_columns(tile):
    side = lax.rem(place(), 2)
    return pl.ds(pl.multiple_of(side * tile, tile), tile)


def part(pair, *index):
    return pair[(0, *index)], pair[(1, *index)]


def inner_kernel(local, diag, t_in, t_out_t, t, other_t, q_inner, t_in_t, t_out):
    outer, inner = outer_block(t_in.shape[-1])
    for half in range(2):
        t_in_t[half] = t_in[half].T
        t_out[half] = t_out_t[half].T
    q_inner[...] = (
        diag[inner, :] * t[inner, :] + dot(part(local, inner), t[...]) - dot(t_in, other_t[outer, :])
    )


def image_kernel(local, q_inner, push_here, w_inner):
    tile = q_inner.shape[0]
    _, inner = outer_block(tile)
    w_inner[...] = q_inner[...] + dot(part(local, inner, outer_columns(tile)), push_here[...])


def total(value):
    return jnp.sum(value, axis=0, keepdims=True)


def moment_kernel(
    local, diag, t_in_t, t_out, t_out_t, t, q_outer, push_here, push_there, got, w_inner,
    r, w, there, edge_y_out, edge_r_out, moments, edge_y_in, edge_r_in,
):
    tile = t_out.shape[-1]
    outer, inner = outer_block(tile)
    push_here, push_there = push_here[...], push_there[...]
    r_outer, r_there = t[outer, :] + push_here, got[0:tile, :] + push_there
    pull = dot(t_out, r_there)
    w_outer = (
        q_outer[...]
        + diag[outer, :] * push_here
        + dot(part(local, outer, outer_columns(tile)), push_here)
        - pull
    )
    r[outer, :] = r_outer
    r[inner, :] = t[inner, :]
    w[outer, :] = w_outer
    w[inner, :] = w_inner[...]
    w_now, r_now = w[...], r[...]
    r_r, r_w = total(r_now * r_now), total(r_now * w_now)
    shift = jnp.where(r_r > 0, r_w / r_r, 0.0)
    y = w_now - shift * r_now
    y_outer = w_outer - shift * r_outer
    a_y = diag[...] * y + dot(local, y)
    y_pull, r_pull = total(y_outer * pull), total(r_outer * pull)
    r_ay = total(r_now * a_y + y * w_now) + y_pull
    moments[...] = jnp.concatenate(
        [r_r, r_w, total(y * y), total(y * a_y), r_ay, r_w + r_pull, shift, y_pull, r_pull]
        + [shift] * (moments.shape[0] - 9),
        axis=0,
    )
    back = dot(t_out_t, r_outer)
    edge_r_out[...] = back
    edge_y_out[...] = dot(t_out_t, y_outer)
    own_there, diag_there = unpack(got[tile:, :])
    there[...] = diag_there * push_there - dot(halves(own_there), push_there) - back - shift * r_there
    edge_y_in[...] = dot(t_in_t, w_inner[...] - shift * r[inner, :])
    edge_r_in[...] = dot(t_in_t, r[inner, :])


def share_kernel(
    moments, edge_y_in, edge_r_in, edge_y_out, edge_r_out, there, got_q, other_t, other_w, out
):
    tile = there.shape[0]
    half = tile // 2
    side = lax.rem(place(), 2)
    outer, _ = outer_block(tile)
    shift = moments[6:7, :]
    q_half = got_q[...]
    q_flip = flip(q_half)
    q_there = jnp.concatenate(
        [jnp.where(side == 0, q_half, q_flip), jnp.where(side == 0, q_flip, q_half)], axis=0
    )
    y_there = q_there + there[...]
    mine = (index_of(shift.shape, 1) >= half) == (side == 1)
    weight = jnp.where(mine, 2.0, 0.0)
    y_partner = other_w[...] - shift * other_t[outer, :]
    y_ay = total(edge_y_in[...] * y_partner) + weight * total(edge_y_out[...] * y_there)
    r_ay = total(edge_r_in[...] * y_partner)
    r_ay += weight * (total(edge_r_out[...] * y_there) + moments[7:8, :])
    r_ar = weight * moments[8:9, :]
    sums = moments[0:8, :]
    row = index_of(sums.shape, 0)
    for place_of, value in ((3, y_ay), (4, r_ay), (5, r_ar)):
        sums -= jnp.where(row == place_of, value, 0.0)
    for pair in range(out.shape[1]):
        out[:, pair] = jnp.broadcast_to(sums[None, 2 * pair : 2 * pair + 2], out[:, pair].shape)


def finish_kernel(shares, x, r, w, out):
    r_rs, r_ws, spreads, y_ay, r_ay, r_ar = [shares[:, row // 2, row % 2, :] for row in range(6)]
    r_r = jnp.sum(r_rs, axis=0, keepdims=True)
    r_w = jnp.sum(r_ws, axis=0, keepdims=True)
    theta = r_w / r_r
    off = jnp.where(r_rs > 0, r_ws / r_rs, 0.0) - theta
    spread = jnp.sum(spreads + r_rs * off * off, axis=0, keepdims=True)
    energy = jnp.sum(y_ay + off * (r_ay + off * r_ar), axis=0, keepdims=True)
    ratio = spread / (theta * theta * r_r)
    energy = jnp.maximum(energy - ratio * theta * spread, LEAST_EIGENVALUE * spread * (1.0 + ratio))
    step = jnp.where(spread > 0, spread / energy, 0.0)
    first = 1.0 / theta
    out[...] = x[...] + (first + step * (1.0 + ratio)) * r[...] - (step * first) * w[...]


def call(kernel, shapes, *operands, last=False):
    place_out = jax.ShapeDtypeStruct if last else pltpu.VMEM
    outs = [place_out(shape[1:], shape[0]) for shape in shapes]
    return pl.pallas_call(
        kernel,
        out_shape=outs if len(outs) > 1 else outs[0],
        in_specs=[VMEM] * len(operands),
        out_specs=[VMEM] * len(outs) if len(outs) > 1 else VMEM,
    )(*[pltpu.with_memory_space_constraint(operand, pltpu.VMEM) for operand in operands])


def body(block_cols, step_tiles, mass, warm_start, source_ids):
    tile = step_tiles.shape[-1]
    rows, columns = warm_start.shape
    assert block_cols.shape[0] == 2 and columns == tile
    devices = lax.axis_size("patch") * lax.axis_size("sub")
    partner = [(i, i ^ 1) for i in range(devices)]
    groups = lax.axis_size("groups")
    across = []
    for group in range(groups):
        here, there = group * devices, (group + 1) % groups * devices
        for i in range(1, devices - 1, 2):
            across += [(here + i, here + i + 1), (here + i + 1, here + i)]
        across += [(here, there), (here + devices - 1, there + devices - 1)]
    single, slots = jnp.float32, block_cols.shape[1]
    assert slots < 8
    field, block = (single, rows, columns), (single, tile, columns)
    square, halfway = (jnp.bfloat16, 2, tile, tile), (single, tile // 2, columns)

    def exchange(value):
        return lax.ppermute(value, ("groups",) + AXES, across)

    other_x = lax.ppermute(warm_start, AXES, partner)
    results = [
        (jnp.bfloat16, 2, tile, rows), block, square, field, (single, slots, tile, tile),
        (jnp.int32, 8, tile), (single, 8, tile), block, (single, tile + tile // 2 + 8, columns),
    ]
    local_outer, diag_outer, t_out_t, x, tiles_inner, names, masses, push_there, send = pl.pallas_call(
        outer_kernel,
        out_shape=[pltpu.VMEM(shape[1:], shape[0]) for shape in results],
        in_specs=[pl.BlockSpec(memory_space=pl.ANY)] * 5,
        out_specs=[VMEM] * len(results),
        scratch_shapes=[
            pltpu.SMEM(block_cols.shape, jnp.int32),
            pltpu.VMEM((slots, tile, tile), single),
            pltpu.VMEM(mass.shape, single),
            pltpu.VMEM(source_ids.shape, jnp.int32),
            pltpu.SemaphoreType.DMA((6,)),
        ],
        name="outer_kernel",
    )(block_cols, step_tiles, mass, warm_start, source_ids)
    push_here = exchange(push_there)
    got = exchange(send)
    local, diag, t_in, t, q_outer, q_send = call(
        inner_row_kernel,
        [(jnp.bfloat16, 2, rows, rows), field, square, field, block, halfway],
        local_outer, diag_outer, x, tiles_inner, names, masses, other_x, send,
    )
    got_q = exchange(q_send)
    other_t = lax.ppermute(t, AXES, partner)
    q_inner, t_in_t, t_out = call(
        inner_kernel, [block, square, square], local, diag, t_in, t_out_t, t, other_t
    )
    w_inner = call(image_kernel, [block], local, q_inner, push_here)
    other_w = lax.ppermute(w_inner, AXES, partner)
    r, w, there, edge_y_out, edge_r_out, moments, edge_y_in, edge_r_in = call(
        moment_kernel, [field, field, block, block, block, (single, 16, columns), block, block],
        local, diag, t_in_t, t_out, t_out_t, t, q_outer, push_here, push_there, got, w_inner,
    )
    shares = call(
        share_kernel, [(single, devices, 3, 2, columns)],
        moments, edge_y_in, edge_r_in, edge_y_out, edge_r_out, there, got_q, other_t, other_w,
    )
    shares = lax.all_to_all(shares, AXES, 0, 0)
    return call(finish_kernel, [field], shares, x, r, w, last=True)


def solution(mesh):
    in_specs = (
        P(("groups", "patch", "sub"), None),
        P(("groups", "patch", "sub"), None, None, None),
        P(("groups", "patch", "sub")),
        P(("groups", "patch", "sub"), None),
        P("groups"),
    )
    out_specs = P(("groups", "patch", "sub"), None)
    return jax.shard_map(body, mesh=mesh, in_specs=in_specs, out_specs=out_specs, check_vma=False)
```

```python
import jax
import jax.numpy as jnp
from jax import lax
from jax.experimental import pallas as pl
from jax.experimental.pallas import tpu as pltpu
from jax.sharding import PartitionSpec as P


AXES = ("patch", "sub")
LEAST_EIGENVALUE = 0.0999
VMEM = pl.BlockSpec(memory_space=pltpu.VMEM)


def halves(a):
    high = a.astype(jnp.bfloat16)
    return high, (a - high.astype(jnp.float32)).astype(jnp.bfloat16)


def dot(a, b):
    a_high, a_low = a[0], a[1]
    b_high, b_low = halves(b)

    def product(p, q):
        return jnp.dot(p, q, preferred_element_type=jnp.float32)

    return product(a_high, b_high) + (product(a_high, b_low) + product(a_low, b_high))


def place():
    return lax.axis_index("patch") * lax.axis_size("sub") + lax.axis_index("sub")


def outer_block(tile):
    side = lax.rem(place(), 2)
    outer = pl.ds(pl.multiple_of(side * tile, tile), tile)
    inner = pl.ds(pl.multiple_of((1 - side) * tile, tile), tile)
    return outer, inner


def flip(x):
    return pltpu.roll(x, x.shape[1] // 2, 1)


def index_of(shape, dimension):
    return lax.broadcasted_iota(jnp.int32, shape, dimension)


def toward(tiles, names, block):
    total = jnp.where(names[0:1, :] == block, tiles[0], 0.0)
    for k in range(1, tiles.shape[0]):
        total += jnp.where(names[k : k + 1, :] == block, tiles[k], 0.0)
    return total


def row_sums(tiles, masses):
    tile = tiles.shape[-1]
    whole = tiles[0]
    for k in range(1, tiles.shape[0]):
        whole += tiles[k]
    eye = index_of((tile, tile), 0) == index_of((tile, tile), 1)
    return jnp.sum(whole + jnp.where(eye, masses[0:1, :], 0.0), axis=1, keepdims=True)


def right_side(names, block, shape):
    vertices = block * shape[0] + index_of(shape, 0)
    return jnp.where(vertices == names[7:8, :], 1.0, 0.0)


def outer_kernel(
    cols_there, tiles_there, mass_there, x_there, sources_there,
    local_outer, diag_outer, t_out_t, x, x_inner, tiles_inner, names, masses, push, send,
    cols, tiles, mass, sources, arrived,
):
    tile = tiles.shape[-1]
    half = tile // 2
    slots = tiles.shape[0]
    position = place()
    side = lax.rem(position, 2)
    first = position * 2
    moves = (
        (cols_there, cols),
        (tiles_there.at[side], tiles),
        (x_there, x),
        (mass_there, mass),
        (sources_there, sources),
        (tiles_there.at[1 - side], tiles_inner),
    )
    copies = [pltpu.make_async_copy(start, end, arrived.at[i]) for i, (start, end) in enumerate(moves)]
    for copy in copies:
        copy.start()
    for copy in copies[:-1]:
        copy.wait()
    eye = index_of((tile, tile), 0) == index_of((tile, tile), 1)
    outer, inner = outer_block(tile)
    x_inner[...] = x[inner, :]
    row = index_of(names.shape, 0)
    named = jnp.broadcast_to(sources[...][None, :], names.shape)
    for k in range(slots):
        named = jnp.where(row == k, cols[1 - side, k], named)
    names[...] = named
    mass_0, mass_1 = mass[0:tile][None, :], mass[tile : 2 * tile][None, :]
    masses[...] = jnp.broadcast_to(jnp.where(side == 0, mass_1, mass_0), masses.shape)

    def one_toward(block):
        slot, scale = jnp.int32(0), 0.0
        for k in range(slots):
            found = cols[side, k] == block
            slot, scale = jnp.where(found, k, slot), jnp.where(found, 1.0, scale)
        return scale * tiles[slot]

    own = jnp.where(cols[side, 0] == first + side, tiles[0], 0.0)
    for k in range(1, slots):
        own += jnp.where(cols[side, k] == first + side, tiles[k], 0.0)
    cross = one_toward(first + 1 - side)
    total = row_sums(tiles, jnp.where(side == 0, mass_0, mass_1))
    diag_outer[...] = jnp.broadcast_to(total, diag_outer.shape)
    store_halves(local_outer, (slice(None), slice(0, tile)), jnp.where(side == 0, -own, -cross))
    store_halves(local_outer, (slice(None), slice(tile, 2 * tile)), jnp.where(side == 0, -cross, -own))
    store_halves(t_out_t, (slice(None),), one_toward(jnp.where(side == 0, first - 1, first + 2)).T)
    x_outer = x[outer, :]
    send[0:tile, :] = (
        right_side(named, first + side, x_outer.shape) - total * x_outer - dot(local_outer, x[...])
    )
    push[...] = dot(t_out_t, x_outer)
    above_diagonal = index_of((half, tile), 1) > index_of((half, tile), 0)
    send[tile : tile + half, :] = jnp.where(above_diagonal, own[:half], flip(own[half:]))
    diagonal = jnp.sum(jnp.where(eye, total, 0.0), axis=0, keepdims=True)
    send[tile + half :, :] = jnp.broadcast_to(diagonal, (8, tile))
    copies[-1].wait()


def store_halves(pair, index, value):
    pair[(0, *index)], pair[(1, *index)] = halves(value)


def inner_row_kernel(
    local_outer, diag_outer, x, tiles, names, masses, other_x, send,
    local, diag, t_in, t, t_inner, q_outer, q_send,
):
    tile = tiles.shape[-1]
    half = tile // 2
    position = place()
    side = lax.rem(position, 2)
    first = position * 2
    outer, inner = outer_block(tile)
    total = row_sums(tiles, masses)
    diag[outer, :] = diag_outer[...]
    diag[inner, :] = jnp.broadcast_to(total, diag_outer.shape)
    own, cross = toward(tiles, names, first + 1 - side), toward(tiles, names, first + side)
    store_halves(local, (inner, slice(0, tile)), jnp.where(side == 0, -cross, -own))
    store_halves(local, (inner, slice(tile, 2 * tile)), jnp.where(side == 0, -own, -cross))
    for k in range(2):
        local[k, outer, :] = local_outer[k]
    store_halves(t_in, (slice(None),), toward(tiles, names, jnp.where(side == 0, first + 2, first - 1)))
    x_inner = x[inner, :]
    t[outer, :] = send[0:tile, :]
    t_inner[...] = (
        right_side(names, first + 1 - side, x_inner.shape)
        - total * x_inner
        - dot(part(local, inner), x[...])
        + dot(t_in, other_x[...])
    )
    t[inner, :] = t_inner[...]
    q = diag_outer[...] * send[0:tile, :] + dot(local_outer, t[...])
    q_outer[...] = q
    turned = jnp.where(side == 0, flip(q), q)
    first_half = index_of((half, tile), 1) < half
    q_send[...] = jnp.where(first_half, turned[:half], flip(turned[half:]))


def unpack(packed):
    tile = packed.shape[1]
    half = tile // 2
    rows = packed[0:half, :]
    row, column = index_of((half, tile), 0), index_of((half, tile), 1)
    upper = jnp.where(column > row, rows, 0.0)
    lower = flip(jnp.where(column < row, rows, 0.0))
    triangles = jnp.concatenate([upper, lower], axis=0)
    eye = index_of((tile, tile), 0) == index_of((tile, tile), 1)
    diagonal = jnp.sum(jnp.where(eye, packed[half : half + 1, :], 0.0), axis=1, keepdims=True)
    return triangles + triangles.T, diagonal


def outer_columns(tile):
    side = lax.rem(place(), 2)
    return pl.ds(pl.multiple_of(side * tile, tile), tile)


def part(pair, *index):
    return pair[(0, *index)], pair[(1, *index)]


def inner_kernel(local, diag, t_in, t_out_t, t, other_t, push_here, w_inner, t_in_t, t_out):
    tile = t_in.shape[-1]
    _, inner = outer_block(tile)
    w_inner[...] = (
        diag[inner, :] * t[inner, :]
        + dot(part(local, inner), t[...])
        + dot(part(local, inner, outer_columns(tile)), push_here[...])
        - dot(t_in, other_t[...])
    )
    for half in range(2):
        t_in_t[half] = t_in[half].T
        t_out[half] = t_out_t[half].T


def total(value):
    return jnp.sum(value, axis=0, keepdims=True)


def moment_kernel(
    local, diag, t_in_t, t_out, t_out_t, t, q_outer, push_here, push_there, got, w_inner,
    r, w, there, edge_y_out, edge_r_out, moments, edge_y_in, edge_r_in,
):
    tile = t_out.shape[-1]
    outer, inner = outer_block(tile)
    push_here, push_there = push_here[...], push_there[...]
    r_outer, r_there = t[outer, :] + push_here, got[0:tile, :] + push_there
    pull = dot(t_out, r_there)
    w_outer = (
        q_outer[...]
        + diag[outer, :] * push_here
        + dot(part(local, outer, outer_columns(tile)), push_here)
        - pull
    )
    r[outer, :] = r_outer
    r[inner, :] = t[inner, :]
    w[outer, :] = w_outer
    w[inner, :] = w_inner[...]
    w_now, r_now = w[...], r[...]
    r_r, r_w = total(r_now * r_now), total(r_now * w_now)
    shift = jnp.where(r_r > 0, r_w / r_r, 0.0)
    y = w_now - shift * r_now
    y_outer = w_outer - shift * r_outer
    a_y = diag[...] * y + dot(local, y)
    y_pull, r_pull = total(y_outer * pull), total(r_outer * pull)
    r_ay = total(r_now * a_y + y * w_now) + y_pull
    moments[...] = jnp.concatenate(
        [r_r, r_w, total(y * y), total(y * a_y), r_ay, r_w + r_pull, shift, y_pull, r_pull]
        + [shift] * (moments.shape[0] - 9),
        axis=0,
    )
    back = dot(t_out_t, r_outer)
    edge_r_out[...] = back
    edge_y_out[...] = dot(t_out_t, y_outer)
    own_there, diag_there = unpack(got[tile:, :])
    there[...] = diag_there * push_there - dot(halves(own_there), push_there) - back - shift * r_there
    edge_y_in[...] = dot(t_in_t, w_inner[...] - shift * r[inner, :])
    edge_r_in[...] = dot(t_in_t, r[inner, :])


def share_kernel(
    moments, edge_y_in, edge_r_in, edge_y_out, edge_r_out, there, got_q, other_t, other_w, out
):
    tile = there.shape[0]
    half = tile // 2
    side = lax.rem(place(), 2)
    shift = moments[6:7, :]
    q_half = got_q[...]
    q_flip = flip(q_half)
    q_there = jnp.concatenate(
        [jnp.where(side == 0, q_half, q_flip), jnp.where(side == 0, q_flip, q_half)], axis=0
    )
    y_there = q_there + there[...]
    mine = (index_of(shift.shape, 1) >= half) == (side == 1)
    weight = jnp.where(mine, 2.0, 0.0)
    y_partner = other_w[...] - shift * other_t[...]
    y_ay = total(edge_y_in[...] * y_partner) + weight * total(edge_y_out[...] * y_there)
    r_ay = total(edge_r_in[...] * y_partner)
    r_ay += weight * (total(edge_r_out[...] * y_there) + moments[7:8, :])
    r_ar = weight * moments[8:9, :]
    sums = moments[0:8, :]
    row = index_of(sums.shape, 0)
    for place_of, value in ((3, y_ay), (4, r_ay), (5, r_ar)):
        sums -= jnp.where(row == place_of, value, 0.0)
    for pair in range(out.shape[1]):
        out[:, pair] = jnp.broadcast_to(sums[None, 2 * pair : 2 * pair + 2], out[:, pair].shape)


def finish_kernel(shares, x, r, w, out):
    r_rs, r_ws, spreads, y_ay, r_ay, r_ar = [shares[:, row // 2, row % 2, :] for row in range(6)]
    r_r = jnp.sum(r_rs, axis=0, keepdims=True)
    r_w = jnp.sum(r_ws, axis=0, keepdims=True)
    theta = r_w / r_r
    off = jnp.where(r_rs > 0, r_ws / r_rs, 0.0) - theta
    spread = jnp.sum(spreads + r_rs * off * off, axis=0, keepdims=True)
    energy = jnp.sum(y_ay + off * (r_ay + off * r_ar), axis=0, keepdims=True)
    ratio = spread / (theta * theta * r_r)
    energy = jnp.maximum(energy - ratio * theta * spread, LEAST_EIGENVALUE * spread * (1.0 + ratio))
    step = jnp.where(spread > 0, spread / energy, 0.0)
    first = 1.0 / theta
    out[...] = x[...] + (first + step * (1.0 + ratio)) * r[...] - (step * first) * w[...]


def call(kernel, shapes, *operands, last=False):
    place_out = jax.ShapeDtypeStruct if last else pltpu.VMEM
    outs = [place_out(shape[1:], shape[0]) for shape in shapes]
    return pl.pallas_call(
        kernel,
        out_shape=outs if len(outs) > 1 else outs[0],
        in_specs=[VMEM] * len(operands),
        out_specs=[VMEM] * len(outs) if len(outs) > 1 else VMEM,
    )(*[pltpu.with_memory_space_constraint(operand, pltpu.VMEM) for operand in operands])


def body(block_cols, step_tiles, mass, warm_start, source_ids):
    tile = step_tiles.shape[-1]
    rows, columns = warm_start.shape
    assert block_cols.shape[0] == 2 and columns == tile
    devices = lax.axis_size("patch") * lax.axis_size("sub")
    partner = [(i, i ^ 1) for i in range(devices)]
    groups = lax.axis_size("groups")
    across = []
    for group in range(groups):
        here, there = group * devices, (group + 1) % groups * devices
        for i in range(1, devices - 1, 2):
            across += [(here + i, here + i + 1), (here + i + 1, here + i)]
        across += [(here, there), (here + devices - 1, there + devices - 1)]
    single, slots = jnp.float32, block_cols.shape[1]
    assert slots < 8
    field, block = (single, rows, columns), (single, tile, columns)
    square, halfway = (jnp.bfloat16, 2, tile, tile), (single, tile // 2, columns)

    def exchange(value):
        return lax.ppermute(value, ("groups",) + AXES, across)

    results = [
        (jnp.bfloat16, 2, tile, rows), block, square, field, block, (single, slots, tile, tile),
        (jnp.int32, 8, tile), (single, 8, tile), block, (single, tile + tile // 2 + 8, columns),
    ]
    local_outer, diag_outer, t_out_t, x, x_inner, tiles_inner, names, masses, push_there, send = pl.pallas_call(
        outer_kernel,
        out_shape=[pltpu.VMEM(shape[1:], shape[0]) for shape in results],
        in_specs=[pl.BlockSpec(memory_space=pl.ANY)] * 5,
        out_specs=[VMEM] * len(results),
        scratch_shapes=[
            pltpu.SMEM(block_cols.shape, jnp.int32),
            pltpu.VMEM((slots, tile, tile), single),
            pltpu.VMEM(mass.shape, single),
            pltpu.VMEM(source_ids.shape, jnp.int32),
            pltpu.SemaphoreType.DMA((6,)),
        ],
        name="outer_kernel",
    )(block_cols, step_tiles, mass, warm_start, source_ids)
    push_here = exchange(push_there)
    other_x = lax.ppermute(x_inner, AXES, partner)
    got = exchange(send)
    local, diag, t_in, t, t_inner, q_outer, q_send = call(
        inner_row_kernel,
        [(jnp.bfloat16, 2, rows, rows), field, square, field, block, block, halfway],
        local_outer, diag_outer, x, tiles_inner, names, masses, other_x, send,
    )
    got_q = exchange(q_send)
    other_t = lax.ppermute(t_inner, AXES, partner)
    w_inner, t_in_t, t_out = call(
        inner_kernel, [block, square, square], local, diag, t_in, t_out_t, t, other_t, push_here
    )
    other_w = lax.ppermute(w_inner, AXES, partner)
    r, w, there, edge_y_out, edge_r_out, moments, edge_y_in, edge_r_in = call(
        moment_kernel, [field, field, block, block, block, (single, 16, columns), block, block],
        local, diag, t_in_t, t_out, t_out_t, t, q_outer, push_here, push_there, got, w_inner,
    )
    shares = call(
        share_kernel, [(single, devices, 3, 2, columns)],
        moments, edge_y_in, edge_r_in, edge_y_out, edge_r_out, there, got_q, other_t, other_w,
    )
    shares = lax.all_to_all(shares, AXES, 0, 0)
    return call(finish_kernel, [field], shares, x, r, w, last=True)


def solution(mesh):
    in_specs = (
        P(("groups", "patch", "sub"), None),
        P(("groups", "patch", "sub"), None, None, None),
        P(("groups", "patch", "sub")),
        P(("groups", "patch", "sub"), None),
        P("groups"),
    )
    out_specs = P(("groups", "patch", "sub"), None)
    return jax.shard_map(body, mesh=mesh, in_specs=in_specs, out_specs=out_specs, check_vma=False)
```

```python
import jax
import jax.numpy as jnp
from jax import lax
from jax.experimental import pallas as pl
from jax.experimental.pallas import tpu as pltpu
from jax.sharding import PartitionSpec as P


AXES = ("patch", "sub")
LEAST_EIGENVALUE = 0.0999
VMEM = pl.BlockSpec(memory_space=pltpu.VMEM)


def halves(a):
    high = a.astype(jnp.bfloat16)
    return high, (a - high.astype(jnp.float32)).astype(jnp.bfloat16)


def dot(a, b):
    a_high, a_low = a[0], a[1]
    b_high, b_low = halves(b)

    def product(p, q):
        return jnp.dot(p, q, preferred_element_type=jnp.float32)

    return product(a_high, b_high) + (product(a_high, b_low) + product(a_low, b_high))


def place():
    return lax.axis_index("patch") * lax.axis_size("sub") + lax.axis_index("sub")


def outer_block(tile):
    side = lax.rem(place(), 2)
    outer = pl.ds(pl.multiple_of(side * tile, tile), tile)
    inner = pl.ds(pl.multiple_of((1 - side) * tile, tile), tile)
    return outer, inner


def flip(x):
    return pltpu.roll(x, x.shape[1] // 2, 1)


def index_of(shape, dimension):
    return lax.broadcasted_iota(jnp.int32, shape, dimension)


def toward(tiles, names, block):
    total = jnp.where(names[0:1, :] == block, tiles[0], 0.0)
    for k in range(1, tiles.shape[0]):
        total += jnp.where(names[k : k + 1, :] == block, tiles[k], 0.0)
    return total


def row_sums(tiles, masses):
    tile = tiles.shape[-1]
    whole = tiles[0]
    for k in range(1, tiles.shape[0]):
        whole += tiles[k]
    eye = index_of((tile, tile), 0) == index_of((tile, tile), 1)
    return jnp.sum(whole + jnp.where(eye, masses[0:1, :], 0.0), axis=1, keepdims=True)


def right_side(names, block, shape):
    vertices = block * shape[0] + index_of(shape, 0)
    return jnp.where(vertices == names[7:8, :], 1.0, 0.0)


def outer_kernel(
    cols_there, tiles_there, mass_there, x_there, sources_there,
    local_outer, diag_outer, t_out_t, x, x_inner, tiles_inner, names, masses, push, send,
    cols, tiles, mass, sources, arrived,
):
    tile = tiles.shape[-1]
    half = tile // 2
    slots = tiles.shape[0]
    position = place()
    side = lax.rem(position, 2)
    first = position * 2
    moves = (
        (cols_there, cols),
        (tiles_there.at[side], tiles),
        (x_there, x),
        (mass_there, mass),
        (sources_there, sources),
        (tiles_there.at[1 - side], tiles_inner),
    )
    copies = [pltpu.make_async_copy(start, end, arrived.at[i]) for i, (start, end) in enumerate(moves)]
    for copy in copies:
        copy.start()
    for copy in copies[:-1]:
        copy.wait()
    eye = index_of((tile, tile), 0) == index_of((tile, tile), 1)
    outer, inner = outer_block(tile)
    x_inner[...] = x[inner, :]
    row = index_of(names.shape, 0)
    named = jnp.broadcast_to(sources[...][None, :], names.shape)
    for k in range(slots):
        named = jnp.where(row == k, cols[1 - side, k], named)
    names[...] = named
    mass_0, mass_1 = mass[0:tile][None, :], mass[tile : 2 * tile][None, :]
    masses[...] = jnp.broadcast_to(jnp.where(side == 0, mass_1, mass_0), masses.shape)

    def one_toward(block):
        slot, scale = jnp.int32(0), 0.0
        for k in range(slots):
            found = cols[side, k] == block
            slot, scale = jnp.where(found, k, slot), jnp.where(found, 1.0, scale)
        return scale * tiles[slot]

    own = jnp.where(cols[side, 0] == first + side, tiles[0], 0.0)
    for k in range(1, slots):
        own += jnp.where(cols[side, k] == first + side, tiles[k], 0.0)
    cross = one_toward(first + 1 - side)
    total = row_sums(tiles, jnp.where(side == 0, mass_0, mass_1))
    diag_outer[...] = jnp.broadcast_to(total, diag_outer.shape)
    store_halves(local_outer, (slice(None), slice(0, tile)), jnp.where(side == 0, -own, -cross))
    store_halves(local_outer, (slice(None), slice(tile, 2 * tile)), jnp.where(side == 0, -cross, -own))
    store_halves(t_out_t, (slice(None),), one_toward(jnp.where(side == 0, first - 1, first + 2)).T)
    x_outer = x[outer, :]
    send[0:tile, :] = (
        right_side(named, first + side, x_outer.shape) - total * x_outer - dot(local_outer, x[...])
    )
    push[...] = dot(t_out_t, x_outer)
    above_diagonal = index_of((half, tile), 1) > index_of((half, tile), 0)
    send[tile : tile + half, :] = jnp.where(above_diagonal, own[:half], flip(own[half:]))
    diagonal = jnp.sum(jnp.where(eye, total, 0.0), axis=0, keepdims=True)
    send[tile + half :, :] = jnp.broadcast_to(diagonal, (8, tile))
    copies[-1].wait()


def store_halves(pair, index, value):
    pair[(0, *index)], pair[(1, *index)] = halves(value)


def inner_row_kernel(
    local_outer, diag_outer, x, tiles, names, masses, other_x, send,
    local, diag, t_in, t, t_inner, q_outer, q_send,
):
    tile = tiles.shape[-1]
    half = tile // 2
    position = place()
    side = lax.rem(position, 2)
    first = position * 2
    outer, inner = outer_block(tile)
    total = row_sums(tiles, masses)
    diag[outer, :] = diag_outer[...]
    diag[inner, :] = jnp.broadcast_to(total, diag_outer.shape)
    own, cross = toward(tiles, names, first + 1 - side), toward(tiles, names, first + side)
    store_halves(local, (inner, slice(0, tile)), jnp.where(side == 0, -cross, -own))
    store_halves(local, (inner, slice(tile, 2 * tile)), jnp.where(side == 0, -own, -cross))
    for k in range(2):
        local[k, outer, :] = local_outer[k]
    store_halves(t_in, (slice(None),), toward(tiles, names, jnp.where(side == 0, first + 2, first - 1)))
    x_inner = x[inner, :]
    t[outer, :] = send[0:tile, :]
    t_inner[...] = (
        right_side(names, first + 1 - side, x_inner.shape)
        - total * x_inner
        - dot(part(local, inner), x[...])
        + dot(t_in, other_x[...])
    )
    t[inner, :] = t_inner[...]
    q = (
        diag_outer[...] * send[0:tile, :]
        + dot(part(local_outer, slice(None), outer_columns(tile)), send[0:tile, :])
        + dot(part(local_outer, slice(None), inner_columns(tile)), t_inner[...])
    )
    q_outer[...] = q
    turned = jnp.where(side == 0, flip(q), q)
    first_half = index_of((half, tile), 1) < half
    q_send[...] = jnp.where(first_half, turned[:half], flip(turned[half:]))


def unpack(packed):
    tile = packed.shape[1]
    half = tile // 2
    rows = packed[0:half, :]
    row, column = index_of((half, tile), 0), index_of((half, tile), 1)
    upper = jnp.where(column > row, rows, 0.0)
    lower = flip(jnp.where(column < row, rows, 0.0))
    triangles = jnp.concatenate([upper, lower], axis=0)
    eye = index_of((tile, tile), 0) == index_of((tile, tile), 1)
    diagonal = jnp.sum(jnp.where(eye, packed[half : half + 1, :], 0.0), axis=1, keepdims=True)
    return triangles + triangles.T, diagonal


def outer_columns(tile):
    side = lax.rem(place(), 2)
    return pl.ds(pl.multiple_of(side * tile, tile), tile)


def inner_columns(tile):
    side = lax.rem(place(), 2)
    return pl.ds(pl.multiple_of((1 - side) * tile, tile), tile)


def part(pair, *index):
    return pair[(0, *index)], pair[(1, *index)]


def inner_kernel(local, diag, t_in, t_out_t, t, other_t, push_here, w_inner, t_in_t, t_out):
    tile = t_in.shape[-1]
    _, inner = outer_block(tile)
    w_inner[...] = (
        diag[inner, :] * t[inner, :]
        + dot(part(local, inner), t[...])
        + dot(part(local, inner, outer_columns(tile)), push_here[...])
        - dot(t_in, other_t[...])
    )
    for half in range(2):
        t_in_t[half] = t_in[half].T
        t_out[half] = t_out_t[half].T


def total(value):
    return jnp.sum(value, axis=0, keepdims=True)


def moment_kernel(
    local, diag, t_in_t, t_out, t_out_t, t, q_outer, push_here, push_there, got, w_inner,
    r, w, there, edge_y_out, edge_r_out, moments, edge_y_in, edge_r_in,
):
    tile = t_out.shape[-1]
    outer, inner = outer_block(tile)
    push_here, push_there = push_here[...], push_there[...]
    r_outer, r_there = t[outer, :] + push_here, got[0:tile, :] + push_there
    pull = dot(t_out, r_there)
    w_outer = (
        q_outer[...]
        + diag[outer, :] * push_here
        + dot(part(local, outer, outer_columns(tile)), push_here)
        - pull
    )
    r[outer, :] = r_outer
    r[inner, :] = t[inner, :]
    w[outer, :] = w_outer
    w[inner, :] = w_inner[...]
    w_now, r_now = w[...], r[...]
    r_r, r_w = total(r_now * r_now), total(r_now * w_now)
    shift = jnp.where(r_r > 0, r_w / r_r, 0.0)
    y = w_now - shift * r_now
    y_outer = w_outer - shift * r_outer
    a_y = diag[...] * y + dot(local, y)
    y_pull, r_pull = total(y_outer * pull), total(r_outer * pull)
    r_ay = total(r_now * a_y + y * w_now) + y_pull
    moments[...] = jnp.concatenate(
        [r_r, r_w, total(y * y), total(y * a_y), r_ay, r_w + r_pull, shift, y_pull, r_pull]
        + [shift] * (moments.shape[0] - 9),
        axis=0,
    )
    back = dot(t_out_t, r_outer)
    edge_r_out[...] = back
    edge_y_out[...] = dot(t_out_t, y_outer)
    own_there, diag_there = unpack(got[tile:, :])
    there[...] = diag_there * push_there - dot(halves(own_there), push_there) - back - shift * r_there
    edge_y_in[...] = dot(t_in_t, w_inner[...] - shift * r[inner, :])
    edge_r_in[...] = dot(t_in_t, r[inner, :])


def share_kernel(
    moments, edge_y_in, edge_r_in, edge_y_out, edge_r_out, there, got_q, other_t, other_w, out
):
    tile = there.shape[0]
    half = tile // 2
    side = lax.rem(place(), 2)
    shift = moments[6:7, :]
    q_half = got_q[...]
    q_flip = flip(q_half)
    q_there = jnp.concatenate(
        [jnp.where(side == 0, q_half, q_flip), jnp.where(side == 0, q_flip, q_half)], axis=0
    )
    y_there = q_there + there[...]
    mine = (index_of(shift.shape, 1) >= half) == (side == 1)
    weight = jnp.where(mine, 2.0, 0.0)
    y_partner = other_w[...] - shift * other_t[...]
    y_ay = total(edge_y_in[...] * y_partner) + weight * total(edge_y_out[...] * y_there)
    r_ay = total(edge_r_in[...] * y_partner)
    r_ay += weight * (total(edge_r_out[...] * y_there) + moments[7:8, :])
    r_ar = weight * moments[8:9, :]
    sums = moments[0:8, :]
    row = index_of(sums.shape, 0)
    for place_of, value in ((3, y_ay), (4, r_ay), (5, r_ar)):
        sums -= jnp.where(row == place_of, value, 0.0)
    for pair in range(out.shape[1]):
        out[:, pair] = jnp.broadcast_to(sums[None, 2 * pair : 2 * pair + 2], out[:, pair].shape)


def finish_kernel(shares, x, r, w, out):
    r_rs, r_ws, spreads, y_ay, r_ay, r_ar = [shares[:, row // 2, row % 2, :] for row in range(6)]
    r_r = jnp.sum(r_rs, axis=0, keepdims=True)
    r_w = jnp.sum(r_ws, axis=0, keepdims=True)
    theta = r_w / r_r
    off = jnp.where(r_rs > 0, r_ws / r_rs, 0.0) - theta
    spread = jnp.sum(spreads + r_rs * off * off, axis=0, keepdims=True)
    energy = jnp.sum(y_ay + off * (r_ay + off * r_ar), axis=0, keepdims=True)
    ratio = spread / (theta * theta * r_r)
    energy = jnp.maximum(energy - ratio * theta * spread, LEAST_EIGENVALUE * spread * (1.0 + ratio))
    step = jnp.where(spread > 0, spread / energy, 0.0)
    first = 1.0 / theta
    out[...] = x[...] + (first + step * (1.0 + ratio)) * r[...] - (step * first) * w[...]


def call(kernel, shapes, *operands, last=False):
    place_out = jax.ShapeDtypeStruct if last else pltpu.VMEM
    outs = [place_out(shape[1:], shape[0]) for shape in shapes]
    return pl.pallas_call(
        kernel,
        out_shape=outs if len(outs) > 1 else outs[0],
        in_specs=[VMEM] * len(operands),
        out_specs=[VMEM] * len(outs) if len(outs) > 1 else VMEM,
    )(*[pltpu.with_memory_space_constraint(operand, pltpu.VMEM) for operand in operands])


def body(block_cols, step_tiles, mass, warm_start, source_ids):
    tile = step_tiles.shape[-1]
    rows, columns = warm_start.shape
    assert block_cols.shape[0] == 2 and columns == tile
    devices = lax.axis_size("patch") * lax.axis_size("sub")
    partner = [(i, i ^ 1) for i in range(devices)]
    groups = lax.axis_size("groups")
    across = []
    for group in range(groups):
        here, there = group * devices, (group + 1) % groups * devices
        for i in range(1, devices - 1, 2):
            across += [(here + i, here + i + 1), (here + i + 1, here + i)]
        across += [(here, there), (here + devices - 1, there + devices - 1)]
    single, slots = jnp.float32, block_cols.shape[1]
    assert slots < 8
    field, block = (single, rows, columns), (single, tile, columns)
    square, halfway = (jnp.bfloat16, 2, tile, tile), (single, tile // 2, columns)

    def exchange(value):
        return lax.ppermute(value, ("groups",) + AXES, across)

    results = [
        (jnp.bfloat16, 2, tile, rows), block, square, field, block, (single, slots, tile, tile),
        (jnp.int32, 8, tile), (single, 8, tile), block, (single, tile + tile // 2 + 8, columns),
    ]
    local_outer, diag_outer, t_out_t, x, x_inner, tiles_inner, names, masses, push_there, send = pl.pallas_call(
        outer_kernel,
        out_shape=[pltpu.VMEM(shape[1:], shape[0]) for shape in results],
        in_specs=[pl.BlockSpec(memory_space=pl.ANY)] * 5,
        out_specs=[VMEM] * len(results),
        scratch_shapes=[
            pltpu.SMEM(block_cols.shape, jnp.int32),
            pltpu.VMEM((slots, tile, tile), single),
            pltpu.VMEM(mass.shape, single),
            pltpu.VMEM(source_ids.shape, jnp.int32),
            pltpu.SemaphoreType.DMA((6,)),
        ],
        name="outer_kernel",
    )(block_cols, step_tiles, mass, warm_start, source_ids)
    push_here = exchange(push_there)
    other_x = lax.ppermute(x_inner, AXES, partner)
    got = exchange(send)
    local, diag, t_in, t, t_inner, q_outer, q_send = call(
        inner_row_kernel,
        [(jnp.bfloat16, 2, rows, rows), field, square, field, block, block, halfway],
        local_outer, diag_outer, x, tiles_inner, names, masses, other_x, send,
    )
    got_q = exchange(q_send)
    other_t = lax.ppermute(t_inner, AXES, partner)
    w_inner, t_in_t, t_out = call(
        inner_kernel, [block, square, square], local, diag, t_in, t_out_t, t, other_t, push_here
    )
    other_w = lax.ppermute(w_inner, AXES, partner)
    r, w, there, edge_y_out, edge_r_out, moments, edge_y_in, edge_r_in = call(
        moment_kernel, [field, field, block, block, block, (single, 16, columns), block, block],
        local, diag, t_in_t, t_out, t_out_t, t, q_outer, push_here, push_there, got, w_inner,
    )
    shares = call(
        share_kernel, [(single, devices, 3, 2, columns)],
        moments, edge_y_in, edge_r_in, edge_y_out, edge_r_out, there, got_q, other_t, other_w,
    )
    shares = lax.all_to_all(shares, AXES, 0, 0)
    return call(finish_kernel, [field], shares, x, r, w, last=True)


def solution(mesh):
    in_specs = (
        P(("groups", "patch", "sub"), None),
        P(("groups", "patch", "sub"), None, None, None),
        P(("groups", "patch", "sub")),
        P(("groups", "patch", "sub"), None),
        P("groups"),
    )
    out_specs = P(("groups", "patch", "sub"), None)
    return jax.shard_map(body, mesh=mesh, in_specs=in_specs, out_specs=out_specs, check_vma=False)
```

```python
import jax
import jax.numpy as jnp
from jax import lax
from jax.experimental import pallas as pl
from jax.experimental.pallas import tpu as pltpu
from jax.sharding import PartitionSpec as P


AXES = ("patch", "sub")
LEAST_EIGENVALUE = 0.0999
VMEM = pl.BlockSpec(memory_space=pltpu.VMEM)


def halves(a):
    high = a.astype(jnp.bfloat16)
    return high, (a - high.astype(jnp.float32)).astype(jnp.bfloat16)


def dot(a, b):
    a_high, a_low = a[0], a[1]
    b_high, b_low = halves(b)

    def product(p, q):
        return jnp.dot(p, q, preferred_element_type=jnp.float32)

    return product(a_high, b_high) + (product(a_high, b_low) + product(a_low, b_high))


def place():
    return lax.axis_index("patch") * lax.axis_size("sub") + lax.axis_index("sub")


def outer_block(tile):
    side = lax.rem(place(), 2)
    outer = pl.ds(pl.multiple_of(side * tile, tile), tile)
    inner = pl.ds(pl.multiple_of((1 - side) * tile, tile), tile)
    return outer, inner


def flip(x):
    return pltpu.roll(x, x.shape[1] // 2, 1)


def index_of(shape, dimension):
    return lax.broadcasted_iota(jnp.int32, shape, dimension)


def toward(tiles, names, block):
    total = jnp.where(names[0:1, :] == block, tiles[0], 0.0)
    for k in range(1, tiles.shape[0]):
        total += jnp.where(names[k : k + 1, :] == block, tiles[k], 0.0)
    return total


def row_sums(tiles, masses):
    tile = tiles.shape[-1]
    whole = tiles[0]
    for k in range(1, tiles.shape[0]):
        whole += tiles[k]
    eye = index_of((tile, tile), 0) == index_of((tile, tile), 1)
    return jnp.sum(whole + jnp.where(eye, masses[0:1, :], 0.0), axis=1, keepdims=True)


def right_side(names, block, shape):
    vertices = block * shape[0] + index_of(shape, 0)
    return jnp.where(vertices == names[7:8, :], 1.0, 0.0)


def outer_kernel(
    cols_there, tiles_there, mass_there, x_there, sources_there,
    local_outer, diag_outer, t_out_t, x, x_inner, tiles_inner, names, masses, push, send,
    cols, tiles, mass, sources, arrived,
):
    tile = tiles.shape[-1]
    half = tile // 2
    slots = tiles.shape[0]
    position = place()
    side = lax.rem(position, 2)
    first = position * 2
    moves = (
        (cols_there, cols),
        (tiles_there.at[side], tiles),
        (x_there, x),
        (mass_there, mass),
        (sources_there, sources),
        (tiles_there.at[1 - side], tiles_inner),
    )
    copies = [pltpu.make_async_copy(start, end, arrived.at[i]) for i, (start, end) in enumerate(moves)]
    for copy in copies:
        copy.start()
    for copy in copies[:-1]:
        copy.wait()
    eye = index_of((tile, tile), 0) == index_of((tile, tile), 1)
    outer, inner = outer_block(tile)
    x_inner[...] = x[inner, :]
    row = index_of(names.shape, 0)
    named = jnp.broadcast_to(sources[...][None, :], names.shape)
    for k in range(slots):
        named = jnp.where(row == k, cols[1 - side, k], named)
    names[...] = named
    mass_0, mass_1 = mass[0:tile][None, :], mass[tile : 2 * tile][None, :]
    masses[...] = jnp.broadcast_to(jnp.where(side == 0, mass_1, mass_0), masses.shape)

    def one_toward(block):
        slot, scale = jnp.int32(0), 0.0
        for k in range(slots):
            found = cols[side, k] == block
            slot, scale = jnp.where(found, k, slot), jnp.where(found, 1.0, scale)
        return scale * tiles[slot]

    own = jnp.where(cols[side, 0] == first + side, tiles[0], 0.0)
    for k in range(1, slots):
        own += jnp.where(cols[side, k] == first + side, tiles[k], 0.0)
    cross = one_toward(first + 1 - side)
    total = row_sums(tiles, jnp.where(side == 0, mass_0, mass_1))
    diag_outer[...] = jnp.broadcast_to(total, diag_outer.shape)
    store_halves(local_outer, (slice(None), slice(0, tile)), jnp.where(side == 0, -own, -cross))
    store_halves(local_outer, (slice(None), slice(tile, 2 * tile)), jnp.where(side == 0, -cross, -own))
    store_halves(t_out_t, (slice(None),), one_toward(jnp.where(side == 0, first - 1, first + 2)).T)
    x_outer = x[outer, :]
    send[0:tile, :] = (
        right_side(named, first + side, x_outer.shape) - total * x_outer - dot(local_outer, x[...])
    )
    push[...] = dot(t_out_t, x_outer)
    above_diagonal = index_of((half, tile), 1) > index_of((half, tile), 0)
    send[tile : tile + half, :] = jnp.where(above_diagonal, own[:half], flip(own[half:]))
    diagonal = jnp.sum(jnp.where(eye, total, 0.0), axis=0, keepdims=True)
    send[tile + half :, :] = jnp.broadcast_to(diagonal, (8, tile))
    copies[-1].wait()


def store_halves(pair, index, value):
    pair[(0, *index)], pair[(1, *index)] = halves(value)


def inner_row_kernel(
    local_outer, diag_outer, x, tiles, names, masses, other_x, send,
    local, diag, t_in, t, t_inner, q_outer, q_send,
):
    tile = tiles.shape[-1]
    half = tile // 2
    position = place()
    side = lax.rem(position, 2)
    first = position * 2
    outer, inner = outer_block(tile)
    total = row_sums(tiles, masses)
    diag[outer, :] = diag_outer[...]
    diag[inner, :] = jnp.broadcast_to(total, diag_outer.shape)
    own, cross = toward(tiles, names, first + 1 - side), toward(tiles, names, first + side)
    store_halves(local, (inner, slice(0, tile)), jnp.where(side == 0, -cross, -own))
    store_halves(local, (inner, slice(tile, 2 * tile)), jnp.where(side == 0, -own, -cross))
    for k in range(2):
        local[k, outer, :] = local_outer[k]
    store_halves(t_in, (slice(None),), toward(tiles, names, jnp.where(side == 0, first + 2, first - 1)))
    x_inner = x[inner, :]
    t[outer, :] = send[0:tile, :]
    t_inner[...] = (
        right_side(names, first + 1 - side, x_inner.shape)
        - total * x_inner
        - dot(part(local, inner), x[...])
        + dot(t_in, other_x[...])
    )
    t[inner, :] = t_inner[...]
    q = (
        diag_outer[...] * send[0:tile, :]
        + dot(part(local_outer, slice(None), outer_columns(tile)), send[0:tile, :])
        + dot(part(local_outer, slice(None), inner_columns(tile)), t_inner[...])
    )
    q_outer[...] = q
    turned = jnp.where(side == 0, flip(q), q)
    first_half = index_of((half, tile), 1) < half
    q_send[...] = jnp.where(first_half, turned[:half], flip(turned[half:]))


def unpack(packed):
    tile = packed.shape[1]
    half = tile // 2
    rows = packed[0:half, :]
    row, column = index_of((half, tile), 0), index_of((half, tile), 1)
    upper = jnp.where(column > row, rows, 0.0)
    lower = flip(jnp.where(column < row, rows, 0.0))
    triangles = jnp.concatenate([upper, lower], axis=0)
    eye = index_of((tile, tile), 0) == index_of((tile, tile), 1)
    diagonal = jnp.sum(jnp.where(eye, packed[half : half + 1, :], 0.0), axis=1, keepdims=True)
    return triangles + triangles.T, diagonal


def outer_columns(tile):
    side = lax.rem(place(), 2)
    return pl.ds(pl.multiple_of(side * tile, tile), tile)


def inner_columns(tile):
    side = lax.rem(place(), 2)
    return pl.ds(pl.multiple_of((1 - side) * tile, tile), tile)


def part(pair, *index):
    return pair[(0, *index)], pair[(1, *index)]


def inner_kernel(local, diag, t_in, t_out_t, t, other_t, push_here, w_inner, t_in_t, t_out):
    tile = t_in.shape[-1]
    _, inner = outer_block(tile)
    w_inner[...] = (
        diag[inner, :] * t[inner, :]
        + dot(part(local, inner), t[...])
        + dot(part(local, inner, outer_columns(tile)), push_here[...])
        - dot(t_in, other_t[...])
    )
    for half in range(2):
        t_in_t[half] = t_in[half].T
        t_out[half] = t_out_t[half].T


def total(value):
    return jnp.sum(value, axis=0, keepdims=True)


def residual_kernel(local, diag, t_in_t, t_out_t, t, q_outer, push_here, r, w_outer, edge_r_out, edge_r_in):
    tile = t_in_t.shape[-1]
    outer, inner = outer_block(tile)
    push = push_here[...]
    r_outer = t[outer, :] + push
    r[outer, :] = r_outer
    r[inner, :] = t[inner, :]
    w_outer[...] = q_outer[...] + diag[outer, :] * push + dot(part(local, outer, outer_columns(tile)), push)
    edge_r_out[...] = dot(t_out_t, r_outer)
    edge_r_in[...] = dot(t_in_t, t[inner, :])


def moment_kernel(
    local, diag, t_in_t, t_out, t_out_t, r, w_local, edge_r_out, push_there, got, w_inner,
    w, there, edge_y_out, moments, edge_y_in,
):
    tile = t_out.shape[-1]
    outer, inner = outer_block(tile)
    push = push_there[...]
    r_outer, r_there = r[outer, :], got[0:tile, :] + push
    pull = dot(t_out, r_there)
    w_outer = w_local[...] - pull
    w[outer, :] = w_outer
    w[inner, :] = w_inner[...]
    w_now, r_now = w[...], r[...]
    r_r, r_w = total(r_now * r_now), total(r_now * w_now)
    shift = jnp.where(r_r > 0, r_w / r_r, 0.0)
    y = w_now - shift * r_now
    y_outer = w_outer - shift * r_outer
    a_y = diag[...] * y + dot(local, y)
    y_pull, r_pull = total(y_outer * pull), total(r_outer * pull)
    r_ay = total(r_now * a_y + y * w_now) + y_pull
    moments[...] = jnp.concatenate(
        [r_r, r_w, total(y * y), total(y * a_y), r_ay, r_w + r_pull, shift, y_pull, r_pull]
        + [shift] * (moments.shape[0] - 9),
        axis=0,
    )
    edge_y_out[...] = dot(t_out_t, y_outer)
    own_there, diag_there = unpack(got[tile:, :])
    there[...] = diag_there * push - dot(halves(own_there), push) - edge_r_out[...] - shift * r_there
    edge_y_in[...] = dot(t_in_t, w_inner[...] - shift * r[inner, :])


def share_kernel(
    moments, edge_y_in, edge_r_in, edge_y_out, edge_r_out, there, got_q, other_t, other_w, out
):
    tile = there.shape[0]
    half = tile // 2
    side = lax.rem(place(), 2)
    shift = moments[6:7, :]
    q_half = got_q[...]
    q_flip = flip(q_half)
    q_there = jnp.concatenate(
        [jnp.where(side == 0, q_half, q_flip), jnp.where(side == 0, q_flip, q_half)], axis=0
    )
    y_there = q_there + there[...]
    mine = (index_of(shift.shape, 1) >= half) == (side == 1)
    weight = jnp.where(mine, 2.0, 0.0)
    y_partner = other_w[...] - shift * other_t[...]
    y_ay = total(edge_y_in[...] * y_partner) + weight * total(edge_y_out[...] * y_there)
    r_ay = total(edge_r_in[...] * y_partner)
    r_ay += weight * (total(edge_r_out[...] * y_there) + moments[7:8, :])
    r_ar = weight * moments[8:9, :]
    sums = moments[0:8, :]
    row = index_of(sums.shape, 0)
    for place_of, value in ((3, y_ay), (4, r_ay), (5, r_ar)):
        sums -= jnp.where(row == place_of, value, 0.0)
    for pair in range(out.shape[1]):
        out[:, pair] = jnp.broadcast_to(sums[None, 2 * pair : 2 * pair + 2], out[:, pair].shape)


def finish_kernel(shares, x, r, w, out):
    r_rs, r_ws, spreads, y_ay, r_ay, r_ar = [shares[:, row // 2, row % 2, :] for row in range(6)]
    r_r = jnp.sum(r_rs, axis=0, keepdims=True)
    r_w = jnp.sum(r_ws, axis=0, keepdims=True)
    theta = r_w / r_r
    off = jnp.where(r_rs > 0, r_ws / r_rs, 0.0) - theta
    spread = jnp.sum(spreads + r_rs * off * off, axis=0, keepdims=True)
    energy = jnp.sum(y_ay + off * (r_ay + off * r_ar), axis=0, keepdims=True)
    ratio = spread / (theta * theta * r_r)
    energy = jnp.maximum(energy - ratio * theta * spread, LEAST_EIGENVALUE * spread * (1.0 + ratio))
    step = jnp.where(spread > 0, spread / energy, 0.0)
    first = 1.0 / theta
    out[...] = x[...] + (first + step * (1.0 + ratio)) * r[...] - (step * first) * w[...]


def call(kernel, shapes, *operands, last=False):
    place_out = jax.ShapeDtypeStruct if last else pltpu.VMEM
    outs = [place_out(shape[1:], shape[0]) for shape in shapes]
    return pl.pallas_call(
        kernel,
        out_shape=outs if len(outs) > 1 else outs[0],
        in_specs=[VMEM] * len(operands),
        out_specs=[VMEM] * len(outs) if len(outs) > 1 else VMEM,
    )(*[pltpu.with_memory_space_constraint(operand, pltpu.VMEM) for operand in operands])


def body(block_cols, step_tiles, mass, warm_start, source_ids):
    tile = step_tiles.shape[-1]
    rows, columns = warm_start.shape
    assert block_cols.shape[0] == 2 and columns == tile
    devices = lax.axis_size("patch") * lax.axis_size("sub")
    partner = [(i, i ^ 1) for i in range(devices)]
    groups = lax.axis_size("groups")
    across = []
    for group in range(groups):
        here, there = group * devices, (group + 1) % groups * devices
        for i in range(1, devices - 1, 2):
            across += [(here + i, here + i + 1), (here + i + 1, here + i)]
        across += [(here, there), (here + devices - 1, there + devices - 1)]
    single, slots = jnp.float32, block_cols.shape[1]
    assert slots < 8
    field, block = (single, rows, columns), (single, tile, columns)
    square, halfway = (jnp.bfloat16, 2, tile, tile), (single, tile // 2, columns)

    def exchange(value):
        return lax.ppermute(value, ("groups",) + AXES, across)

    results = [
        (jnp.bfloat16, 2, tile, rows), block, square, field, block, (single, slots, tile, tile),
        (jnp.int32, 8, tile), (single, 8, tile), block, (single, tile + tile // 2 + 8, columns),
    ]
    local_outer, diag_outer, t_out_t, x, x_inner, tiles_inner, names, masses, push_there, send = pl.pallas_call(
        outer_kernel,
        out_shape=[pltpu.VMEM(shape[1:], shape[0]) for shape in results],
        in_specs=[pl.BlockSpec(memory_space=pl.ANY)] * 5,
        out_specs=[VMEM] * len(results),
        scratch_shapes=[
            pltpu.SMEM(block_cols.shape, jnp.int32),
            pltpu.VMEM((slots, tile, tile), single),
            pltpu.VMEM(mass.shape, single),
            pltpu.VMEM(source_ids.shape, jnp.int32),
            pltpu.SemaphoreType.DMA((6,)),
        ],
        name="outer_kernel",
    )(block_cols, step_tiles, mass, warm_start, source_ids)
    push_here = exchange(push_there)
    other_x = lax.ppermute(x_inner, AXES, partner)
    got = exchange(send)
    local, diag, t_in, t, t_inner, q_outer, q_send = call(
        inner_row_kernel,
        [(jnp.bfloat16, 2, rows, rows), field, square, field, block, block, halfway],
        local_outer, diag_outer, x, tiles_inner, names, masses, other_x, send,
    )
    got_q = exchange(q_send)
    other_t = lax.ppermute(t_inner, AXES, partner)
    w_inner, t_in_t, t_out = call(
        inner_kernel, [block, square, square], local, diag, t_in, t_out_t, t, other_t, push_here
    )
    other_w = lax.ppermute(w_inner, AXES, partner)
    r, w_local, edge_r_out, edge_r_in = call(
        residual_kernel, [field, block, block, block],
        local, diag, t_in_t, t_out_t, t, q_outer, push_here,
    )
    w, there, edge_y_out, moments, edge_y_in = call(
        moment_kernel, [field, block, block, (single, 16, columns), block],
        local, diag, t_in_t, t_out, t_out_t, r, w_local, edge_r_out, push_there, got, w_inner,
    )
    shares = call(
        share_kernel, [(single, devices, 3, 2, columns)],
        moments, edge_y_in, edge_r_in, edge_y_out, edge_r_out, there, got_q, other_t, other_w,
    )
    shares = lax.all_to_all(shares, AXES, 0, 0)
    return call(finish_kernel, [field], shares, x, r, w, last=True)


def solution(mesh):
    in_specs = (
        P(("groups", "patch", "sub"), None),
        P(("groups", "patch", "sub"), None, None, None),
        P(("groups", "patch", "sub")),
        P(("groups", "patch", "sub"), None),
        P("groups"),
    )
    out_specs = P(("groups", "patch", "sub"), None)
    return jax.shard_map(body, mesh=mesh, in_specs=in_specs, out_specs=out_specs, check_vma=False)
```

```python
import jax
import jax.numpy as jnp
from jax import lax
from jax.experimental import pallas as pl
from jax.experimental.pallas import tpu as pltpu
from jax.sharding import PartitionSpec as P


AXES = ("patch", "sub")
LEAST_EIGENVALUE = 0.0999
VMEM = pl.BlockSpec(memory_space=pltpu.VMEM)


def halves(a):
    high = a.astype(jnp.bfloat16)
    return high, (a - high.astype(jnp.float32)).astype(jnp.bfloat16)


def dot(a, b):
    a_high, a_low = a[0], a[1]
    b_high, b_low = halves(b)

    def product(p, q):
        return jnp.dot(p, q, preferred_element_type=jnp.float32)

    return product(a_high, b_high) + (product(a_high, b_low) + product(a_low, b_high))


def place():
    return lax.axis_index("patch") * lax.axis_size("sub") + lax.axis_index("sub")


def outer_block(tile):
    side = lax.axis_index("sub")
    outer = pl.ds(pl.multiple_of(side * tile, tile), tile)
    inner = pl.ds(pl.multiple_of((1 - side) * tile, tile), tile)
    return outer, inner


def flip(x):
    return pltpu.roll(x, x.shape[1] // 2, 1)


def index_of(shape, dimension):
    return lax.broadcasted_iota(jnp.int32, shape, dimension)


def toward(tiles, names, block):
    total = jnp.where(names[0:1, :] == block, tiles[0], 0.0)
    for k in range(1, tiles.shape[0]):
        total += jnp.where(names[k : k + 1, :] == block, tiles[k], 0.0)
    return total


def row_sums(tiles, masses):
    tile = tiles.shape[-1]
    whole = tiles[0]
    for k in range(1, tiles.shape[0]):
        whole += tiles[k]
    eye = index_of((tile, tile), 0) == index_of((tile, tile), 1)
    return jnp.sum(whole + jnp.where(eye, masses[0:1, :], 0.0), axis=1, keepdims=True)


def right_side(names, block, shape):
    vertices = block * shape[0] + index_of(shape, 0)
    return jnp.where(vertices == names[7:8, :], 1.0, 0.0)


def outer_kernel(
    cols_there, tiles_there, mass_there, x_there, sources_there,
    local_outer, diag_outer, t_out_t, x, x_inner, tiles_inner, names, masses, push, send,
    cols, tiles, mass, sources, arrived,
):
    tile = tiles.shape[-1]
    half = tile // 2
    slots = tiles.shape[0]
    position = place()
    side = lax.axis_index("sub")
    first = position * 2
    moves = (
        (cols_there, cols),
        (tiles_there.at[side], tiles),
        (x_there, x),
        (mass_there, mass),
        (sources_there, sources),
        (tiles_there.at[1 - side], tiles_inner),
    )
    copies = [pltpu.make_async_copy(start, end, arrived.at[i]) for i, (start, end) in enumerate(moves)]
    for copy in copies:
        copy.start()
    for copy in copies[:-1]:
        copy.wait()
    eye = index_of((tile, tile), 0) == index_of((tile, tile), 1)
    outer, inner = outer_block(tile)
    x_inner[...] = x[inner, :]
    row = index_of(names.shape, 0)
    named = jnp.broadcast_to(sources[...][None, :], names.shape)
    for k in range(slots):
        named = jnp.where(row == k, cols[1 - side, k], named)
    names[...] = named
    mass_0, mass_1 = mass[0:tile][None, :], mass[tile : 2 * tile][None, :]
    masses[...] = jnp.broadcast_to(jnp.where(side == 0, mass_1, mass_0), masses.shape)

    def one_toward(block):
        slot, scale = jnp.int32(0), 0.0
        for k in range(slots):
            found = cols[side, k] == block
            slot, scale = jnp.where(found, k, slot), jnp.where(found, 1.0, scale)
        return scale * tiles[slot]

    own = jnp.where(cols[side, 0] == first + side, tiles[0], 0.0)
    for k in range(1, slots):
        own += jnp.where(cols[side, k] == first + side, tiles[k], 0.0)
    cross = one_toward(first + 1 - side)
    total = row_sums(tiles, jnp.where(side == 0, mass_0, mass_1))
    diag_outer[...] = jnp.broadcast_to(total, diag_outer.shape)
    store_halves(local_outer, (slice(None), slice(0, tile)), jnp.where(side == 0, -own, -cross))
    store_halves(local_outer, (slice(None), slice(tile, 2 * tile)), jnp.where(side == 0, -cross, -own))
    store_halves(t_out_t, (slice(None),), one_toward(jnp.where(side == 0, first - 1, first + 2)).T)
    x_outer = x[outer, :]
    send[0:tile, :] = (
        right_side(named, first + side, x_outer.shape) - total * x_outer - dot(local_outer, x[...])
    )
    push[...] = dot(t_out_t, x_outer)
    above_diagonal = index_of((half, tile), 1) > index_of((half, tile), 0)
    send[tile : tile + half, :] = jnp.where(above_diagonal, own[:half], flip(own[half:]))
    diagonal = jnp.sum(jnp.where(eye, total, 0.0), axis=0, keepdims=True)
    send[tile + half :, :] = jnp.broadcast_to(diagonal, (8, tile))
    copies[-1].wait()


def store_halves(pair, index, value):
    pair[(0, *index)], pair[(1, *index)] = halves(value)


def inner_row_kernel(
    local_outer, diag_outer, x, tiles, names, masses, other_x, send,
    local, diag, t_in, t, t_inner, q_outer, q_send,
):
    tile = tiles.shape[-1]
    half = tile // 2
    position = place()
    side = lax.axis_index("sub")
    first = position * 2
    outer, inner = outer_block(tile)
    total = row_sums(tiles, masses)
    diag[outer, :] = diag_outer[...]
    diag[inner, :] = jnp.broadcast_to(total, diag_outer.shape)
    own, cross = toward(tiles, names, first + 1 - side), toward(tiles, names, first + side)
    store_halves(local, (inner, slice(0, tile)), jnp.where(side == 0, -cross, -own))
    store_halves(local, (inner, slice(tile, 2 * tile)), jnp.where(side == 0, -own, -cross))
    for k in range(2):
        local[k, outer, :] = local_outer[k]
    store_halves(t_in, (slice(None),), toward(tiles, names, jnp.where(side == 0, first + 2, first - 1)))
    x_inner = x[inner, :]
    t[outer, :] = send[0:tile, :]
    t_inner[...] = (
        right_side(names, first + 1 - side, x_inner.shape)
        - total * x_inner
        - dot(part(local, inner), x[...])
        + dot(t_in, other_x[...])
    )
    t[inner, :] = t_inner[...]
    q = (
        diag_outer[...] * send[0:tile, :]
        + dot(part(local_outer, slice(None), outer_columns(tile)), send[0:tile, :])
        + dot(part(local_outer, slice(None), inner_columns(tile)), t_inner[...])
    )
    q_outer[...] = q
    turned = jnp.where(side == 0, flip(q), q)
    first_half = index_of((half, tile), 1) < half
    q_send[...] = jnp.where(first_half, turned[:half], flip(turned[half:]))


def unpack(packed):
    tile = packed.shape[1]
    half = tile // 2
    rows = packed[0:half, :]
    row, column = index_of((half, tile), 0), index_of((half, tile), 1)
    upper = jnp.where(column > row, rows, 0.0)
    lower = flip(jnp.where(column < row, rows, 0.0))
    triangles = jnp.concatenate([upper, lower], axis=0)
    eye = index_of((tile, tile), 0) == index_of((tile, tile), 1)
    diagonal = jnp.sum(jnp.where(eye, packed[half : half + 1, :], 0.0), axis=1, keepdims=True)
    return triangles + triangles.T, diagonal


def outer_columns(tile):
    side = lax.axis_index("sub")
    return pl.ds(pl.multiple_of(side * tile, tile), tile)


def inner_columns(tile):
    side = lax.axis_index("sub")
    return pl.ds(pl.multiple_of((1 - side) * tile, tile), tile)


def part(pair, *index):
    return pair[(0, *index)], pair[(1, *index)]


def inner_kernel(local, diag, t_in, t_out_t, t, other_t, push_here, w_inner, t_in_t, t_out):
    tile = t_in.shape[-1]
    _, inner = outer_block(tile)
    w_inner[...] = (
        diag[inner, :] * t[inner, :]
        + dot(part(local, inner), t[...])
        + dot(part(local, inner, outer_columns(tile)), push_here[...])
        - dot(t_in, other_t[...])
    )
    for half in range(2):
        t_in_t[half] = t_in[half].T
        t_out[half] = t_out_t[half].T


def total(value):
    return jnp.sum(value, axis=0, keepdims=True)


def residual_kernel(local, diag, t_in_t, t_out_t, t, q_outer, push_here, r, w_outer, edge_r_out, edge_r_in):
    tile = t_in_t.shape[-1]
    outer, inner = outer_block(tile)
    push = push_here[...]
    r_outer = t[outer, :] + push
    r[outer, :] = r_outer
    r[inner, :] = t[inner, :]
    w_outer[...] = q_outer[...] + diag[outer, :] * push + dot(part(local, outer, outer_columns(tile)), push)
    edge_r_out[...] = dot(t_out_t, r_outer)
    edge_r_in[...] = dot(t_in_t, t[inner, :])


def moment_kernel(
    local, diag, t_in_t, t_out, t_out_t, r, w_local, edge_r_out, push_there, got, w_inner,
    w, there, edge_y_out, moments, edge_y_in,
):
    tile = t_out.shape[-1]
    outer, inner = outer_block(tile)
    push = push_there[...]
    r_outer, r_there = r[outer, :], got[0:tile, :] + push
    pull = dot(t_out, r_there)
    w_outer = w_local[...] - pull
    w[outer, :] = w_outer
    w[inner, :] = w_inner[...]
    w_now, r_now = w[...], r[...]
    r_r, r_w = total(r_now * r_now), total(r_now * w_now)
    shift = jnp.where(r_r > 0, r_w / r_r, 0.0)
    y = w_now - shift * r_now
    y_outer = w_outer - shift * r_outer
    a_y = diag[...] * y + dot(local, y)
    y_pull, r_pull = total(y_outer * pull), total(r_outer * pull)
    r_ay = total(r_now * a_y + y * w_now) + y_pull
    moments[...] = jnp.concatenate(
        [r_r, r_w, total(y * y), total(y * a_y), r_ay, r_w + r_pull, shift, y_pull, r_pull]
        + [shift] * (moments.shape[0] - 9),
        axis=0,
    )
    edge_y_out[...] = dot(t_out_t, y_outer)
    own_there, diag_there = unpack(got[tile:, :])
    there[...] = diag_there * push - dot(halves(own_there), push) - edge_r_out[...] - shift * r_there
    edge_y_in[...] = dot(t_in_t, w_inner[...] - shift * r[inner, :])


def share_kernel(
    moments, edge_y_in, edge_r_in, edge_y_out, edge_r_out, there, got_q, other_t, other_w, out
):
    tile = there.shape[0]
    half = tile // 2
    side = lax.axis_index("sub")
    shift = moments[6:7, :]
    q_half = got_q[...]
    q_flip = flip(q_half)
    q_there = jnp.concatenate(
        [jnp.where(side == 0, q_half, q_flip), jnp.where(side == 0, q_flip, q_half)], axis=0
    )
    y_there = q_there + there[...]
    mine = (index_of(shift.shape, 1) >= half) == (side == 1)
    weight = jnp.where(mine, 2.0, 0.0)
    y_partner = other_w[...] - shift * other_t[...]
    y_ay = total(edge_y_in[...] * y_partner) + weight * total(edge_y_out[...] * y_there)
    r_ay = total(edge_r_in[...] * y_partner)
    r_ay += weight * (total(edge_r_out[...] * y_there) + moments[7:8, :])
    r_ar = weight * moments[8:9, :]
    sums = moments[0:8, :]
    row = index_of(sums.shape, 0)
    for place_of, value in ((3, y_ay), (4, r_ay), (5, r_ar)):
        sums -= jnp.where(row == place_of, value, 0.0)
    for pair in range(out.shape[1]):
        out[:, pair] = jnp.broadcast_to(sums[None, 2 * pair : 2 * pair + 2], out[:, pair].shape)


def finish_kernel(shares, x, r, w, out):
    r_rs, r_ws, spreads, y_ay, r_ay, r_ar = [shares[:, row // 2, row % 2, :] for row in range(6)]
    r_r = jnp.sum(r_rs, axis=0, keepdims=True)
    r_w = jnp.sum(r_ws, axis=0, keepdims=True)
    theta = r_w / r_r
    off = jnp.where(r_rs > 0, r_ws / r_rs, 0.0) - theta
    spread = jnp.sum(spreads + r_rs * off * off, axis=0, keepdims=True)
    energy = jnp.sum(y_ay + off * (r_ay + off * r_ar), axis=0, keepdims=True)
    ratio = spread / (theta * theta * r_r)
    energy = jnp.maximum(energy - ratio * theta * spread, LEAST_EIGENVALUE * spread * (1.0 + ratio))
    step = jnp.where(spread > 0, spread / energy, 0.0)
    first = 1.0 / theta
    out[...] = x[...] + (first + step * (1.0 + ratio)) * r[...] - (step * first) * w[...]


def call(kernel, shapes, *operands, last=False):
    place_out = jax.ShapeDtypeStruct if last else pltpu.VMEM
    outs = [place_out(shape[1:], shape[0]) for shape in shapes]
    return pl.pallas_call(
        kernel,
        out_shape=outs if len(outs) > 1 else outs[0],
        in_specs=[VMEM] * len(operands),
        out_specs=[VMEM] * len(outs) if len(outs) > 1 else VMEM,
    )(*[pltpu.with_memory_space_constraint(operand, pltpu.VMEM) for operand in operands])


def body(block_cols, step_tiles, mass, warm_start, source_ids):
    tile = step_tiles.shape[-1]
    rows, columns = warm_start.shape
    assert block_cols.shape[0] == 2 and columns == tile and lax.axis_size("sub") == 2
    devices = lax.axis_size("patch") * lax.axis_size("sub")
    partner = [(i, i ^ 1) for i in range(devices)]
    groups = lax.axis_size("groups")
    across = []
    for group in range(groups):
        here, there = group * devices, (group + 1) % groups * devices
        for i in range(1, devices - 1, 2):
            across += [(here + i, here + i + 1), (here + i + 1, here + i)]
        across += [(here, there), (here + devices - 1, there + devices - 1)]
    single, slots = jnp.float32, block_cols.shape[1]
    assert slots < 8
    field, block = (single, rows, columns), (single, tile, columns)
    square, halfway = (jnp.bfloat16, 2, tile, tile), (single, tile // 2, columns)

    def exchange(value):
        return lax.ppermute(value, ("groups",) + AXES, across)

    results = [
        (jnp.bfloat16, 2, tile, rows), block, square, field, block, (single, slots, tile, tile),
        (jnp.int32, 8, tile), (single, 8, tile), block, (single, tile + tile // 2 + 8, columns),
    ]
    local_outer, diag_outer, t_out_t, x, x_inner, tiles_inner, names, masses, push_there, send = pl.pallas_call(
        outer_kernel,
        out_shape=[pltpu.VMEM(shape[1:], shape[0]) for shape in results],
        in_specs=[pl.BlockSpec(memory_space=pl.ANY)] * 5,
        out_specs=[VMEM] * len(results),
        scratch_shapes=[
            pltpu.SMEM(block_cols.shape, jnp.int32),
            pltpu.VMEM((slots, tile, tile), single),
            pltpu.VMEM(mass.shape, single),
            pltpu.VMEM(source_ids.shape, jnp.int32),
            pltpu.SemaphoreType.DMA((6,)),
        ],
        name="outer_kernel",
    )(block_cols, step_tiles, mass, warm_start, source_ids)
    push_here = exchange(push_there)
    other_x = lax.ppermute(x_inner, AXES, partner)
    got = exchange(send)
    local, diag, t_in, t, t_inner, q_outer, q_send = call(
        inner_row_kernel,
        [(jnp.bfloat16, 2, rows, rows), field, square, field, block, block, halfway],
        local_outer, diag_outer, x, tiles_inner, names, masses, other_x, send,
    )
    got_q = exchange(q_send)
    other_t = lax.ppermute(t_inner, AXES, partner)
    w_inner, t_in_t, t_out = call(
        inner_kernel, [block, square, square], local, diag, t_in, t_out_t, t, other_t, push_here
    )
    other_w = lax.ppermute(w_inner, AXES, partner)
    r, w_local, edge_r_out, edge_r_in = call(
        residual_kernel, [field, block, block, block],
        local, diag, t_in_t, t_out_t, t, q_outer, push_here,
    )
    w, there, edge_y_out, moments, edge_y_in = call(
        moment_kernel, [field, block, block, (single, 16, columns), block],
        local, diag, t_in_t, t_out, t_out_t, r, w_local, edge_r_out, push_there, got, w_inner,
    )
    shares = call(
        share_kernel, [(single, devices, 3, 2, columns)],
        moments, edge_y_in, edge_r_in, edge_y_out, edge_r_out, there, got_q, other_t, other_w,
    )
    shares = lax.all_to_all(shares, AXES, 0, 0)
    return call(finish_kernel, [field], shares, x, r, w, last=True)


def solution(mesh):
    in_specs = (
        P(("groups", "patch", "sub"), None),
        P(("groups", "patch", "sub"), None, None, None),
        P(("groups", "patch", "sub")),
        P(("groups", "patch", "sub"), None),
        P("groups"),
    )
    out_specs = P(("groups", "patch", "sub"), None)
    return jax.shard_map(body, mesh=mesh, in_specs=in_specs, out_specs=out_specs, check_vma=False)
```

```python
import jax
import jax.numpy as jnp
from jax import lax
from jax.experimental import pallas as pl
from jax.experimental.pallas import tpu as pltpu
from jax.sharding import PartitionSpec as P


AXES = ("patch", "sub")
LEAST_EIGENVALUE = 0.0999
VMEM = pl.BlockSpec(memory_space=pltpu.VMEM)


def halves(a):
    high = a.astype(jnp.bfloat16)
    return high, (a - high.astype(jnp.float32)).astype(jnp.bfloat16)


def dot(a, b):
    a_high, a_low = a[0], a[1]
    b_high, b_low = halves(b)

    def product(p, q):
        return jnp.dot(p, q, preferred_element_type=jnp.float32)

    return product(a_high, b_high) + (product(a_high, b_low) + product(a_low, b_high))


def place():
    return lax.axis_index("patch") * lax.axis_size("sub") + lax.axis_index("sub")


def outer_block(tile):
    side = lax.axis_index("sub")
    outer = pl.ds(pl.multiple_of(side * tile, tile), tile)
    inner = pl.ds(pl.multiple_of((1 - side) * tile, tile), tile)
    return outer, inner


def flip(x):
    return pltpu.roll(x, x.shape[1] // 2, 1)


def index_of(shape, dimension):
    return lax.broadcasted_iota(jnp.int32, shape, dimension)


def toward(tiles, names, block):
    total = jnp.where(names[0:1, :] == block, tiles[0], 0.0)
    for k in range(1, tiles.shape[0]):
        total += jnp.where(names[k : k + 1, :] == block, tiles[k], 0.0)
    return total


def row_sums(tiles, masses):
    tile = tiles.shape[-1]
    whole = tiles[0]
    for k in range(1, tiles.shape[0]):
        whole += tiles[k]
    eye = index_of((tile, tile), 0) == index_of((tile, tile), 1)
    return jnp.sum(whole + jnp.where(eye, masses[0:1, :], 0.0), axis=1, keepdims=True)


def right_side(names, block, shape):
    vertices = block * shape[0] + index_of(shape, 0)
    return jnp.where(vertices == names[7:8, :], 1.0, 0.0)


def outer_kernel(
    cols_there, tiles_there, mass_there, x_there, sources_there,
    local_outer, diag_outer, t_out_t, x, tiles_inner, names, masses, push, send,
    cols, tiles, mass, sources, arrived,
):
    tile = tiles.shape[-1]
    half = tile // 2
    slots = tiles.shape[0]
    position = place()
    side = lax.axis_index("sub")
    first = position * 2
    moves = (
        (cols_there, cols),
        (tiles_there.at[side], tiles),
        (x_there, x),
        (mass_there, mass),
        (sources_there, sources),
        (tiles_there.at[1 - side], tiles_inner),
    )
    copies = [pltpu.make_async_copy(start, end, arrived.at[i]) for i, (start, end) in enumerate(moves)]
    for copy in copies:
        copy.start()
    for copy in copies[:-1]:
        copy.wait()
    eye = index_of((tile, tile), 0) == index_of((tile, tile), 1)
    outer, _ = outer_block(tile)
    row = index_of(names.shape, 0)
    named = jnp.broadcast_to(sources[...][None, :], names.shape)
    for k in range(slots):
        named = jnp.where(row == k, cols[1 - side, k], named)
    names[...] = named
    mass_0, mass_1 = mass[0:tile][None, :], mass[tile : 2 * tile][None, :]
    masses[...] = jnp.broadcast_to(jnp.where(side == 0, mass_1, mass_0), masses.shape)

    def one_toward(block):
        slot, scale = jnp.int32(0), 0.0
        for k in range(slots):
            found = cols[side, k] == block
            slot, scale = jnp.where(found, k, slot), jnp.where(found, 1.0, scale)
        return scale * tiles[slot]

    own = jnp.where(cols[side, 0] == first + side, tiles[0], 0.0)
    for k in range(1, slots):
        own += jnp.where(cols[side, k] == first + side, tiles[k], 0.0)
    cross = one_toward(first + 1 - side)
    total = row_sums(tiles, jnp.where(side == 0, mass_0, mass_1))
    diag_outer[...] = jnp.broadcast_to(total, diag_outer.shape)
    store_halves(local_outer, (slice(None), slice(0, tile)), jnp.where(side == 0, -own, -cross))
    store_halves(local_outer, (slice(None), slice(tile, 2 * tile)), jnp.where(side == 0, -cross, -own))
    store_halves(t_out_t, (slice(None),), one_toward(jnp.where(side == 0, first - 1, first + 2)).T)
    x_outer = x[outer, :]
    send[0:tile, :] = (
        right_side(named, first + side, x_outer.shape) - total * x_outer - dot(local_outer, x[...])
    )
    push[...] = dot(t_out_t, x_outer)
    above_diagonal = index_of((half, tile), 1) > index_of((half, tile), 0)
    send[tile : tile + half, :] = jnp.where(above_diagonal, own[:half], flip(own[half:]))
    diagonal = jnp.sum(jnp.where(eye, total, 0.0), axis=0, keepdims=True)
    send[tile + half :, :] = jnp.broadcast_to(diagonal, (8, tile))
    copies[-1].wait()


def store_halves(pair, index, value):
    pair[(0, *index)], pair[(1, *index)] = halves(value)


def inner_row_kernel(
    local_outer, diag_outer, x, tiles, names, masses, other_x, send,
    local, diag, t_in, t, t_inner, q_outer, q_send,
):
    tile = tiles.shape[-1]
    half = tile // 2
    position = place()
    side = lax.axis_index("sub")
    first = position * 2
    outer, inner = outer_block(tile)
    total = row_sums(tiles, masses)
    diag[outer, :] = diag_outer[...]
    diag[inner, :] = jnp.broadcast_to(total, diag_outer.shape)
    own, cross = toward(tiles, names, first + 1 - side), toward(tiles, names, first + side)
    store_halves(local, (inner, slice(0, tile)), jnp.where(side == 0, -cross, -own))
    store_halves(local, (inner, slice(tile, 2 * tile)), jnp.where(side == 0, -own, -cross))
    for k in range(2):
        local[k, outer, :] = local_outer[k]
    store_halves(t_in, (slice(None),), toward(tiles, names, jnp.where(side == 0, first + 2, first - 1)))
    x_inner = x[inner, :]
    t[outer, :] = send[0:tile, :]
    t_inner[...] = (
        right_side(names, first + 1 - side, x_inner.shape)
        - total * x_inner
        - dot(part(local, inner), x[...])
        + dot(t_in, other_x[outer, :])
    )
    t[inner, :] = t_inner[...]
    q = (
        diag_outer[...] * send[0:tile, :]
        + dot(part(local_outer, slice(None), outer_columns(tile)), send[0:tile, :])
        + dot(part(local_outer, slice(None), inner_columns(tile)), t_inner[...])
    )
    q_outer[...] = q
    turned = jnp.where(side == 0, flip(q), q)
    first_half = index_of((half, tile), 1) < half
    q_send[...] = jnp.where(first_half, turned[:half], flip(turned[half:]))


def unpack(packed):
    tile = packed.shape[1]
    half = tile // 2
    rows = packed[0:half, :]
    row, column = index_of((half, tile), 0), index_of((half, tile), 1)
    upper = jnp.where(column > row, rows, 0.0)
    lower = flip(jnp.where(column < row, rows, 0.0))
    triangles = jnp.concatenate([upper, lower], axis=0)
    eye = index_of((tile, tile), 0) == index_of((tile, tile), 1)
    diagonal = jnp.sum(jnp.where(eye, packed[half : half + 1, :], 0.0), axis=1, keepdims=True)
    return triangles + triangles.T, diagonal


def outer_columns(tile):
    side = lax.axis_index("sub")
    return pl.ds(pl.multiple_of(side * tile, tile), tile)


def inner_columns(tile):
    side = lax.axis_index("sub")
    return pl.ds(pl.multiple_of((1 - side) * tile, tile), tile)


def part(pair, *index):
    return pair[(0, *index)], pair[(1, *index)]


def inner_kernel(local, diag, t_in, t_out_t, t, other_t, push_here, w_inner, t_in_t, t_out):
    tile = t_in.shape[-1]
    _, inner = outer_block(tile)
    w_inner[...] = (
        diag[inner, :] * t[inner, :]
        + dot(part(local, inner), t[...])
        + dot(part(local, inner, outer_columns(tile)), push_here[...])
        - dot(t_in, other_t[...])
    )
    for half in range(2):
        t_in_t[half] = t_in[half].T
        t_out[half] = t_out_t[half].T


def total(value):
    return jnp.sum(value, axis=0, keepdims=True)


def residual_kernel(local, diag, t_in_t, t_out_t, t, q_outer, push_here, r, w_outer, edge_r_out, edge_r_in):
    tile = t_in_t.shape[-1]
    outer, inner = outer_block(tile)
    push = push_here[...]
    r_outer = t[outer, :] + push
    r[outer, :] = r_outer
    r[inner, :] = t[inner, :]
    w_outer[...] = q_outer[...] + diag[outer, :] * push + dot(part(local, outer, outer_columns(tile)), push)
    edge_r_out[...] = dot(t_out_t, r_outer)
    edge_r_in[...] = dot(t_in_t, t[inner, :])


def moment_kernel(
    local, diag, t_in_t, t_out, t_out_t, r, w_local, edge_r_out, push_there, got, w_inner,
    w, there, edge_y_out, moments, edge_y_in,
):
    tile = t_out.shape[-1]
    outer, inner = outer_block(tile)
    push = push_there[...]
    r_outer, r_there = r[outer, :], got[0:tile, :] + push
    pull = dot(t_out, r_there)
    w_outer = w_local[...] - pull
    w[outer, :] = w_outer
    w[inner, :] = w_inner[...]
    w_now, r_now = w[...], r[...]
    r_r, r_w = total(r_now * r_now), total(r_now * w_now)
    shift = jnp.where(r_r > 0, r_w / r_r, 0.0)
    y = w_now - shift * r_now
    y_outer = w_outer - shift * r_outer
    a_y = diag[...] * y + dot(local, y)
    y_pull, r_pull = total(y_outer * pull), total(r_outer * pull)
    r_ay = total(r_now * a_y + y * w_now) + y_pull
    moments[...] = jnp.concatenate(
        [r_r, r_w, total(y * y), total(y * a_y), r_ay, r_w + r_pull, shift, y_pull, r_pull]
        + [shift] * (moments.shape[0] - 9),
        axis=0,
    )
    edge_y_out[...] = dot(t_out_t, y_outer)
    own_there, diag_there = unpack(got[tile:, :])
    there[...] = diag_there * push - dot(halves(own_there), push) - edge_r_out[...] - shift * r_there
    edge_y_in[...] = dot(t_in_t, w_inner[...] - shift * r[inner, :])


def share_kernel(
    moments, edge_y_in, edge_r_in, edge_y_out, edge_r_out, there, got_q, other_t, other_w, out
):
    tile = there.shape[0]
    half = tile // 2
    side = lax.axis_index("sub")
    shift = moments[6:7, :]
    q_half = got_q[...]
    q_flip = flip(q_half)
    q_there = jnp.concatenate(
        [jnp.where(side == 0, q_half, q_flip), jnp.where(side == 0, q_flip, q_half)], axis=0
    )
    y_there = q_there + there[...]
    mine = (index_of(shift.shape, 1) >= half) == (side == 1)
    weight = jnp.where(mine, 2.0, 0.0)
    y_partner = other_w[...] - shift * other_t[...]
    y_ay = total(edge_y_in[...] * y_partner) + weight * total(edge_y_out[...] * y_there)
    r_ay = total(edge_r_in[...] * y_partner)
    r_ay += weight * (total(edge_r_out[...] * y_there) + moments[7:8, :])
    r_ar = weight * moments[8:9, :]
    sums = moments[0:8, :]
    row = index_of(sums.shape, 0)
    for place_of, value in ((3, y_ay), (4, r_ay), (5, r_ar)):
        sums -= jnp.where(row == place_of, value, 0.0)
    for pair in range(out.shape[1]):
        out[:, pair] = jnp.broadcast_to(sums[None, 2 * pair : 2 * pair + 2], out[:, pair].shape)


def finish_kernel(shares, x, r, w, out):
    r_rs, r_ws, spreads, y_ay, r_ay, r_ar = [shares[:, row // 2, row % 2, :] for row in range(6)]
    r_r = jnp.sum(r_rs, axis=0, keepdims=True)
    r_w = jnp.sum(r_ws, axis=0, keepdims=True)
    theta = r_w / r_r
    off = jnp.where(r_rs > 0, r_ws / r_rs, 0.0) - theta
    spread = jnp.sum(spreads + r_rs * off * off, axis=0, keepdims=True)
    energy = jnp.sum(y_ay + off * (r_ay + off * r_ar), axis=0, keepdims=True)
    ratio = spread / (theta * theta * r_r)
    energy = jnp.maximum(energy - ratio * theta * spread, LEAST_EIGENVALUE * spread * (1.0 + ratio))
    step = jnp.where(spread > 0, spread / energy, 0.0)
    first = 1.0 / theta
    out[...] = x[...] + (first + step * (1.0 + ratio)) * r[...] - (step * first) * w[...]


def call(kernel, shapes, *operands, last=False):
    place_out = jax.ShapeDtypeStruct if last else pltpu.VMEM
    outs = [place_out(shape[1:], shape[0]) for shape in shapes]
    return pl.pallas_call(
        kernel,
        out_shape=outs if len(outs) > 1 else outs[0],
        in_specs=[VMEM] * len(operands),
        out_specs=[VMEM] * len(outs) if len(outs) > 1 else VMEM,
    )(*[pltpu.with_memory_space_constraint(operand, pltpu.VMEM) for operand in operands])


def body(block_cols, step_tiles, mass, warm_start, source_ids):
    tile = step_tiles.shape[-1]
    rows, columns = warm_start.shape
    assert block_cols.shape[0] == 2 and columns == tile and lax.axis_size("sub") == 2
    devices = lax.axis_size("patch") * lax.axis_size("sub")
    partner = [(i, i ^ 1) for i in range(devices)]
    groups = lax.axis_size("groups")
    across = []
    for group in range(groups):
        here, there = group * devices, (group + 1) % groups * devices
        for i in range(1, devices - 1, 2):
            across += [(here + i, here + i + 1), (here + i + 1, here + i)]
        across += [(here, there), (here + devices - 1, there + devices - 1)]
    single, slots = jnp.float32, block_cols.shape[1]
    assert slots < 8
    field, block = (single, rows, columns), (single, tile, columns)
    square, halfway = (jnp.bfloat16, 2, tile, tile), (single, tile // 2, columns)

    def exchange(value):
        return lax.ppermute(value, ("groups",) + AXES, across)

    other_x = lax.ppermute(warm_start, AXES, partner)
    results = [
        (jnp.bfloat16, 2, tile, rows), block, square, field, (single, slots, tile, tile),
        (jnp.int32, 8, tile), (single, 8, tile), block, (single, tile + tile // 2 + 8, columns),
    ]
    local_outer, diag_outer, t_out_t, x, tiles_inner, names, masses, push_there, send = pl.pallas_call(
        outer_kernel,
        out_shape=[pltpu.VMEM(shape[1:], shape[0]) for shape in results],
        in_specs=[pl.BlockSpec(memory_space=pl.ANY)] * 5,
        out_specs=[VMEM] * len(results),
        scratch_shapes=[
            pltpu.SMEM(block_cols.shape, jnp.int32),
            pltpu.VMEM((slots, tile, tile), single),
            pltpu.VMEM(mass.shape, single),
            pltpu.VMEM(source_ids.shape, jnp.int32),
            pltpu.SemaphoreType.DMA((6,)),
        ],
        name="outer_kernel",
    )(block_cols, step_tiles, mass, warm_start, source_ids)
    push_here = exchange(push_there)
    got = exchange(send)
    local, diag, t_in, t, t_inner, q_outer, q_send = call(
        inner_row_kernel,
        [(jnp.bfloat16, 2, rows, rows), field, square, field, block, block, halfway],
        local_outer, diag_outer, x, tiles_inner, names, masses, other_x, send,
    )
    got_q = exchange(q_send)
    other_t = lax.ppermute(t_inner, AXES, partner)
    w_inner, t_in_t, t_out = call(
        inner_kernel, [block, square, square], local, diag, t_in, t_out_t, t, other_t, push_here
    )
    other_w = lax.ppermute(w_inner, AXES, partner)
    r, w_local, edge_r_out, edge_r_in = call(
        residual_kernel, [field, block, block, block],
        local, diag, t_in_t, t_out_t, t, q_outer, push_here,
    )
    w, there, edge_y_out, moments, edge_y_in = call(
        moment_kernel, [field, block, block, (single, 16, columns), block],
        local, diag, t_in_t, t_out, t_out_t, r, w_local, edge_r_out, push_there, got, w_inner,
    )
    shares = call(
        share_kernel, [(single, devices, 3, 2, columns)],
        moments, edge_y_in, edge_r_in, edge_y_out, edge_r_out, there, got_q, other_t, other_w,
    )
    shares = lax.all_to_all(shares, AXES, 0, 0)
    return call(finish_kernel, [field], shares, x, r, w, last=True)


def solution(mesh):
    in_specs = (
        P(("groups", "patch", "sub"), None),
        P(("groups", "patch", "sub"), None, None, None),
        P(("groups", "patch", "sub")),
        P(("groups", "patch", "sub"), None),
        P("groups"),
    )
    out_specs = P(("groups", "patch", "sub"), None)
    return jax.shard_map(body, mesh=mesh, in_specs=in_specs, out_specs=out_specs, check_vma=False)
```

```python
import jax
import jax.numpy as jnp
from jax import lax
from jax.experimental import pallas as pl
from jax.experimental.pallas import tpu as pltpu
from jax.sharding import PartitionSpec as P


AXES = ("patch", "sub")
LEAST_EIGENVALUE = 0.0999
VMEM = pl.BlockSpec(memory_space=pltpu.VMEM)


def halves(a):
    high = a.astype(jnp.bfloat16)
    return high, (a - high.astype(jnp.float32)).astype(jnp.bfloat16)


def dot(a, b):
    a_high, a_low = a[0], a[1]
    b_high, b_low = halves(b)

    def product(p, q):
        return jnp.dot(p, q, preferred_element_type=jnp.float32)

    return product(a_high, b_high) + (product(a_high, b_low) + product(a_low, b_high))


def place():
    return lax.axis_index("patch") * lax.axis_size("sub") + lax.axis_index("sub")


def outer_block(tile):
    side = lax.axis_index("sub")
    outer = pl.ds(pl.multiple_of(side * tile, tile), tile)
    inner = pl.ds(pl.multiple_of((1 - side) * tile, tile), tile)
    return outer, inner


def flip(x):
    return pltpu.roll(x, x.shape[1] // 2, 1)


def index_of(shape, dimension):
    return lax.broadcasted_iota(jnp.int32, shape, dimension)


def toward(tiles, names, block):
    total = jnp.where(names[0:1, :] == block, tiles[0], 0.0)
    for k in range(1, tiles.shape[0]):
        total += jnp.where(names[k : k + 1, :] == block, tiles[k], 0.0)
    return total


def row_sums(tiles, masses):
    tile = tiles.shape[-1]
    whole = tiles[0]
    for k in range(1, tiles.shape[0]):
        whole += tiles[k]
    eye = index_of((tile, tile), 0) == index_of((tile, tile), 1)
    return jnp.sum(whole + jnp.where(eye, masses[0:1, :], 0.0), axis=1, keepdims=True)


def right_side(names, block, shape):
    vertices = block * shape[0] + index_of(shape, 0)
    return jnp.where(vertices == names[7:8, :], 1.0, 0.0)


def outer_kernel(
    cols_there, tiles_there, mass_there, x_there, sources_there,
    local_outer, diag_outer, t_out_t, x, tiles_inner, names, masses, push, send,
    cols, tiles, mass, sources, arrived,
):
    tile = tiles.shape[-1]
    half = tile // 2
    slots = tiles.shape[0]
    position = place()
    side = lax.axis_index("sub")
    first = position * 2
    moves = (
        (cols_there, cols),
        (tiles_there.at[side], tiles),
        (x_there, x),
        (mass_there, mass),
        (sources_there, sources),
        (tiles_there.at[1 - side], tiles_inner),
    )
    copies = [pltpu.make_async_copy(start, end, arrived.at[i]) for i, (start, end) in enumerate(moves)]
    for copy in copies:
        copy.start()
    for copy in copies[:-1]:
        copy.wait()
    eye = index_of((tile, tile), 0) == index_of((tile, tile), 1)
    outer, _ = outer_block(tile)
    row = index_of(names.shape, 0)
    named = jnp.broadcast_to(sources[...][None, :], names.shape)
    for k in range(slots):
        named = jnp.where(row == k, cols[1 - side, k], named)
    names[...] = named
    mass_0, mass_1 = mass[0:tile][None, :], mass[tile : 2 * tile][None, :]
    masses[...] = jnp.broadcast_to(jnp.where(side == 0, mass_1, mass_0), masses.shape)

    def one_toward(block):
        slot, scale = jnp.int32(0), 0.0
        for k in range(slots):
            found = cols[side, k] == block
            slot, scale = jnp.where(found, k, slot), jnp.where(found, 1.0, scale)
        return scale * tiles[slot]

    own = jnp.where(cols[side, 0] == first + side, tiles[0], 0.0)
    for k in range(1, slots):
        own += jnp.where(cols[side, k] == first + side, tiles[k], 0.0)
    cross = one_toward(first + 1 - side)
    total = row_sums(tiles, jnp.where(side == 0, mass_0, mass_1))
    diag_outer[...] = jnp.broadcast_to(total, diag_outer.shape)
    store_halves(local_outer, (slice(None), slice(0, tile)), jnp.where(side == 0, -own, -cross))
    store_halves(local_outer, (slice(None), slice(tile, 2 * tile)), jnp.where(side == 0, -cross, -own))
    store_halves(t_out_t, (slice(None),), one_toward(jnp.where(side == 0, first - 1, first + 2)).T)
    x_outer = x[outer, :]
    send[0:tile, :] = (
        right_side(named, first + side, x_outer.shape) - total * x_outer - dot(local_outer, x[...])
    )
    push[...] = dot(t_out_t, x_outer)
    above_diagonal = index_of((half, tile), 1) > index_of((half, tile), 0)
    send[tile : tile + half, :] = jnp.where(above_diagonal, own[:half], flip(own[half:]))
    diagonal = jnp.sum(jnp.where(eye, total, 0.0), axis=0, keepdims=True)
    send[tile + half :, :] = jnp.broadcast_to(diagonal, (8, tile))
    copies[-1].wait()


def store_halves(pair, index, value):
    pair[(0, *index)], pair[(1, *index)] = halves(value)


def inner_row_kernel(
    local_outer, diag_outer, x, tiles, names, masses, other_x, send,
    local, diag, t_in, t, t_inner, q_outer, q_send,
):
    tile = tiles.shape[-1]
    half = tile // 2
    position = place()
    side = lax.axis_index("sub")
    first = position * 2
    outer, inner = outer_block(tile)
    total = row_sums(tiles, masses)
    diag[outer, :] = diag_outer[...]
    diag[inner, :] = jnp.broadcast_to(total, diag_outer.shape)
    own, cross = toward(tiles, names, first + 1 - side), toward(tiles, names, first + side)
    store_halves(local, (inner, slice(0, tile)), jnp.where(side == 0, -cross, -own))
    store_halves(local, (inner, slice(tile, 2 * tile)), jnp.where(side == 0, -own, -cross))
    for k in range(2):
        local[k, outer, :] = local_outer[k]
    store_halves(t_in, (slice(None),), toward(tiles, names, jnp.where(side == 0, first + 2, first - 1)))
    x_inner = x[inner, :]
    t[outer, :] = send[0:tile, :]
    t_inner[...] = (
        right_side(names, first + 1 - side, x_inner.shape)
        - total * x_inner
        - dot(part(local, inner), x[...])
        + dot(t_in, other_x[outer, :])
    )
    t[inner, :] = t_inner[...]
    q = (
        diag_outer[...] * send[0:tile, :]
        + dot(part(local_outer, slice(None), outer_columns(tile)), send[0:tile, :])
        + dot(part(local_outer, slice(None), inner_columns(tile)), t_inner[...])
    )
    q_outer[...] = q
    turned = jnp.where(side == 0, flip(q), q)
    first_half = index_of((half, tile), 1) < half
    q_send[...] = jnp.where(first_half, turned[:half], flip(turned[half:]))


def unpack(packed):
    tile = packed.shape[1]
    half = tile // 2
    rows = packed[0:half, :]
    row, column = index_of((half, tile), 0), index_of((half, tile), 1)
    upper = jnp.where(column > row, rows, 0.0)
    lower = flip(jnp.where(column < row, rows, 0.0))
    triangles = jnp.concatenate([upper, lower], axis=0)
    eye = index_of((tile, tile), 0) == index_of((tile, tile), 1)
    diagonal = jnp.sum(jnp.where(eye, packed[half : half + 1, :], 0.0), axis=1, keepdims=True)
    return triangles + triangles.T, diagonal


def outer_columns(tile):
    side = lax.axis_index("sub")
    return pl.ds(pl.multiple_of(side * tile, tile), tile)


def inner_columns(tile):
    side = lax.axis_index("sub")
    return pl.ds(pl.multiple_of((1 - side) * tile, tile), tile)


def part(pair, *index):
    return pair[(0, *index)], pair[(1, *index)]


def inner_kernel(local, diag, t_in, t_out_t, t, other_t, push_here, w_inner, t_in_t, t_out):
    tile = t_in.shape[-1]
    _, inner = outer_block(tile)
    w_inner[...] = (
        diag[inner, :] * t[inner, :]
        + dot(part(local, inner), t[...])
        + dot(part(local, inner, outer_columns(tile)), push_here[...])
        - dot(t_in, other_t[...])
    )
    for half in range(2):
        t_in_t[half] = t_in[half].T
        t_out[half] = t_out_t[half].T


def total(value):
    return jnp.sum(value, axis=0, keepdims=True)


def residual_kernel(local, diag, t_in_t, t_out_t, t, q_outer, push_here, r, w_outer, edge_r_out, edge_r_in):
    tile = t_in_t.shape[-1]
    outer, inner = outer_block(tile)
    push = push_here[...]
    r_outer = t[outer, :] + push
    r[outer, :] = r_outer
    r[inner, :] = t[inner, :]
    w_outer[...] = q_outer[...] + diag[outer, :] * push + dot(part(local, outer, outer_columns(tile)), push)
    edge_r_out[...] = dot(t_out_t, r_outer)
    edge_r_in[...] = dot(t_in_t, t[inner, :])


def moment_kernel(
    local, diag, t_in_t, t_out, t_out_t, r, w_local, edge_r_out, push_there, got, w_inner,
    w, there, edge_y_out, moments, edge_y_in,
):
    tile = t_out.shape[-1]
    outer, inner = outer_block(tile)
    push = push_there[...]
    r_outer, r_there = r[outer, :], got[0:tile, :] + push
    pull = dot(t_out, r_there)
    w_outer = w_local[...] - pull
    w[outer, :] = w_outer
    w[inner, :] = w_inner[...]
    w_now, r_now = w[...], r[...]
    r_r, r_w = total(r_now * r_now), total(r_now * w_now)
    shift = jnp.where(r_r > 0, r_w / r_r, 0.0)
    y = w_now - shift * r_now
    y_outer = w_outer - shift * r_outer
    a_y = diag[...] * y + dot(local, y)
    y_pull, r_pull = total(y_outer * pull), total(r_outer * pull)
    r_ay = total(r_now * a_y + y * w_now) + y_pull
    moments[...] = jnp.concatenate(
        [r_r, r_w, total(y * y), total(y * a_y), r_ay, r_w + r_pull, shift, y_pull, r_pull]
        + [shift] * (moments.shape[0] - 9),
        axis=0,
    )
    edge_y_out[...] = dot(t_out_t, y_outer)
    own_there, diag_there = unpack(got[tile:, :])
    there[...] = diag_there * push - dot(halves(own_there), push) - edge_r_out[...] - shift * r_there
    edge_y_in[...] = dot(t_in_t, w_inner[...] - shift * r[inner, :])


def share_kernel(
    moments, edge_y_in, edge_r_in, edge_y_out, edge_r_out, there, got_q, other_t, other_w, out
):
    tile = there.shape[0]
    half = tile // 2
    side = lax.axis_index("sub")
    shift = moments[6:7, :]
    q_half = got_q[...]
    q_flip = flip(q_half)
    q_there = jnp.concatenate(
        [jnp.where(side == 0, q_half, q_flip), jnp.where(side == 0, q_flip, q_half)], axis=0
    )
    y_there = q_there + there[...]
    mine = (index_of(shift.shape, 1) >= half) == (side == 1)
    weight = jnp.where(mine, 2.0, 0.0)
    y_partner = other_w[...] - shift * other_t[...]
    y_ay = total(edge_y_in[...] * y_partner) + weight * total(edge_y_out[...] * y_there)
    r_ay = total(edge_r_in[...] * y_partner)
    r_ay += weight * (total(edge_r_out[...] * y_there) + moments[7:8, :])
    r_ar = weight * moments[8:9, :]
    sums = moments[0:8, :]
    row = index_of(sums.shape, 0)
    for place_of, value in ((3, y_ay), (4, r_ay), (5, r_ar)):
        sums -= jnp.where(row == place_of, value, 0.0)
    for pair in range(out.shape[1]):
        out[:, pair] = jnp.broadcast_to(sums[None, 2 * pair : 2 * pair + 2], out[:, pair].shape)


def finish_kernel(shares, x, r, w, out):
    devices = shares.shape[0] // lax.axis_size("groups")
    mine = pl.ds(lax.axis_index("groups") * devices, devices)
    r_rs, r_ws, spreads, y_ay, r_ay, r_ar = [shares[mine, row // 2, row % 2, :] for row in range(6)]
    r_r = jnp.sum(r_rs, axis=0, keepdims=True)
    r_w = jnp.sum(r_ws, axis=0, keepdims=True)
    theta = r_w / r_r
    off = jnp.where(r_rs > 0, r_ws / r_rs, 0.0) - theta
    spread = jnp.sum(spreads + r_rs * off * off, axis=0, keepdims=True)
    energy = jnp.sum(y_ay + off * (r_ay + off * r_ar), axis=0, keepdims=True)
    ratio = spread / (theta * theta * r_r)
    energy = jnp.maximum(energy - ratio * theta * spread, LEAST_EIGENVALUE * spread * (1.0 + ratio))
    step = jnp.where(spread > 0, spread / energy, 0.0)
    first = 1.0 / theta
    out[...] = x[...] + (first + step * (1.0 + ratio)) * r[...] - (step * first) * w[...]


def call(kernel, shapes, *operands, last=False):
    place_out = jax.ShapeDtypeStruct if last else pltpu.VMEM
    outs = [place_out(shape[1:], shape[0]) for shape in shapes]
    return pl.pallas_call(
        kernel,
        out_shape=outs if len(outs) > 1 else outs[0],
        in_specs=[VMEM] * len(operands),
        out_specs=[VMEM] * len(outs) if len(outs) > 1 else VMEM,
    )(*[pltpu.with_memory_space_constraint(operand, pltpu.VMEM) for operand in operands])


def body(block_cols, step_tiles, mass, warm_start, source_ids):
    tile = step_tiles.shape[-1]
    rows, columns = warm_start.shape
    assert block_cols.shape[0] == 2 and columns == tile and lax.axis_size("sub") == 2
    devices = lax.axis_size("patch") * lax.axis_size("sub")
    partner = [(i, i ^ 1) for i in range(devices)]
    groups = lax.axis_size("groups")
    across = []
    for group in range(groups):
        here, there = group * devices, (group + 1) % groups * devices
        for i in range(1, devices - 1, 2):
            across += [(here + i, here + i + 1), (here + i + 1, here + i)]
        across += [(here, there), (here + devices - 1, there + devices - 1)]
    single, slots = jnp.float32, block_cols.shape[1]
    assert slots < 8
    field, block = (single, rows, columns), (single, tile, columns)
    square, halfway = (jnp.bfloat16, 2, tile, tile), (single, tile // 2, columns)

    def exchange(value):
        return lax.ppermute(value, ("groups",) + AXES, across)

    other_x = lax.ppermute(warm_start, AXES, partner)
    results = [
        (jnp.bfloat16, 2, tile, rows), block, square, field, (single, slots, tile, tile),
        (jnp.int32, 8, tile), (single, 8, tile), block, (single, tile + tile // 2 + 8, columns),
    ]
    local_outer, diag_outer, t_out_t, x, tiles_inner, names, masses, push_there, send = pl.pallas_call(
        outer_kernel,
        out_shape=[pltpu.VMEM(shape[1:], shape[0]) for shape in results],
        in_specs=[pl.BlockSpec(memory_space=pl.ANY)] * 5,
        out_specs=[VMEM] * len(results),
        scratch_shapes=[
            pltpu.SMEM(block_cols.shape, jnp.int32),
            pltpu.VMEM((slots, tile, tile), single),
            pltpu.VMEM(mass.shape, single),
            pltpu.VMEM(source_ids.shape, jnp.int32),
            pltpu.SemaphoreType.DMA((6,)),
        ],
        name="outer_kernel",
    )(block_cols, step_tiles, mass, warm_start, source_ids)
    push_here = exchange(push_there)
    got = exchange(send)
    local, diag, t_in, t, t_inner, q_outer, q_send = call(
        inner_row_kernel,
        [(jnp.bfloat16, 2, rows, rows), field, square, field, block, block, halfway],
        local_outer, diag_outer, x, tiles_inner, names, masses, other_x, send,
    )
    got_q = exchange(q_send)
    other_t = lax.ppermute(t_inner, AXES, partner)
    w_inner, t_in_t, t_out = call(
        inner_kernel, [block, square, square], local, diag, t_in, t_out_t, t, other_t, push_here
    )
    other_w = lax.ppermute(w_inner, AXES, partner)
    r, w_local, edge_r_out, edge_r_in = call(
        residual_kernel, [field, block, block, block],
        local, diag, t_in_t, t_out_t, t, q_outer, push_here,
    )
    w, there, edge_y_out, moments, edge_y_in = call(
        moment_kernel, [field, block, block, (single, 16, columns), block],
        local, diag, t_in_t, t_out, t_out_t, r, w_local, edge_r_out, push_there, got, w_inner,
    )
    shares = call(
        share_kernel, [(single, groups * devices, 3, 2, columns)],
        moments, edge_y_in, edge_r_in, edge_y_out, edge_r_out, there, got_q, other_t, other_w,
    )
    shares = lax.all_to_all(shares, ("groups",) + AXES, 0, 0)
    return call(finish_kernel, [field], shares, x, r, w, last=True)


def solution(mesh):
    in_specs = (
        P(("groups", "patch", "sub"), None),
        P(("groups", "patch", "sub"), None, None, None),
        P(("groups", "patch", "sub")),
        P(("groups", "patch", "sub"), None),
        P("groups"),
    )
    out_specs = P(("groups", "patch", "sub"), None)
    return jax.shard_map(body, mesh=mesh, in_specs=in_specs, out_specs=out_specs, check_vma=False)
```

```python
import jax
import jax.numpy as jnp
from jax import lax
from jax.experimental import pallas as pl
from jax.experimental.pallas import tpu as pltpu
from jax.sharding import PartitionSpec as P


AXES = ("patch", "sub")
LEAST_EIGENVALUE = 0.0999
VMEM = pl.BlockSpec(memory_space=pltpu.VMEM)


def halves(a):
    high = a.astype(jnp.bfloat16)
    return high, (a - high.astype(jnp.float32)).astype(jnp.bfloat16)


def dot(a, b):
    a_high, a_low = a[0], a[1]
    b_high, b_low = halves(b)

    def product(p, q):
        return jnp.dot(p, q, preferred_element_type=jnp.float32)

    return product(a_high, b_high) + (product(a_high, b_low) + product(a_low, b_high))


def place():
    return lax.axis_index("patch") * lax.axis_size("sub") + lax.axis_index("sub")


def outer_block(tile):
    side = lax.axis_index("sub")
    outer = pl.ds(pl.multiple_of(side * tile, tile), tile)
    inner = pl.ds(pl.multiple_of((1 - side) * tile, tile), tile)
    return outer, inner


def flip(x):
    return pltpu.roll(x, x.shape[1] // 2, 1)


def index_of(shape, dimension):
    return lax.broadcasted_iota(jnp.int32, shape, dimension)


def toward(tiles, names, block):
    total = jnp.where(names[0:1, :] == block, tiles[0], 0.0)
    for k in range(1, tiles.shape[0]):
        total += jnp.where(names[k : k + 1, :] == block, tiles[k], 0.0)
    return total


def row_sums(tiles, masses):
    tile = tiles.shape[-1]
    whole = tiles[0]
    for k in range(1, tiles.shape[0]):
        whole += tiles[k]
    eye = index_of((tile, tile), 0) == index_of((tile, tile), 1)
    return jnp.sum(whole + jnp.where(eye, masses[0:1, :], 0.0), axis=1, keepdims=True)


def right_side(names, block, shape):
    vertices = block * shape[0] + index_of(shape, 0)
    return jnp.where(vertices == names[7:8, :], 1.0, 0.0)


def outer_kernel(
    cols_there, tiles_there, mass_there, x_there, sources_there,
    local_outer, diag_outer, t_out_t, x, x_inner, tiles_inner, names, masses, push, send,
    cols, tiles, mass, sources, arrived,
):
    tile = tiles.shape[-1]
    half = tile // 2
    slots = tiles.shape[0]
    position = place()
    side = lax.axis_index("sub")
    first = position * 2
    moves = (
        (cols_there, cols),
        (tiles_there.at[side], tiles),
        (x_there, x),
        (mass_there, mass),
        (sources_there, sources),
        (tiles_there.at[1 - side], tiles_inner),
    )
    copies = [pltpu.make_async_copy(start, end, arrived.at[i]) for i, (start, end) in enumerate(moves)]
    for copy in copies:
        copy.start()
    for copy in copies[:-1]:
        copy.wait()
    eye = index_of((tile, tile), 0) == index_of((tile, tile), 1)
    outer, inner = outer_block(tile)
    x_inner[...] = x[inner, :]
    row = index_of(names.shape, 0)
    named = jnp.broadcast_to(sources[...][None, :], names.shape)
    for k in range(slots):
        named = jnp.where(row == k, cols[1 - side, k], named)
    names[...] = named
    mass_0, mass_1 = mass[0:tile][None, :], mass[tile : 2 * tile][None, :]
    masses[...] = jnp.broadcast_to(jnp.where(side == 0, mass_1, mass_0), masses.shape)

    def one_toward(block):
        slot, scale = jnp.int32(0), 0.0
        for k in range(slots):
            found = cols[side, k] == block
            slot, scale = jnp.where(found, k, slot), jnp.where(found, 1.0, scale)
        return scale * tiles[slot]

    own = jnp.where(cols[side, 0] == first + side, tiles[0], 0.0)
    for k in range(1, slots):
        own += jnp.where(cols[side, k] == first + side, tiles[k], 0.0)
    cross = one_toward(first + 1 - side)
    total = row_sums(tiles, jnp.where(side == 0, mass_0, mass_1))
    diag_outer[...] = jnp.broadcast_to(total, diag_outer.shape)
    store_halves(local_outer, (slice(None), slice(0, tile)), jnp.where(side == 0, -own, -cross))
    store_halves(local_outer, (slice(None), slice(tile, 2 * tile)), jnp.where(side == 0, -cross, -own))
    store_halves(t_out_t, (slice(None),), one_toward(jnp.where(side == 0, first - 1, first + 2)).T)
    x_outer = x[outer, :]
    send[0:tile, :] = (
        right_side(named, first + side, x_outer.shape) - total * x_outer - dot(local_outer, x[...])
    )
    push[...] = dot(t_out_t, x_outer)
    above_diagonal = index_of((half, tile), 1) > index_of((half, tile), 0)
    send[tile : tile + half, :] = jnp.where(above_diagonal, own[:half], flip(own[half:]))
    diagonal = jnp.sum(jnp.where(eye, total, 0.0), axis=0, keepdims=True)
    send[tile + half :, :] = jnp.broadcast_to(diagonal, (8, tile))
    copies[-1].wait()


def store_halves(pair, index, value):
    pair[(0, *index)], pair[(1, *index)] = halves(value)


def inner_row_kernel(
    local_outer, diag_outer, x, tiles, names, masses, other_x, send,
    local, diag, t_in, t, t_inner, q_outer, q_send,
):
    tile = tiles.shape[-1]
    half = tile // 2
    position = place()
    side = lax.axis_index("sub")
    first = position * 2
    outer, inner = outer_block(tile)
    total = row_sums(tiles, masses)
    diag[...] = jnp.broadcast_to(total, diag.shape)
    own, cross = toward(tiles, names, first + 1 - side), toward(tiles, names, first + side)
    store_halves(local, (slice(None), slice(0, tile)), jnp.where(side == 0, -cross, -own))
    store_halves(local, (slice(None), slice(tile, 2 * tile)), jnp.where(side == 0, -own, -cross))
    store_halves(t_in, (slice(None),), toward(tiles, names, jnp.where(side == 0, first + 2, first - 1)))
    x_inner = x[inner, :]
    t[outer, :] = send[0:tile, :]
    t_inner[...] = (
        right_side(names, first + 1 - side, x_inner.shape)
        - total * x_inner
        - dot(local, x[...])
        + dot(t_in, other_x[...])
    )
    t[inner, :] = t_inner[...]
    q = (
        diag_outer[...] * send[0:tile, :]
        + dot(part(local_outer, slice(None), outer_columns(tile)), send[0:tile, :])
        + dot(part(local_outer, slice(None), inner_columns(tile)), t_inner[...])
    )
    q_outer[...] = q
    turned = jnp.where(side == 0, flip(q), q)
    first_half = index_of((half, tile), 1) < half
    q_send[...] = jnp.where(first_half, turned[:half], flip(turned[half:]))


def unpack(packed):
    tile = packed.shape[1]
    half = tile // 2
    rows = packed[0:half, :]
    row, column = index_of((half, tile), 0), index_of((half, tile), 1)
    upper = jnp.where(column > row, rows, 0.0)
    lower = flip(jnp.where(column < row, rows, 0.0))
    triangles = jnp.concatenate([upper, lower], axis=0)
    eye = index_of((tile, tile), 0) == index_of((tile, tile), 1)
    diagonal = jnp.sum(jnp.where(eye, packed[half : half + 1, :], 0.0), axis=1, keepdims=True)
    return triangles + triangles.T, diagonal


def outer_columns(tile):
    side = lax.axis_index("sub")
    return pl.ds(pl.multiple_of(side * tile, tile), tile)


def inner_columns(tile):
    side = lax.axis_index("sub")
    return pl.ds(pl.multiple_of((1 - side) * tile, tile), tile)


def part(pair, *index):
    return pair[(0, *index)], pair[(1, *index)]


def inner_kernel(local, diag, t_in, t_out_t, t, other_t, push_here, w_inner, t_in_t, t_out):
    tile = t_in.shape[-1]
    _, inner = outer_block(tile)
    w_inner[...] = (
        diag[...] * t[inner, :]
        + dot(local, t[...])
        + dot(part(local, slice(None), outer_columns(tile)), push_here[...])
        - dot(t_in, other_t[...])
    )
    for half in range(2):
        t_in_t[half] = t_in[half].T
        t_out[half] = t_out_t[half].T


def total(value):
    return jnp.sum(value, axis=0, keepdims=True)


def residual_kernel(local, diag, t_in_t, t_out_t, t, q_outer, push_here, r, w_outer, edge_r_out, edge_r_in):
    tile = t_in_t.shape[-1]
    outer, inner = outer_block(tile)
    push = push_here[...]
    r_outer = t[outer, :] + push
    r[outer, :] = r_outer
    r[inner, :] = t[inner, :]
    w_outer[...] = (
        q_outer[...] + diag[...] * push + dot(part(local, slice(None), outer_columns(tile)), push)
    )
    edge_r_out[...] = dot(t_out_t, r_outer)
    edge_r_in[...] = dot(t_in_t, t[inner, :])


def moment_kernel(
    local_outer, diag_outer, local_inner, diag_inner, t_in_t, t_out, t_out_t, r, w_local, edge_r_out, push_there, got, w_inner,
    w, there, edge_y_out, moments, edge_y_in,
):
    tile = t_out.shape[-1]
    outer, inner = outer_block(tile)
    push = push_there[...]
    r_outer, r_there = r[outer, :], got[0:tile, :] + push
    pull = dot(t_out, r_there)
    w_outer = w_local[...] - pull
    w[outer, :] = w_outer
    w[inner, :] = w_inner[...]
    w_now, r_now = w[...], r[...]
    r_r, r_w = total(r_now * r_now), total(r_now * w_now)
    shift = jnp.where(r_r > 0, r_w / r_r, 0.0)
    y = w_now - shift * r_now
    y_outer = w_outer - shift * r_outer
    y_inner = w_inner[...] - shift * r[inner, :]
    a_outer = diag_outer[...] * y_outer + dot(local_outer, y)
    a_inner = diag_inner[...] * y_inner + dot(local_inner, y)
    y_ay = total(y_outer * a_outer + y_inner * a_inner)
    y_pull, r_pull = total(y_outer * pull), total(r_outer * pull)
    r_ay = total(y * w_now) + total(r_outer * a_outer + r[inner, :] * a_inner) + y_pull
    moments[...] = jnp.concatenate(
        [r_r, r_w, total(y * y), y_ay, r_ay, r_w + r_pull, shift, y_pull, r_pull]
        + [shift] * (moments.shape[0] - 9),
        axis=0,
    )
    edge_y_out[...] = dot(t_out_t, y_outer)
    own_there, diag_there = unpack(got[tile:, :])
    there[...] = diag_there * push - dot(halves(own_there), push) - edge_r_out[...] - shift * r_there
    edge_y_in[...] = dot(t_in_t, y_inner)


def partner_kernel(moments, edge_y_in, edge_r_in, other_t, other_w, sums):
    y_partner = other_w[...] - moments[6:7, :] * other_t[...]
    row = index_of(moments.shape, 0)
    y_ay = jnp.where(row == 3, total(edge_y_in[...] * y_partner), 0.0)
    sums[...] = moments[...] - y_ay - jnp.where(row == 4, total(edge_r_in[...] * y_partner), 0.0)


def share_kernel(moments, edge_y_out, edge_r_out, there, got_q, out):
    tile = there.shape[0]
    half = tile // 2
    side = lax.axis_index("sub")
    q_half = got_q[...]
    q_flip = flip(q_half)
    q_there = jnp.concatenate(
        [jnp.where(side == 0, q_half, q_flip), jnp.where(side == 0, q_flip, q_half)], axis=0
    )
    y_there = q_there + there[...]
    mine = (index_of((1, out.shape[-1]), 1) >= half) == (side == 1)
    weight = jnp.where(mine, 2.0, 0.0)
    y_ay = weight * total(edge_y_out[...] * y_there)
    r_ay = weight * (total(edge_r_out[...] * y_there) + moments[7:8, :])
    r_ar = weight * moments[8:9, :]
    sums = moments[0:8, :]
    row = index_of(sums.shape, 0)
    for place_of, value in ((3, y_ay), (4, r_ay), (5, r_ar)):
        sums -= jnp.where(row == place_of, value, 0.0)
    for pair in range(out.shape[1]):
        out[:, pair] = jnp.broadcast_to(sums[None, 2 * pair : 2 * pair + 2], out[:, pair].shape)


def finish_kernel(shares, x, r, w, out):
    r_rs, r_ws, spreads, y_ay, r_ay, r_ar = [shares[:, row // 2, row % 2, :] for row in range(6)]
    r_r = jnp.sum(r_rs, axis=0, keepdims=True)
    r_w = jnp.sum(r_ws, axis=0, keepdims=True)
    theta = r_w / r_r
    off = jnp.where(r_rs > 0, r_ws / r_rs, 0.0) - theta
    spread = jnp.sum(spreads + r_rs * off * off, axis=0, keepdims=True)
    energy = jnp.sum(y_ay + off * (r_ay + off * r_ar), axis=0, keepdims=True)
    ratio = spread / (theta * theta * r_r)
    energy = jnp.maximum(energy - ratio * theta * spread, LEAST_EIGENVALUE * spread * (1.0 + ratio))
    step = jnp.where(spread > 0, spread / energy, 0.0)
    first = 1.0 / theta
    out[...] = x[...] + (first + step * (1.0 + ratio)) * r[...] - (step * first) * w[...]


def call(kernel, shapes, *operands, last=False):
    place_out = jax.ShapeDtypeStruct if last else pltpu.VMEM
    outs = [place_out(shape[1:], shape[0]) for shape in shapes]
    return pl.pallas_call(
        kernel,
        out_shape=outs if len(outs) > 1 else outs[0],
        in_specs=[VMEM] * len(operands),
        out_specs=[VMEM] * len(outs) if len(outs) > 1 else VMEM,
    )(*[pltpu.with_memory_space_constraint(operand, pltpu.VMEM) for operand in operands])


def body(block_cols, step_tiles, mass, warm_start, source_ids):
    tile = step_tiles.shape[-1]
    rows, columns = warm_start.shape
    assert block_cols.shape[0] == 2 and columns == tile and lax.axis_size("sub") == 2
    devices = lax.axis_size("patch") * lax.axis_size("sub")
    partner = [(i, i ^ 1) for i in range(devices)]
    groups = lax.axis_size("groups")
    across = []
    for group in range(groups):
        here, there = group * devices, (group + 1) % groups * devices
        for i in range(1, devices - 1, 2):
            across += [(here + i, here + i + 1), (here + i + 1, here + i)]
        across += [(here, there), (here + devices - 1, there + devices - 1)]
    single, slots = jnp.float32, block_cols.shape[1]
    assert slots < 8
    field, block = (single, rows, columns), (single, tile, columns)
    square, halfway = (jnp.bfloat16, 2, tile, tile), (single, tile // 2, columns)

    def exchange(value):
        return lax.ppermute(value, ("groups",) + AXES, across)

    results = [
        (jnp.bfloat16, 2, tile, rows), block, square, field, block, (single, slots, tile, tile),
        (jnp.int32, 8, tile), (single, 8, tile), block, (single, tile + tile // 2 + 8, columns),
    ]
    local_outer, diag_outer, t_out_t, x, x_inner, tiles_inner, names, masses, push_there, send = pl.pallas_call(
        outer_kernel,
        out_shape=[pltpu.VMEM(shape[1:], shape[0]) for shape in results],
        in_specs=[pl.BlockSpec(memory_space=pl.ANY)] * 5,
        out_specs=[VMEM] * len(results),
        scratch_shapes=[
            pltpu.SMEM(block_cols.shape, jnp.int32),
            pltpu.VMEM((slots, tile, tile), single),
            pltpu.VMEM(mass.shape, single),
            pltpu.VMEM(source_ids.shape, jnp.int32),
            pltpu.SemaphoreType.DMA((6,)),
        ],
        name="outer_kernel",
    )(block_cols, step_tiles, mass, warm_start, source_ids)
    push_here = exchange(push_there)
    other_x = lax.ppermute(x_inner, AXES, partner)
    got = exchange(send)
    local_inner, diag_inner, t_in, t, t_inner, q_outer, q_send = call(
        inner_row_kernel,
        [(jnp.bfloat16, 2, tile, rows), block, square, field, block, block, halfway],
        local_outer, diag_outer, x, tiles_inner, names, masses, other_x, send,
    )
    got_q = exchange(q_send)
    other_t = lax.ppermute(t_inner, AXES, partner)
    w_inner, t_in_t, t_out = call(
        inner_kernel, [block, square, square], local_inner, diag_inner, t_in, t_out_t, t, other_t, push_here
    )
    other_w = lax.ppermute(w_inner, AXES, partner)
    r, w_local, edge_r_out, edge_r_in = call(
        residual_kernel, [field, block, block, block],
        local_outer, diag_outer, t_in_t, t_out_t, t, q_outer, push_here,
    )
    w, there, edge_y_out, moments, edge_y_in = call(
        moment_kernel, [field, block, block, (single, 16, columns), block],
        local_outer, diag_outer, local_inner, diag_inner, t_in_t, t_out, t_out_t, r, w_local, edge_r_out, push_there, got, w_inner,
    )
    moments = call(
        partner_kernel, [(single, 16, columns)], moments, edge_y_in, edge_r_in, other_t, other_w
    )
    shares = call(
        share_kernel, [(single, devices, 3, 2, columns)], moments, edge_y_out, edge_r_out, there, got_q
    )
    shares = lax.all_to_all(shares, AXES, 0, 0)
    return call(finish_kernel, [field], shares, x, r, w, last=True)


def solution(mesh):
    in_specs = (
        P(("groups", "patch", "sub"), None),
        P(("groups", "patch", "sub"), None, None, None),
        P(("groups", "patch", "sub")),
        P(("groups", "patch", "sub"), None),
        P("groups"),
    )
    out_specs = P(("groups", "patch", "sub"), None)
    return jax.shard_map(body, mesh=mesh, in_specs=in_specs, out_specs=out_specs, check_vma=False)
```

```python
import jax
import jax.numpy as jnp
from jax import lax
from jax.experimental import pallas as pl
from jax.experimental.pallas import tpu as pltpu
from jax.sharding import PartitionSpec as P


AXES = ("patch", "sub")
LEAST_EIGENVALUE = 0.0999
VMEM = pl.BlockSpec(memory_space=pltpu.VMEM)


def halves(a):
    high = a.astype(jnp.bfloat16)
    return high, (a - high.astype(jnp.float32)).astype(jnp.bfloat16)


def dot(a, b):
    a_high, a_low = a[0], a[1]
    b_high, b_low = halves(b)

    def product(p, q):
        return jnp.dot(p, q, preferred_element_type=jnp.float32)

    return product(a_high, b_high) + (product(a_high, b_low) + product(a_low, b_high))


def place():
    return lax.axis_index("patch") * lax.axis_size("sub") + lax.axis_index("sub")


def outer_block(tile):
    side = lax.axis_index("sub")
    outer = pl.ds(pl.multiple_of(side * tile, tile), tile)
    inner = pl.ds(pl.multiple_of((1 - side) * tile, tile), tile)
    return outer, inner


def flip(x):
    return pltpu.roll(x, x.shape[1] // 2, 1)


def index_of(shape, dimension):
    return lax.broadcasted_iota(jnp.int32, shape, dimension)


def toward(tiles, names, block):
    total = jnp.where(names[0:1, :] == block, tiles[0], 0.0)
    for k in range(1, tiles.shape[0]):
        total += jnp.where(names[k : k + 1, :] == block, tiles[k], 0.0)
    return total


def row_sums(tiles, masses):
    tile = tiles.shape[-1]
    whole = tiles[0]
    for k in range(1, tiles.shape[0]):
        whole += tiles[k]
    eye = index_of((tile, tile), 0) == index_of((tile, tile), 1)
    return jnp.sum(whole + jnp.where(eye, masses[0:1, :], 0.0), axis=1, keepdims=True)


def right_side(names, block, shape):
    vertices = block * shape[0] + index_of(shape, 0)
    return jnp.where(vertices == names[7:8, :], 1.0, 0.0)


def outer_kernel(
    cols_there, tiles_there, mass_there, x_there, sources_there,
    local_outer, diag_outer, t_out_t, x, x_inner, tiles_inner, names, masses, push, send,
    cols, tiles, mass, sources, arrived,
):
    tile = tiles.shape[-1]
    half = tile // 2
    slots = tiles.shape[0]
    position = place()
    side = lax.axis_index("sub")
    first = position * 2
    moves = (
        (cols_there, cols),
        (tiles_there.at[side], tiles),
        (x_there, x),
        (mass_there, mass),
        (sources_there, sources),
        (tiles_there.at[1 - side], tiles_inner),
    )
    copies = [pltpu.make_async_copy(start, end, arrived.at[i]) for i, (start, end) in enumerate(moves)]
    for copy in copies:
        copy.start()
    for copy in copies[:-1]:
        copy.wait()
    eye = index_of((tile, tile), 0) == index_of((tile, tile), 1)
    outer, inner = outer_block(tile)
    x_inner[...] = x[inner, :]
    row = index_of(names.shape, 0)
    named = jnp.broadcast_to(sources[...][None, :], names.shape)
    for k in range(slots):
        named = jnp.where(row == k, cols[1 - side, k], named)
    names[...] = named
    mass_0, mass_1 = mass[0:tile][None, :], mass[tile : 2 * tile][None, :]
    masses[...] = jnp.broadcast_to(jnp.where(side == 0, mass_1, mass_0), masses.shape)

    def one_toward(block):
        slot, scale = jnp.int32(0), 0.0
        for k in range(slots):
            found = cols[side, k] == block
            slot, scale = jnp.where(found, k, slot), jnp.where(found, 1.0, scale)
        return scale * tiles[slot]

    own = jnp.where(cols[side, 0] == first + side, tiles[0], 0.0)
    for k in range(1, slots):
        own += jnp.where(cols[side, k] == first + side, tiles[k], 0.0)
    cross = one_toward(first + 1 - side)
    total = row_sums(tiles, jnp.where(side == 0, mass_0, mass_1))
    diag_outer[...] = jnp.broadcast_to(total, diag_outer.shape)
    store_halves(local_outer, (slice(None), slice(0, tile)), jnp.where(side == 0, -own, -cross))
    store_halves(local_outer, (slice(None), slice(tile, 2 * tile)), jnp.where(side == 0, -cross, -own))
    store_halves(t_out_t, (slice(None),), one_toward(jnp.where(side == 0, first - 1, first + 2)).T)
    x_outer = x[outer, :]
    send[0:tile, :] = (
        right_side(named, first + side, x_outer.shape) - total * x_outer - dot(local_outer, x[...])
    )
    push[...] = dot(t_out_t, x_outer)
    above_diagonal = index_of((half, tile), 1) > index_of((half, tile), 0)
    send[tile : tile + half, :] = jnp.where(above_diagonal, own[:half], flip(own[half:]))
    diagonal = jnp.sum(jnp.where(eye, total, 0.0), axis=0, keepdims=True)
    send[tile + half :, :] = jnp.broadcast_to(diagonal, (8, tile))
    copies[-1].wait()


def store_halves(pair, index, value):
    pair[(0, *index)], pair[(1, *index)] = halves(value)


def inner_row_kernel(
    local_outer, diag_outer, x, tiles, names, masses, other_x, send,
    local, diag, t_in, t, t_inner, q_outer, q_send,
):
    tile = tiles.shape[-1]
    half = tile // 2
    position = place()
    side = lax.axis_index("sub")
    first = position * 2
    outer, inner = outer_block(tile)
    total = row_sums(tiles, masses)
    diag[outer, :] = diag_outer[...]
    diag[inner, :] = jnp.broadcast_to(total, diag_outer.shape)
    own, cross = toward(tiles, names, first + 1 - side), toward(tiles, names, first + side)
    store_halves(local, (inner, slice(0, tile)), jnp.where(side == 0, -cross, -own))
    store_halves(local, (inner, slice(tile, 2 * tile)), jnp.where(side == 0, -own, -cross))
    for k in range(2):
        local[k, outer, :] = local_outer[k]
    store_halves(t_in, (slice(None),), toward(tiles, names, jnp.where(side == 0, first + 2, first - 1)))
    x_inner = x[inner, :]
    t[outer, :] = send[0:tile, :]
    t_inner[...] = (
        right_side(names, first + 1 - side, x_inner.shape)
        - total * x_inner
        - dot(part(local, inner), x[...])
        + dot(t_in, other_x[...])
    )
    t[inner, :] = t_inner[...]
    q = (
        diag_outer[...] * send[0:tile, :]
        + dot(part(local_outer, slice(None), outer_columns(tile)), send[0:tile, :])
        + dot(part(local_outer, slice(None), inner_columns(tile)), t_inner[...])
    )
    q_outer[...] = q
    turned = jnp.where(side == 0, flip(q), q)
    first_half = index_of((half, tile), 1) < half
    q_send[...] = jnp.where(first_half, turned[:half], flip(turned[half:]))


def unpack(packed):
    tile = packed.shape[1]
    half = tile // 2
    rows = packed[0:half, :]
    row, column = index_of((half, tile), 0), index_of((half, tile), 1)
    upper = jnp.where(column > row, rows, 0.0)
    lower = flip(jnp.where(column < row, rows, 0.0))
    triangles = jnp.concatenate([upper, lower], axis=0)
    eye = index_of((tile, tile), 0) == index_of((tile, tile), 1)
    diagonal = jnp.sum(jnp.where(eye, packed[half : half + 1, :], 0.0), axis=1, keepdims=True)
    return triangles + triangles.T, diagonal


def outer_columns(tile):
    side = lax.axis_index("sub")
    return pl.ds(pl.multiple_of(side * tile, tile), tile)


def inner_columns(tile):
    side = lax.axis_index("sub")
    return pl.ds(pl.multiple_of((1 - side) * tile, tile), tile)


def part(pair, *index):
    return pair[(0, *index)], pair[(1, *index)]


def inner_kernel(local, diag, t_in, t_out_t, t, other_t, push_here, w_inner, t_in_t, t_out):
    tile = t_in.shape[-1]
    _, inner = outer_block(tile)
    w_inner[...] = (
        diag[inner, :] * t[inner, :]
        + dot(part(local, inner), t[...])
        + dot(part(local, inner, outer_columns(tile)), push_here[...])
        - dot(t_in, other_t[...])
    )
    for half in range(2):
        t_in_t[half] = t_in[half].T
        t_out[half] = t_out_t[half].T


def total(value):
    return jnp.sum(value, axis=0, keepdims=True)


def residual_kernel(local, diag, t_in_t, t_out_t, t, q_outer, push_here, r, w_outer, edge_r_out, edge_r_in):
    tile = t_in_t.shape[-1]
    outer, inner = outer_block(tile)
    push = push_here[...]
    r_outer = t[outer, :] + push
    r[outer, :] = r_outer
    r[inner, :] = t[inner, :]
    w_outer[...] = q_outer[...] + diag[outer, :] * push + dot(part(local, outer, outer_columns(tile)), push)
    edge_r_out[...] = dot(t_out_t, r_outer)
    edge_r_in[...] = dot(t_in_t, t[inner, :])


def moment_kernel(
    local, diag, t_in_t, t_out, t_out_t, r, w_local, edge_r_out, push_there, got, w_inner,
    w, there, edge_y_out, moments, edge_y_in,
):
    tile = t_out.shape[-1]
    outer, inner = outer_block(tile)
    push = push_there[...]
    r_outer, r_there = r[outer, :], got[0:tile, :] + push
    pull = dot(t_out, r_there)
    w_outer = w_local[...] - pull
    w[outer, :] = w_outer
    w[inner, :] = w_inner[...]
    w_now, r_now = w[...], r[...]
    r_r, r_w = total(r_now * r_now), total(r_now * w_now)
    shift = jnp.where(r_r > 0, r_w / r_r, 0.0)
    y = w_now - shift * r_now
    y_outer = w_outer - shift * r_outer
    a_y = diag[...] * y + dot(local, y)
    y_pull, r_pull = total(y_outer * pull), total(r_outer * pull)
    r_ay = total(r_now * a_y + y * w_now) + y_pull
    moments[...] = jnp.concatenate(
        [r_r, r_w, total(y * y), total(y * a_y), r_ay, r_w + r_pull, shift, y_pull, r_pull]
        + [shift] * (moments.shape[0] - 9),
        axis=0,
    )
    edge_y_out[...] = dot(t_out_t, y_outer)
    own_there, diag_there = unpack(got[tile:, :])
    there[...] = diag_there * push - dot(halves(own_there), push) - edge_r_out[...] - shift * r_there
    edge_y_in[...] = dot(t_in_t, w_inner[...] - shift * r[inner, :])


def share_kernel(
    moments, edge_y_in, edge_r_in, edge_y_out, edge_r_out, there, got_q, other_t, other_w, out
):
    tile = there.shape[0]
    half = tile // 2
    side = lax.axis_index("sub")
    shift = moments[6:7, :]
    q_half = got_q[...]
    q_flip = flip(q_half)
    q_there = jnp.concatenate(
        [jnp.where(side == 0, q_half, q_flip), jnp.where(side == 0, q_flip, q_half)], axis=0
    )
    y_there = q_there + there[...]
    mine = (index_of(shift.shape, 1) >= half) == (side == 1)
    weight = jnp.where(mine, 2.0, 0.0)
    y_partner = other_w[...] - shift * other_t[...]
    y_ay = total(edge_y_in[...] * y_partner) + weight * total(edge_y_out[...] * y_there)
    r_ay = total(edge_r_in[...] * y_partner)
    r_ay += weight * (total(edge_r_out[...] * y_there) + moments[7:8, :])
    r_ar = weight * moments[8:9, :]
    sums = moments[0:8, :]
    row = index_of(sums.shape, 0)
    for place_of, value in ((3, y_ay), (4, r_ay), (5, r_ar)):
        sums -= jnp.where(row == place_of, value, 0.0)
    for pair in range(out.shape[1]):
        out[:, pair] = jnp.broadcast_to(sums[None, 2 * pair : 2 * pair + 2], out[:, pair].shape)


def finish_kernel(shares, x, r, w, out_there, out, left):
    r_rs, r_ws, spreads, y_ay, r_ay, r_ar = [shares[:, row // 2, row % 2, :] for row in range(6)]
    r_r = jnp.sum(r_rs, axis=0, keepdims=True)
    r_w = jnp.sum(r_ws, axis=0, keepdims=True)
    theta = r_w / r_r
    off = jnp.where(r_rs > 0, r_ws / r_rs, 0.0) - theta
    spread = jnp.sum(spreads + r_rs * off * off, axis=0, keepdims=True)
    energy = jnp.sum(y_ay + off * (r_ay + off * r_ar), axis=0, keepdims=True)
    ratio = spread / (theta * theta * r_r)
    energy = jnp.maximum(energy - ratio * theta * spread, LEAST_EIGENVALUE * spread * (1.0 + ratio))
    step = jnp.where(spread > 0, spread / energy, 0.0)
    first = 1.0 / theta
    by_r, by_w = first + step * (1.0 + ratio), step * first
    rows = out.shape[0] // 2
    copies = []
    for half in range(2):
        here = pl.ds(half * rows, rows)
        out[here, :] = x[here, :] + by_r * r[here, :] - by_w * w[here, :]
        copies.append(pltpu.make_async_copy(out.at[here], out_there.at[here], left.at[half]))
        copies[half].start()
    for copy in copies:
        copy.wait()


def call(kernel, shapes, *operands):
    outs = [pltpu.VMEM(shape[1:], shape[0]) for shape in shapes]
    return pl.pallas_call(
        kernel,
        out_shape=outs if len(outs) > 1 else outs[0],
        in_specs=[VMEM] * len(operands),
        out_specs=[VMEM] * len(outs) if len(outs) > 1 else VMEM,
    )(*[pltpu.with_memory_space_constraint(operand, pltpu.VMEM) for operand in operands])


def body(block_cols, step_tiles, mass, warm_start, source_ids):
    tile = step_tiles.shape[-1]
    rows, columns = warm_start.shape
    assert block_cols.shape[0] == 2 and columns == tile and lax.axis_size("sub") == 2
    devices = lax.axis_size("patch") * lax.axis_size("sub")
    partner = [(i, i ^ 1) for i in range(devices)]
    groups = lax.axis_size("groups")
    across = []
    for group in range(groups):
        here, there = group * devices, (group + 1) % groups * devices
        for i in range(1, devices - 1, 2):
            across += [(here + i, here + i + 1), (here + i + 1, here + i)]
        across += [(here, there), (here + devices - 1, there + devices - 1)]
    single, slots = jnp.float32, block_cols.shape[1]
    assert slots < 8
    field, block = (single, rows, columns), (single, tile, columns)
    square, halfway = (jnp.bfloat16, 2, tile, tile), (single, tile // 2, columns)

    def exchange(value):
        return lax.ppermute(value, ("groups",) + AXES, across)

    results = [
        (jnp.bfloat16, 2, tile, rows), block, square, field, block, (single, slots, tile, tile),
        (jnp.int32, 8, tile), (single, 8, tile), block, (single, tile + tile // 2 + 8, columns),
    ]
    local_outer, diag_outer, t_out_t, x, x_inner, tiles_inner, names, masses, push_there, send = pl.pallas_call(
        outer_kernel,
        out_shape=[pltpu.VMEM(shape[1:], shape[0]) for shape in results],
        in_specs=[pl.BlockSpec(memory_space=pl.ANY)] * 5,
        out_specs=[VMEM] * len(results),
        scratch_shapes=[
            pltpu.SMEM(block_cols.shape, jnp.int32),
            pltpu.VMEM((slots, tile, tile), single),
            pltpu.VMEM(mass.shape, single),
            pltpu.VMEM(source_ids.shape, jnp.int32),
            pltpu.SemaphoreType.DMA((6,)),
        ],
        name="outer_kernel",
    )(block_cols, step_tiles, mass, warm_start, source_ids)
    push_here = exchange(push_there)
    other_x = lax.ppermute(x_inner, AXES, partner)
    got = exchange(send)
    local, diag, t_in, t, t_inner, q_outer, q_send = call(
        inner_row_kernel,
        [(jnp.bfloat16, 2, rows, rows), field, square, field, block, block, halfway],
        local_outer, diag_outer, x, tiles_inner, names, masses, other_x, send,
    )
    got_q = exchange(q_send)
    other_t = lax.ppermute(t_inner, AXES, partner)
    w_inner, t_in_t, t_out = call(
        inner_kernel, [block, square, square], local, diag, t_in, t_out_t, t, other_t, push_here
    )
    other_w = lax.ppermute(w_inner, AXES, partner)
    r, w_local, edge_r_out, edge_r_in = call(
        residual_kernel, [field, block, block, block],
        local, diag, t_in_t, t_out_t, t, q_outer, push_here,
    )
    w, there, edge_y_out, moments, edge_y_in = call(
        moment_kernel, [field, block, block, (single, 16, columns), block],
        local, diag, t_in_t, t_out, t_out_t, r, w_local, edge_r_out, push_there, got, w_inner,
    )
    shares = call(
        share_kernel, [(single, devices, 3, 2, columns)],
        moments, edge_y_in, edge_r_in, edge_y_out, edge_r_out, there, got_q, other_t, other_w,
    )
    shares = lax.all_to_all(shares, AXES, 0, 0)
    return pl.pallas_call(
        finish_kernel,
        out_shape=jax.ShapeDtypeStruct((rows, columns), single),
        in_specs=[VMEM] * 4,
        out_specs=pl.BlockSpec(memory_space=pl.ANY),
        scratch_shapes=[pltpu.VMEM((rows, columns), single), pltpu.SemaphoreType.DMA((2,))],
        name="finish_kernel",
    )(*[pltpu.with_memory_space_constraint(operand, pltpu.VMEM) for operand in (shares, x, r, w)])


def solution(mesh):
    in_specs = (
        P(("groups", "patch", "sub"), None),
        P(("groups", "patch", "sub"), None, None, None),
        P(("groups", "patch", "sub")),
        P(("groups", "patch", "sub"), None),
        P("groups"),
    )
    out_specs = P(("groups", "patch", "sub"), None)
    return jax.shard_map(body, mesh=mesh, in_specs=in_specs, out_specs=out_specs, check_vma=False)
```

```python
import jax
import jax.numpy as jnp
from jax import lax
from jax.experimental import pallas as pl
from jax.experimental.pallas import tpu as pltpu
from jax.sharding import PartitionSpec as P


AXES = ("patch", "sub")
LEAST_EIGENVALUE = 0.0999
VMEM = pl.BlockSpec(memory_space=pltpu.VMEM)


def halves(a):
    high = a.astype(jnp.bfloat16)
    return high, (a - high.astype(jnp.float32)).astype(jnp.bfloat16)


def dot(a, b):
    a_high, a_low = a[0], a[1]
    b_high, b_low = halves(b)

    def product(p, q):
        return jnp.dot(p, q, preferred_element_type=jnp.float32)

    return product(a_high, b_high) + (product(a_high, b_low) + product(a_low, b_high))


def place():
    return lax.axis_index("patch") * lax.axis_size("sub") + lax.axis_index("sub")


def outer_block(tile):
    side = lax.axis_index("sub")
    outer = pl.ds(pl.multiple_of(side * tile, tile), tile)
    inner = pl.ds(pl.multiple_of((1 - side) * tile, tile), tile)
    return outer, inner


def flip(x):
    return pltpu.roll(x, x.shape[1] // 2, 1)


def index_of(shape, dimension):
    return lax.broadcasted_iota(jnp.int32, shape, dimension)


def toward(tiles, names, block):
    total = jnp.where(names[0:1, :] == block, tiles[0], 0.0)
    for k in range(1, tiles.shape[0]):
        total += jnp.where(names[k : k + 1, :] == block, tiles[k], 0.0)
    return total


def row_sums(tiles, masses):
    tile = tiles.shape[-1]
    whole = tiles[0]
    for k in range(1, tiles.shape[0]):
        whole += tiles[k]
    eye = index_of((tile, tile), 0) == index_of((tile, tile), 1)
    return jnp.sum(whole + jnp.where(eye, masses[0:1, :], 0.0), axis=1, keepdims=True)


def right_side(names, block, shape):
    vertices = block * shape[0] + index_of(shape, 0)
    return jnp.where(vertices == names[7:8, :], 1.0, 0.0)


def outer_kernel(
    cols_there, tiles_there, mass_there, x_there, sources_there,
    local_outer, diag_outer, t_out_t, x, x_inner, names, masses, push, send,
    cols, tiles, mass, sources, arrived,
):
    tile = tiles.shape[-1]
    half = tile // 2
    slots = tiles.shape[0]
    position = place()
    side = lax.axis_index("sub")
    first = position * 2
    moves = (
        (cols_there, cols),
        (tiles_there.at[side], tiles),
        (x_there, x),
        (mass_there, mass),
        (sources_there, sources),
    )
    copies = [pltpu.make_async_copy(start, end, arrived.at[i]) for i, (start, end) in enumerate(moves)]
    for copy in copies:
        copy.start()
    for copy in copies:
        copy.wait()
    eye = index_of((tile, tile), 0) == index_of((tile, tile), 1)
    outer, inner = outer_block(tile)
    x_inner[...] = x[inner, :]
    row = index_of(names.shape, 0)
    named = jnp.broadcast_to(sources[...][None, :], names.shape)
    for k in range(slots):
        named = jnp.where(row == k, cols[1 - side, k], named)
    names[...] = named
    mass_0, mass_1 = mass[0:tile][None, :], mass[tile : 2 * tile][None, :]
    masses[...] = jnp.broadcast_to(jnp.where(side == 0, mass_1, mass_0), masses.shape)

    def one_toward(block):
        slot, scale = jnp.int32(0), 0.0
        for k in range(slots):
            found = cols[side, k] == block
            slot, scale = jnp.where(found, k, slot), jnp.where(found, 1.0, scale)
        return scale * tiles[slot]

    own = jnp.where(cols[side, 0] == first + side, tiles[0], 0.0)
    for k in range(1, slots):
        own += jnp.where(cols[side, k] == first + side, tiles[k], 0.0)
    cross = one_toward(first + 1 - side)
    total = row_sums(tiles, jnp.where(side == 0, mass_0, mass_1))
    diag_outer[...] = jnp.broadcast_to(total, diag_outer.shape)
    store_halves(local_outer, (slice(None), slice(0, tile)), jnp.where(side == 0, -own, -cross))
    store_halves(local_outer, (slice(None), slice(tile, 2 * tile)), jnp.where(side == 0, -cross, -own))
    store_halves(t_out_t, (slice(None),), one_toward(jnp.where(side == 0, first - 1, first + 2)).T)
    x_outer = x[outer, :]
    send[0:tile, :] = (
        right_side(named, first + side, x_outer.shape) - total * x_outer - dot(local_outer, x[...])
    )
    push[...] = dot(t_out_t, x_outer)
    above_diagonal = index_of((half, tile), 1) > index_of((half, tile), 0)
    send[tile : tile + half, :] = jnp.where(above_diagonal, own[:half], flip(own[half:]))
    diagonal = jnp.sum(jnp.where(eye, total, 0.0), axis=0, keepdims=True)
    send[tile + half :, :] = jnp.broadcast_to(diagonal, (8, tile))


def store_halves(pair, index, value):
    pair[(0, *index)], pair[(1, *index)] = halves(value)


def inner_row_kernel(
    local_outer, diag_outer, x, all_tiles, names, masses, other_x, send,
    local, diag, t_in, t, t_inner, q_outer, q_send,
):
    tiles = all_tiles.at[1 - lax.axis_index("sub")]
    tile = tiles.shape[-1]
    half = tile // 2
    position = place()
    side = lax.axis_index("sub")
    first = position * 2
    outer, inner = outer_block(tile)
    total = row_sums(tiles, masses)
    diag[outer, :] = diag_outer[...]
    diag[inner, :] = jnp.broadcast_to(total, diag_outer.shape)
    own, cross = toward(tiles, names, first + 1 - side), toward(tiles, names, first + side)
    store_halves(local, (inner, slice(0, tile)), jnp.where(side == 0, -cross, -own))
    store_halves(local, (inner, slice(tile, 2 * tile)), jnp.where(side == 0, -own, -cross))
    for k in range(2):
        local[k, outer, :] = local_outer[k]
    store_halves(t_in, (slice(None),), toward(tiles, names, jnp.where(side == 0, first + 2, first - 1)))
    x_inner = x[inner, :]
    t[outer, :] = send[0:tile, :]
    t_inner[...] = (
        right_side(names, first + 1 - side, x_inner.shape)
        - total * x_inner
        - dot(part(local, inner), x[...])
        + dot(t_in, other_x[...])
    )
    t[inner, :] = t_inner[...]
    q = (
        diag_outer[...] * send[0:tile, :]
        + dot(part(local_outer, slice(None), outer_columns(tile)), send[0:tile, :])
        + dot(part(local_outer, slice(None), inner_columns(tile)), t_inner[...])
    )
    q_outer[...] = q
    turned = jnp.where(side == 0, flip(q), q)
    first_half = index_of((half, tile), 1) < half
    q_send[...] = jnp.where(first_half, turned[:half], flip(turned[half:]))


def unpack(packed):
    tile = packed.shape[1]
    half = tile // 2
    rows = packed[0:half, :]
    row, column = index_of((half, tile), 0), index_of((half, tile), 1)
    upper = jnp.where(column > row, rows, 0.0)
    lower = flip(jnp.where(column < row, rows, 0.0))
    triangles = jnp.concatenate([upper, lower], axis=0)
    eye = index_of((tile, tile), 0) == index_of((tile, tile), 1)
    diagonal = jnp.sum(jnp.where(eye, packed[half : half + 1, :], 0.0), axis=1, keepdims=True)
    return triangles + triangles.T, diagonal


def outer_columns(tile):
    side = lax.axis_index("sub")
    return pl.ds(pl.multiple_of(side * tile, tile), tile)


def inner_columns(tile):
    side = lax.axis_index("sub")
    return pl.ds(pl.multiple_of((1 - side) * tile, tile), tile)


def part(pair, *index):
    return pair[(0, *index)], pair[(1, *index)]


def inner_kernel(local, diag, t_in, t_out_t, t, other_t, push_here, w_inner, t_in_t, t_out):
    tile = t_in.shape[-1]
    _, inner = outer_block(tile)
    w_inner[...] = (
        diag[inner, :] * t[inner, :]
        + dot(part(local, inner), t[...])
        + dot(part(local, inner, outer_columns(tile)), push_here[...])
        - dot(t_in, other_t[...])
    )
    for half in range(2):
        t_in_t[half] = t_in[half].T
        t_out[half] = t_out_t[half].T


def total(value):
    return jnp.sum(value, axis=0, keepdims=True)


def residual_kernel(local, diag, t_in_t, t_out_t, t, q_outer, push_here, r, w_outer, edge_r_out, edge_r_in):
    tile = t_in_t.shape[-1]
    outer, inner = outer_block(tile)
    push = push_here[...]
    r_outer = t[outer, :] + push
    r[outer, :] = r_outer
    r[inner, :] = t[inner, :]
    w_outer[...] = q_outer[...] + diag[outer, :] * push + dot(part(local, outer, outer_columns(tile)), push)
    edge_r_out[...] = dot(t_out_t, r_outer)
    edge_r_in[...] = dot(t_in_t, t[inner, :])


def moment_kernel(
    local, diag, t_in_t, t_out, t_out_t, r, w_local, edge_r_out, push_there, got, w_inner,
    w, there, edge_y_out, moments, edge_y_in,
):
    tile = t_out.shape[-1]
    outer, inner = outer_block(tile)
    push = push_there[...]
    r_outer, r_there = r[outer, :], got[0:tile, :] + push
    pull = dot(t_out, r_there)
    w_outer = w_local[...] - pull
    w[outer, :] = w_outer
    w[inner, :] = w_inner[...]
    w_now, r_now = w[...], r[...]
    r_r, r_w = total(r_now * r_now), total(r_now * w_now)
    shift = jnp.where(r_r > 0, r_w / r_r, 0.0)
    y = w_now - shift * r_now
    y_outer = w_outer - shift * r_outer
    a_y = diag[...] * y + dot(local, y)
    y_pull, r_pull = total(y_outer * pull), total(r_outer * pull)
    r_ay = total(r_now * a_y + y * w_now) + y_pull
    moments[...] = jnp.concatenate(
        [r_r, r_w, total(y * y), total(y * a_y), r_ay, r_w + r_pull, shift, y_pull, r_pull]
        + [shift] * (moments.shape[0] - 9),
        axis=0,
    )
    edge_y_out[...] = dot(t_out_t, y_outer)
    own_there, diag_there = unpack(got[tile:, :])
    there[...] = diag_there * push - dot(halves(own_there), push) - edge_r_out[...] - shift * r_there
    edge_y_in[...] = dot(t_in_t, w_inner[...] - shift * r[inner, :])


def share_kernel(
    moments, edge_y_in, edge_r_in, edge_y_out, edge_r_out, there, got_q, other_t, other_w, out
):
    tile = there.shape[0]
    half = tile // 2
    side = lax.axis_index("sub")
    shift = moments[6:7, :]
    q_half = got_q[...]
    q_flip = flip(q_half)
    q_there = jnp.concatenate(
        [jnp.where(side == 0, q_half, q_flip), jnp.where(side == 0, q_flip, q_half)], axis=0
    )
    y_there = q_there + there[...]
    mine = (index_of(shift.shape, 1) >= half) == (side == 1)
    weight = jnp.where(mine, 2.0, 0.0)
    y_partner = other_w[...] - shift * other_t[...]
    y_ay = total(edge_y_in[...] * y_partner) + weight * total(edge_y_out[...] * y_there)
    r_ay = total(edge_r_in[...] * y_partner)
    r_ay += weight * (total(edge_r_out[...] * y_there) + moments[7:8, :])
    r_ar = weight * moments[8:9, :]
    sums = moments[0:8, :]
    row = index_of(sums.shape, 0)
    for place_of, value in ((3, y_ay), (4, r_ay), (5, r_ar)):
        sums -= jnp.where(row == place_of, value, 0.0)
    for pair in range(out.shape[1]):
        out[:, pair] = jnp.broadcast_to(sums[None, 2 * pair : 2 * pair + 2], out[:, pair].shape)


def finish_kernel(shares, x, r, w, out):
    r_rs, r_ws, spreads, y_ay, r_ay, r_ar = [shares[:, row // 2, row % 2, :] for row in range(6)]
    r_r = jnp.sum(r_rs, axis=0, keepdims=True)
    r_w = jnp.sum(r_ws, axis=0, keepdims=True)
    theta = r_w / r_r
    off = jnp.where(r_rs > 0, r_ws / r_rs, 0.0) - theta
    spread = jnp.sum(spreads + r_rs * off * off, axis=0, keepdims=True)
    energy = jnp.sum(y_ay + off * (r_ay + off * r_ar), axis=0, keepdims=True)
    ratio = spread / (theta * theta * r_r)
    energy = jnp.maximum(energy - ratio * theta * spread, LEAST_EIGENVALUE * spread * (1.0 + ratio))
    step = jnp.where(spread > 0, spread / energy, 0.0)
    first = 1.0 / theta
    out[...] = x[...] + (first + step * (1.0 + ratio)) * r[...] - (step * first) * w[...]


def call(kernel, shapes, *operands, last=False):
    place_out = jax.ShapeDtypeStruct if last else pltpu.VMEM
    outs = [place_out(shape[1:], shape[0]) for shape in shapes]
    return pl.pallas_call(
        kernel,
        out_shape=outs if len(outs) > 1 else outs[0],
        in_specs=[VMEM] * len(operands),
        out_specs=[VMEM] * len(outs) if len(outs) > 1 else VMEM,
    )(*[pltpu.with_memory_space_constraint(operand, pltpu.VMEM) for operand in operands])


def body(block_cols, step_tiles, mass, warm_start, source_ids):
    tile = step_tiles.shape[-1]
    rows, columns = warm_start.shape
    assert block_cols.shape[0] == 2 and columns == tile and lax.axis_size("sub") == 2
    devices = lax.axis_size("patch") * lax.axis_size("sub")
    partner = [(i, i ^ 1) for i in range(devices)]
    groups = lax.axis_size("groups")
    across = []
    for group in range(groups):
        here, there = group * devices, (group + 1) % groups * devices
        for i in range(1, devices - 1, 2):
            across += [(here + i, here + i + 1), (here + i + 1, here + i)]
        across += [(here, there), (here + devices - 1, there + devices - 1)]
    single, slots = jnp.float32, block_cols.shape[1]
    assert slots < 8
    field, block = (single, rows, columns), (single, tile, columns)
    square, halfway = (jnp.bfloat16, 2, tile, tile), (single, tile // 2, columns)

    def exchange(value):
        return lax.ppermute(value, ("groups",) + AXES, across)

    results = [
        (jnp.bfloat16, 2, tile, rows), block, square, field, block,
        (jnp.int32, 8, tile), (single, 8, tile), block, (single, tile + tile // 2 + 8, columns),
    ]
    local_outer, diag_outer, t_out_t, x, x_inner, names, masses, push_there, send = pl.pallas_call(
        outer_kernel,
        out_shape=[pltpu.VMEM(shape[1:], shape[0]) for shape in results],
        in_specs=[pl.BlockSpec(memory_space=pl.ANY)] * 5,
        out_specs=[VMEM] * len(results),
        scratch_shapes=[
            pltpu.SMEM(block_cols.shape, jnp.int32),
            pltpu.VMEM((slots, tile, tile), single),
            pltpu.VMEM(mass.shape, single),
            pltpu.VMEM(source_ids.shape, jnp.int32),
            pltpu.SemaphoreType.DMA((5,)),
        ],
        name="outer_kernel",
    )(block_cols, step_tiles, mass, warm_start, source_ids)
    push_here = exchange(push_there)
    other_x = lax.ppermute(x_inner, AXES, partner)
    got = exchange(send)
    local, diag, t_in, t, t_inner, q_outer, q_send = call(
        inner_row_kernel,
        [(jnp.bfloat16, 2, rows, rows), field, square, field, block, block, halfway],
        local_outer, diag_outer, x, step_tiles, names, masses, other_x, send,
    )
    got_q = exchange(q_send)
    other_t = lax.ppermute(t_inner, AXES, partner)
    w_inner, t_in_t, t_out = call(
        inner_kernel, [block, square, square], local, diag, t_in, t_out_t, t, other_t, push_here
    )
    other_w = lax.ppermute(w_inner, AXES, partner)
    r, w_local, edge_r_out, edge_r_in = call(
        residual_kernel, [field, block, block, block],
        local, diag, t_in_t, t_out_t, t, q_outer, push_here,
    )
    w, there, edge_y_out, moments, edge_y_in = call(
        moment_kernel, [field, block, block, (single, 16, columns), block],
        local, diag, t_in_t, t_out, t_out_t, r, w_local, edge_r_out, push_there, got, w_inner,
    )
    shares = call(
        share_kernel, [(single, devices, 3, 2, columns)],
        moments, edge_y_in, edge_r_in, edge_y_out, edge_r_out, there, got_q, other_t, other_w,
    )
    shares = lax.all_to_all(shares, AXES, 0, 0)
    return call(finish_kernel, [field], shares, x, r, w, last=True)


def solution(mesh):
    in_specs = (
        P(("groups", "patch", "sub"), None),
        P(("groups", "patch", "sub"), None, None, None),
        P(("groups", "patch", "sub")),
        P(("groups", "patch", "sub"), None),
        P("groups"),
    )
    out_specs = P(("groups", "patch", "sub"), None)
    return jax.shard_map(body, mesh=mesh, in_specs=in_specs, out_specs=out_specs, check_vma=False)
```
